32 devices in a mesh: dp: 4 (over y, x), tensor: 8 (over z, core).
Axes of the slice: x: 2, y: 2, z: 4, core: 2. Of those that a mesh axis runs over, the one named last changes fastest.
Arguments:
- attention_output: bfloat16 [512, 8192], P('dp', 'tensor'), may hold values from -6 to 6
- residual: bfloat16 [512, 8192], P('dp', 'tensor'), may hold values from -6 to 6
- output_weight: bfloat16 [8192, 8192], P('tensor'), may hold values from -0.09375 to 0.09375
- down_factors: bfloat16 [256, 8192, 16], P('dp', 'tensor'), may hold values from -0.0625 to 0.0625
- up_factors: bfloat16 [256, 16, 8192], P('dp', None, 'tensor'), may hold values from -1.5 to 1.5
- adapter_index: int32 [512], P('dp'), may hold values from 0 to 255, as said below
Outputs:
- layer_out: bfloat16 [512, 8192], P('dp', 'tensor')
The draws below stay inside these ranges and needn't reach their ends.
Inputs may be any that keep to these rules, and one draw needn't show every extreme that they name: adapter_index // 64 is the request group that owns the adapter. Of one group's 128 rows at most 64 use adapters owned by one group, and in every draw some group owns the adapters of exactly 64 rows of every group.
All inputs are finite; a program needn't handle non-finite values.
Results may differ from the reference program's by a relative error of at most 0.0041.
Values may be sent and summed in bfloat16 or wider, within the bound.
A program may use at most 64 MiB of HBM per device.

```python
import jax
import jax.numpy as jnp
from jax import lax

MODEL_WIDTH = 8192
ADAPTER_RANK = 16
ADP_DEV = 64
ROWS = 128
ATTENTION_WIDTH = 8192
ADAPTER_COUNT = 256
CAP = 64
ROWS_ALL = 512
N_DP = 4


def draw_adapter_index(key, part):
    hot_key = jax.random.fold_in(key, 11)
    group_key = jax.random.fold_in(key, 23)
    hot_group = jax.random.randint(hot_key, (), 0, N_DP)

    def one_group(group_index):
        base_key = jax.random.fold_in(group_key, group_index)
        key_one = jax.random.fold_in(base_key, 1)
        key_two = jax.random.fold_in(base_key, 2)
        key_three = jax.random.fold_in(base_key, 3)
        key_four = jax.random.fold_in(base_key, 4)
        others = (hot_group + 1 + jnp.arange((N_DP - 1) * CAP) // CAP) % N_DP
        others = jax.random.permutation(key_one, others)[:ROWS - CAP]
        owners = jnp.concatenate([jnp.full((CAP,), hot_group, jnp.int32), others.astype(jnp.int32)])
        owners = jax.random.permutation(key_two, owners)
        top_bound = jax.random.randint(key_three, (ROWS,), 1, ADP_DEV + 1)
        local_index = jax.random.randint(key_four, (ROWS,), 0, ADP_DEV) % top_bound
        return owners * ADP_DEV + local_index
    table = jax.vmap(one_group)(jnp.arange(N_DP))
    return table.reshape(-1).astype(jnp.int32)


def strengthened(result, rng, source, target, parts, factor):
    def block_of(dim):
        return (jnp.arange(result.shape[dim]) // (result.shape[dim] // parts)).reshape((-1,) + (1,) * (result.ndim - 1 - dim))

    near = jax.random.permutation(rng, parts)[block_of(target)]
    far = (block_of(target) + parts // 2) % parts
    return jnp.where((block_of(source) == near) | (block_of(source) == far), factor * result, result)


def levels(stream_key, dims, cuts, least, high):
    loudness, own = 1.0, jax.random.fold_in(stream_key, 6)
    for axis_at, parts in cuts:
        steps = jnp.exp(jax.random.uniform(jax.random.fold_in(own, axis_at), (parts,), jnp.float32, least / len(cuts), high / len(cuts)))
        loudness = loudness * jnp.repeat(steps, dims[axis_at] // parts).reshape([-1 if axis == axis_at else 1 for axis in range(len(dims))])
    return loudness


def bell_draw(key, shape, scale, limit, cuts=(), kind=jnp.bfloat16):
    level = levels(key, shape, cuts, -0.22, 0.18) if cuts else 1.0
    result = jax.random.normal(key, shape, jnp.float32) * scale * level
    return jnp.minimum(jnp.maximum(result, -limit), limit).astype(kind)


def noise_with(stream_key, dims, deviation, reach, pieces, heavy, dtype=jnp.bfloat16):
    values = deviation * jax.random.normal(stream_key, dims, jnp.float32)
    if pieces:
        values = values * levels(stream_key, dims, pieces, -0.22, 0.18)
    return jnp.clip(strengthened(values, jax.random.fold_in(stream_key, 3), *heavy), -reach, reach).astype(dtype)


def setup_inputs(seed: int = 0) -> dict:
    keys = jax.random.split(jax.random.key(seed), 7)
    attention_output = bell_draw(keys[0], (ROWS_ALL, ATTENTION_WIDTH), 1.0, 6.0, ((0, 4), (1, 8)))
    residual = bell_draw(keys[1], (ROWS_ALL, MODEL_WIDTH), 1.0, 6.0, ((0, 4), (1, 8)))
    output_weight = noise_with(keys[2], (ATTENTION_WIDTH, MODEL_WIDTH), ATTENTION_WIDTH ** -0.5, 0.09375, ((0, 8),), (0, 1, 8, 2.0))
    down_factors = bell_draw(keys[3], (ADAPTER_COUNT, ATTENTION_WIDTH, ADAPTER_RANK), ATTENTION_WIDTH ** -0.5, 0.0625, ((0, 4), (1, 8)))
    up_factors = bell_draw(keys[4], (ADAPTER_COUNT, ADAPTER_RANK, MODEL_WIDTH), ADAPTER_RANK ** -0.5, 1.5, ((0, 4), (2, 8)))
    adapter_index = draw_adapter_index(jax.random.fold_in(keys[6], 71), 0)
    return {"attention_output": attention_output, "residual": residual, "output_weight": output_weight, "down_factors": down_factors, "up_factors": up_factors, "adapter_index": adapter_index}


def reference(attention_output, residual, output_weight, down_factors, up_factors, adapter_index):
    base_out = jnp.dot(attention_output, output_weight, preferred_element_type=jnp.float32)
    blocks = ROWS_ALL // ROWS

    def branch(block_in):
        x_rows, row_indices = block_in
        selected_down = down_factors[row_indices].astype(jnp.float32)
        shrink = jnp.einsum("rk,rkj->rj", x_rows.astype(jnp.float32), selected_down).astype(jnp.bfloat16)
        selected_up = up_factors[row_indices].astype(jnp.float32)
        return jnp.einsum("rj,rjc->rc", shrink.astype(jnp.float32), selected_up).astype(jnp.bfloat16)

    expand = lax.map(branch, (attention_output.reshape(blocks, ROWS, ATTENTION_WIDTH), adapter_index.reshape(blocks, ROWS)))
    expand = expand.reshape(ROWS_ALL, MODEL_WIDTH)
    total = residual.astype(jnp.float32) + base_out + expand.astype(jnp.float32)
    return total.astype(jnp.bfloat16)
```

```python
import contextlib
import functools

import jax
import jax.numpy as jnp
from jax import lax
from jax.experimental import pallas as pl
from jax.experimental.pallas import tpu as pltpu
from jax.sharding import PartitionSpec as P

MESH = pl.DeviceIdType.MESH
F32 = jnp.float32
BF16 = jnp.bfloat16
LANES = 128
PIECES = 4
AHEAD = 4
FIRST = 2
ORDER = (
    ("near", 0), ("project", 0, 1), ("project", 0, 2), ("settle", 0, 0), ("far", 0),
    ("project", 0, 3), ("settle", 0, 1), ("place", 1), ("near", 1), ("far", 1), ("factors",),
    ("project", 0, 4), ("settle", 0, 2), ("project", 0, 5), ("settle", 0, 3),
    ("project", 0, 6), ("settle", 0, 4), ("project", 0, 7), ("settle", 0, 5),
    ("project", 1, 0), ("settle", 0, 6), ("project", 1, 1), ("settle", 0, 7), ("greet",),
    ("project", 1, 2), ("on", 0, 1, 0), ("on", 0, 1, 1),
    ("shrink", 0), ("project", 1, 3), ("project", 1, 4), ("meet",), ("sum", 0),
    ("on", 0, 1, 2), ("on", 0, 1, 3),
    ("project", 1, 5), ("settle", 1, 0), ("settle", 1, 1),
    ("first", 1, 0, 0), ("first", 1, 0, 1), ("first", 1, 0, 2),
    ("project", 1, 6), ("project", 1, 7),
    ("shrink", 1), ("on", 0, 2, 0), ("on", 0, 2, 1), ("sum", 1),
    ("settle", 1, 2), ("settle", 1, 3), ("settle", 1, 4), ("settle", 1, 5),
    ("settle", 1, 6), ("settle", 1, 7),
    ("first", 1, 0, 3),
    ("first", 1, 1, 0), ("first", 1, 1, 1), ("first", 1, 1, 2), ("first", 1, 1, 3),
    ("first", 1, 2, 0), ("first", 1, 2, 1), ("first", 1, 2, 2), ("first", 1, 2, 3),
    ("on", 0, 2, 2), ("on", 0, 2, 3),
    ("expand", 0), ("on", 1, 1, 0), ("expand", 1),
    ("on", 1, 1, 1), ("on", 1, 1, 2), ("on", 1, 1, 3),
    ("on", 1, 2, 0), ("on", 1, 2, 1), ("on", 1, 2, 2), ("on", 1, 2, 3),
)
scope = contextlib.nullcontext


def kernel(
    groups, members, rank, owned, halves, pieces,
    x_hbm, res_ref, idx_hbm, w_ref, down_ref, up_ref, out_ref,
    x_ref, idx_ref, wbuf, dbuf, ubuf, rbuf, own, psend, precv, rrecv, lrecv, rsend, lsend,
    xsend, xrecv, packed, arp, arz, esend, eback,
    w_sem, d_sem, ps_sem, pr_sem, rs_sem, ls_sem, hr_sem,
    xs_sem, xr_sem, as_sem, ar_sem, zs_sem, zr_sem, es_sem, er_sem, dp_sem, z_sem,
):
    chips = members // 2
    g = lax.axis_index("dp")
    t = lax.axis_index("tensor")
    z = t // 2
    c = lax.rem(t, 2)
    partner = z * 2 + (1 - c)
    rows, depth = x_ref.shape
    width = out_ref.shape[1]
    part = xrecv.shape[2]
    slots = groups * part
    low = z < chips // 2
    piece = width // pieces
    last_chip = chips - 1

    def core_of(chip):
        return (g, chip * 2 + c)

    bits = groups.bit_length() - 1
    cube = groups == 1 << bits

    def peer(k):
        if not cube:
            return lax.rem(g + k, groups)
        to = g
        for b in range(bits):
            if k >> b & 1:
                to = to + (1 << b) * (1 - 2 * lax.rem(g // (1 << b), 2))
        return to

    def source_of(k):
        return peer(k) if cube else lax.rem(g + groups - k, groups)

    near = [1 << b for b in range(bits)] if cube else list(range(1, groups))
    far = [k for k in range(1, groups) if k not in near]
    rounds = bits - 1 if far else 0

    barrier = pltpu.get_barrier_semaphore()
    pl.semaphore_signal(barrier, inc=1, device_id=(g, partner), device_id_type=MESH)

    @pl.when(z > 0)
    def _():
        pl.semaphore_signal(barrier, inc=1, device_id=core_of(z - 1), device_id_type=MESH)

    @pl.when(z < last_chip)
    def _():
        pl.semaphore_signal(barrier, inc=1, device_id=core_of(z + 1), device_id_type=MESH)

    for k in near:
        pl.semaphore_signal(barrier, inc=1, device_id=(peer(k), t), device_id_type=MESH)

    def block_chip(i):
        return jnp.where(low, chips - 1 - i, i)

    blocks = [(n, 0, width) for n in range(members)]
    if pieces % 2 == 0:
        blocks[:1] = [(0, p * width // 2, width // 2) for p in range(2)]
    chunks = len(blocks)
    loaded = set()

    def weight_copy(j):
        n, offset, size = blocks[j]
        column = block_chip(n % chips) * 2 + n // chips
        start = pl.multiple_of(column * width + offset, LANES)
        return pltpu.make_async_copy(
            w_ref.at[:, pl.ds(start, size)], wbuf.at[n, :, pl.ds(offset, size)],
            w_sem.at[j % AHEAD],
        )

    def weights(n, column):
        for j in range(chunks):
            if j not in loaded and blocks[j][:2] <= (n, column) and blocks[j][0] == n:
                weight_copy(j).wait()
                loaded.add(j)
                if j + AHEAD < chunks:
                    weight_copy(j + AHEAD).start()

    down_copy = pltpu.make_async_copy(down_ref, dbuf, d_sem.at[0])
    up_copy = pltpu.make_async_copy(up_ref, ubuf, d_sem.at[1])
    res_copy = pltpu.make_async_copy(res_ref, rbuf, d_sem.at[2])
    x_copy = pltpu.make_async_copy(x_hbm, x_ref, d_sem.at[0])
    idx_copy = pltpu.make_async_copy(idx_hbm, idx_ref, d_sem.at[1])
    idx_copy.start()
    x_copy.start()
    for j in range(min(FIRST, chunks)):
        weight_copy(j).start()

    def enter():
        near_chips = jnp.where(z > 0, 1, 0) + jnp.where(z < last_chip, 1, 0)
        pl.semaphore_wait(barrier, 1 + len(near) + near_chips)

    def tell(b):
        pl.semaphore_signal(
            dp_sem.at[b], inc=1, device_id=(peer(1 << b), t), device_id_type=MESH
        )

    def tell_chip(n, to):
        pl.semaphore_signal(z_sem.at[n], inc=1, device_id=core_of(to), device_id_type=MESH)

    def greet_far():
        for b in range(rounds):
            pl.semaphore_wait(dp_sem.at[b], 1)
            if b + 1 < rounds:
                tell(b + 1)

    def greet_ends():
        if chips < 3:
            return

        @pl.when(z == 0)
        def _():
            tell_chip(0, z + 1)

        @pl.when(z == last_chip)
        def _():
            tell_chip(1, z - 1)

    def greet_chips():
        if chips < 3:
            return

        @pl.when((z > 0) & low)
        def _():
            pl.semaphore_wait(z_sem.at[0], 1)
            tell_chip(0, z + 1)
            pl.semaphore_wait(z_sem.at[1], 1)
            tell_chip(1, z - 1)

        @pl.when((z < last_chip) & jnp.logical_not(low))
        def _():
            pl.semaphore_wait(z_sem.at[1], 1)
            tell_chip(1, z - 1)
            pl.semaphore_wait(z_sem.at[0], 1)
            tell_chip(0, z + 1)

    def meet_chips():
        if chips < 3:
            return

        @pl.when(z == 0)
        def _():
            pl.semaphore_wait(z_sem.at[1], 1)

        @pl.when(z == last_chip)
        def _():
            pl.semaphore_wait(z_sem.at[0], 1)

    idx_copy.wait()
    for j in range(FIRST, min(AHEAD, chunks)):
        weight_copy(j).start()
    idx_row = idx_ref[...]
    r_i = lax.broadcasted_iota(jnp.int32, (rows, rows), 0)
    c_i = lax.broadcasted_iota(jnp.int32, (rows, rows), 1)
    idx_full = jnp.broadcast_to(idx_row, (rows, rows))
    idx_col = jnp.sum(jnp.where(r_i == c_i, idx_full, 0), axis=1, keepdims=True)
    own_row = idx_row // owned
    own_col = idx_col // owned
    same = own_col == own_row
    rank_row = jnp.sum(jnp.where(same & (r_i < c_i), 1, 0), axis=0, keepdims=True)
    rank_col = jnp.sum(jnp.where(same & (c_i < r_i), 1, 0), axis=1, keepdims=True)

    def slot_of(place_rank, owner, h):
        inside = place_rank - h * part
        keep = (inside >= 0) & (inside < part)
        return jnp.where(keep, owner * part + inside, -1)

    number_row = lax.rem(idx_row, owned) + 1
    step = min(256, depth)

    def row_copy(h, k):
        to = peer(k)
        return pltpu.make_async_remote_copy(
            src_ref=xsend.at[h, to], dst_ref=xrecv.at[h, g],
            send_sem=xs_sem.at[0], recv_sem=xr_sem.at[h],
            device_id=(to, t), device_id_type=MESH,
        )

    others = pl.ds(0, groups - 1)

    def all_of(send, recv, send_sem, recv_sem):
        return pltpu.make_async_remote_copy(
            src_ref=send, dst_ref=recv, send_sem=send_sem, recv_sem=recv_sem,
            device_id=(g, partner), device_id_type=MESH,
        )

    def rows_wait(h):
        all_of(
            xsend.at[h, others], xrecv.at[h, others], xs_sem.at[0], xr_sem.at[h]
        ).wait_recv()

    def place_rows(h):
        slot_row = slot_of(rank_row, own_row, h)
        placing = lax.broadcasted_iota(jnp.int32, (slots, rows), 0) == slot_row
        request = jnp.sum(jnp.where(placing, number_row, 0), axis=1, keepdims=True)
        place = jnp.where(placing, 1.0, 0.0).astype(BF16)
        numbers = jnp.broadcast_to(request.astype(F32), (slots, LANES)).astype(BF16)
        for k in range(groups):
            xsend[h, k, :, depth:] = numbers[k * part:(k + 1) * part]
        for j in range(depth // step):
            moved = jnp.dot(
                place, x_ref[:, j * step:(j + 1) * step], preferred_element_type=F32
            ).astype(BF16)
            for k in range(groups):
                xsend[h, k, :, j * step:(j + 1) * step] = moved[k * part:(k + 1) * part]
        xrecv[h, g] = xsend[h, g]

    tile = min(256, piece)
    tiles = piece // tile

    def pair_copy(chip, q):
        k = chip * pieces + q
        return pltpu.make_async_remote_copy(
            src_ref=psend.at[k], dst_ref=precv.at[k], send_sem=ps_sem.at[0],
            recv_sem=pr_sem.at[k], device_id=(g, partner), device_id_type=MESH,
        )

    strip = 16

    def hop(chip, q, to, send, recv, s_sem, shift):
        k = chip * pieces + q
        return pltpu.make_async_remote_copy(
            src_ref=send.at[k], dst_ref=recv.at[k], send_sem=s_sem.at[0],
            recv_sem=hr_sem.at[k + shift * pieces], device_id=(g, to * 2 + c),
            device_id_type=MESH,
        )

    right = functools.partial(hop, send=rsend, recv=rrecv, s_sem=rs_sem, shift=1)
    left = functools.partial(hop, send=lsend, recv=lrecv, s_sem=ls_sem, shift=0)

    def pass_on(chip, q, first, to, make, send, recv):
        k = chip * pieces + q
        if not first:
            make(chip, q, to).wait_recv()

        @pl.loop(0, rows // strip)
        def _(n):
            at = pl.ds(pl.multiple_of(n * strip, strip), strip)
            value = own[k, at] + precv[k, at].astype(F32)
            if not first:
                value = value + recv[k, at].astype(F32)
            send[k, at] = value.astype(BF16)

        make(chip, q, to).start()

    sent = set()

    def send_first(core, turn, q):
        if turn >= last_chip or ("first", core, turn, q) in sent:
            return
        sent.add(("first", core, turn, q))

        @pl.when((c == core) & (z == 0))
        def _():
            pass_on(chips - 1 - turn, q, True, z + 1, right, rsend, rrecv)

        @pl.when((c == core) & (z == last_chip))
        def _():
            pass_on(turn, q, True, z - 1, left, lsend, lrecv)

    def send_on(core, turn, q):
        if turn == 0 or turn >= last_chip or ("on", core, turn, q) in sent:
            return
        sent.add(("on", core, turn, q))

        @pl.when((c == core) & (z > 0) & (z <= turn))
        def _():
            pass_on(chips - 1 - turn + z, q, False, z + 1, right, rsend, rrecv)

        @pl.when((c == core) & (z < last_chip) & (last_chip - z <= turn))
        def _():
            pass_on(turn - chips + 1 + z, q, False, z - 1, left, lsend, lrecv)

    wave = 2 if pieces % 2 == 0 else 1

    steps = [(i, q) for i in range(chips) for q in range(0, pieces, wave)]

    def product(n, q, into, k):
        for m in range(tiles * wave):
            at = q * piece + m * tile
            into[k + m // tiles, :, m % tiles * tile:(m % tiles + 1) * tile] = jnp.dot(
                x_ref[...], wbuf[n, :, at:at + tile], preferred_element_type=F32
            ).astype(into.dtype)

    def project(phase, n):
        i, q = steps[n]
        block = phase * chips + i
        k = block_chip(i) * pieces + q
        weights(block, q * piece)

        @pl.when(c == phase)
        def _():
            product(block, q, own, k)

        @pl.when(c != phase)
        def _():
            product(block, q, psend, k)
            if phase + n > 0:
                send_other(n)

    def send_other(n):
        i, q = steps[n]
        for p in range(wave):
            pair_copy(block_chip(i), q + p).start()

    def settle(phase, n):
        i, first = steps[n]
        for q in range(first, first + wave):
            @pl.when(c == phase)
            def _():
                pair_copy(block_chip(i), q).wait_recv()

            if phase == 0:
                send_first(0, i, q)

    lane_number = (lax.broadcasted_iota(jnp.int32, (slots, LANES), 1) // rank + 1).astype(F32)
    per_tile = LANES // rank
    tile_count = owned * rank // LANES
    chunk = min(512, owned * rank)

    def term_pair(h):
        return pltpu.make_async_remote_copy(
            src_ref=packed.at[h], dst_ref=arp.at[h], send_sem=as_sem.at[0],
            recv_sem=ar_sem.at[h], device_id=(g, partner), device_id_type=MESH,
        )

    def term_copy(h, k, core):
        to = lax.rem(z + k, chips)
        return pltpu.make_async_remote_copy(
            src_ref=arz.at[h, z], dst_ref=arz.at[h, z], send_sem=zs_sem.at[0],
            recv_sem=zr_sem.at[h], device_id=(g, to * 2 + core), device_id_type=MESH,
        )

    def terms_wait(h):
        @pl.when(c == 0)
        def _():
            all_of(arz.at[h], arz.at[h], zs_sem.at[0], zr_sem.at[h]).wait_recv()

        if chips > 1:
            @pl.when(c == 1)
            def _():
                far_chips = pl.ds(0, chips - 1)
                all_of(
                    arz.at[h, far_chips], arz.at[h, far_chips], zs_sem.at[0], zr_sem.at[h]
                ).wait_recv()

    def wanted_of(h):
        return xrecv[h, :, :, depth:].reshape(slots, LANES).astype(F32)

    def shrink_rows(h):
        rows_wait(h)
        if h == 0:
            down_copy.wait()
        wanted = wanted_of(h).T[:rank]
        flat = xrecv[h, :, :, :depth].reshape(slots, depth)
        mine = jnp.zeros((rank, slots), F32)
        for first in range(0, owned * rank, chunk):
            every = lax.dot_general(
                dbuf[first:first + chunk, :], flat, (((1,), (1,)), ((), ())),
                preferred_element_type=F32,
            )
            for p in range(chunk // rank):
                number = float(first // rank + p + 1)
                mine = jnp.where(wanted == number, every[p * rank:(p + 1) * rank], mine)
        packed[h] = mine

        @pl.when(c == 0)
        def _():
            term_pair(h).start()

    def sum_send(h):
        @pl.when(c == 1)
        def _():
            term_pair(h).wait_recv()
            arz[h, z] = packed[h] + arp[h]
            term_copy(h, 0, 0).start()
            for k in range(1, chips):
                for core in range(2):
                    term_copy(h, k, core).start()

    def back_copy(h, k):
        to = peer(k)
        return pltpu.make_async_remote_copy(
            src_ref=esend.at[h, to], dst_ref=eback.at[h, g],
            send_sem=es_sem.at[0], recv_sem=er_sem.at[h],
            device_id=(to, t), device_id_type=MESH,
        )

    def back_wait(h):
        all_of(
            esend.at[h, others], eback.at[h, others], es_sem.at[0], er_sem.at[h]
        ).wait_recv()

    wide = min(256, width)

    def expand_rows(h):
        terms_wait(h)
        total = arz[h, 0]
        for k in range(1, chips):
            total = total + arz[h, k]
        total = total.astype(BF16).astype(F32)
        if h == 0:
            up_copy.wait()
        wanted = wanted_of(h)
        shrink = jnp.concatenate([total] * per_tile, axis=0).T
        spread = jnp.concatenate(
            [
                jnp.where(wanted == lane_number + float(m * per_tile), shrink, 0.0).astype(BF16)
                for m in range(tile_count)
            ],
            axis=1,
        )

        @pl.loop(0, width // wide)
        def _(n):
            cols = pl.ds(pl.multiple_of(n * wide, LANES), wide)
            grown = jnp.dot(spread, ubuf[:, cols], preferred_element_type=F32).astype(BF16)
            for k in range(groups):
                esend[h, k, :, cols] = grown[k * part:(k + 1) * part]

        for k in range(1, groups):
            back_copy(h, k).start()
        eback[h, g] = esend[h, g]

    with scope("x"):
        x_copy.wait()
    with scope("place0"):
        place_rows(0)
    with scope("project0_0"):
        project(0, 0)
    with scope("enter"):
        enter()

    @pl.when(c == 1)
    def _():
        send_other(0)

    if rounds:
        tell(0)
    greet_ends()

    def near_rows(h):
        for k in near:
            row_copy(h, k).start()

    def far_rows(h):
        if h == 0:
            greet_far()
        for k in far:
            row_copy(h, k).start()

    def load_factors():
        down_copy.start()
        up_copy.start()
        res_copy.start()

    stages = {
        "project": project, "settle": settle, "place": place_rows, "near": near_rows,
        "far": far_rows, "greet": greet_chips, "meet": meet_chips, "factors": load_factors,
        "shrink": shrink_rows, "sum": sum_send, "expand": expand_rows,
        "first": send_first, "on": send_on,
    }
    for name, *at in ORDER:
        if name in ("first", "on"):
            if at[2] >= pieces:
                continue
        elif name in ("project", "settle"):
            if at[1] >= len(steps):
                continue
        elif at and at[0] >= halves:
            continue
        with scope(name + "_".join(str(v) for v in at)):
            stages[name](*at)
    for turn in range(last_chip):
        for q in range(pieces):
            for core in range(2):
                send_first(core, turn, q)
                send_on(core, turn, q)

    res_copy.wait()

    def branch_of(h, q, n):
        slot_col = slot_of(rank_col, own_col, h)
        unplace = jnp.where(
            lax.broadcasted_iota(jnp.int32, (rows, slots), 1) == slot_col, 1.0, 0.0
        ).astype(BF16)
        first = q * piece + n * tile
        back = eback[h, :, :, first:first + tile].reshape(slots, tile)
        return jnp.dot(unplace, back, preferred_element_type=F32)

    for h in range(halves):
        with scope("backwait%d" % h):
            back_wait(h)
        for q in range(pieces):
            for n in range(tiles):
                cols = slice(n * tile, (n + 1) * tile)
                first = q * piece + n * tile
                value = own[z * pieces + q, :, cols] + branch_of(h, q, n)
                if h == 0:
                    value = (
                        value + precv[z * pieces + q, :, cols].astype(F32)
                        + rbuf[:, first:first + tile].astype(F32)
                    )
                own[z * pieces + q, :, cols] = value

    for q in range(pieces):
        mine_at = z * pieces + q
        mark = scope("fin%d" % q)
        mark.__enter__()

        def finish(use_right, use_left):
            @pl.loop(0, rows // strip)
            def _(n):
                at = pl.ds(pl.multiple_of(n * strip, strip), strip)
                value = own[mine_at, at]
                if use_right:
                    value = value + rrecv[mine_at, at].astype(F32)
                if use_left:
                    value = value + lrecv[mine_at, at].astype(F32)
                out_ref[at, q * piece:(q + 1) * piece] = value.astype(BF16)

        if chips == 1:
            finish(False, False)
        else:
            @pl.when(z == 0)
            def _():
                left(z, q, z).wait_recv()
                finish(False, True)

            @pl.when(z == chips - 1)
            def _():
                right(z, q, z).wait_recv()
                finish(True, False)

            @pl.when((z > 0) & (z < chips - 1))
            def _():
                right(z, q, z).wait_recv()
                left(z, q, z).wait_recv()
                finish(True, True)
        mark.__exit__(None, None, None)

    tail = scope("tail")
    tail.__enter__()
    all_of(psend, precv, ps_sem.at[0], ps_sem.at[0]).wait_send()

    @pl.when(c == 0)
    def _():
        all_of(packed, arp, as_sem.at[0], as_sem.at[0]).wait_send()

    @pl.when(c == 1)
    def _():
        all_of(arz, arz, zs_sem.at[0], zs_sem.at[0]).wait_send()
        if chips > 1:
            far_chips = pl.ds(0, chips - 1)
            all_of(
                arz.at[:, far_chips], arz.at[:, far_chips], zs_sem.at[0], zs_sem.at[0]
            ).wait_send()

    if groups > 1:
        all_of(
            xsend.at[:, others], xrecv.at[:, others], xs_sem.at[0], xs_sem.at[0]
        ).wait_send()
        all_of(
            esend.at[:, others], eback.at[:, others], es_sem.at[0], es_sem.at[0]
        ).wait_send()
    for chip in range(chips):
        @pl.when(z == chip)
        def _():
            if chip < last_chip:
                sent = pl.ds(0, (last_chip - chip) * pieces)
                all_of(
                    rsend.at[sent], rrecv.at[sent], rs_sem.at[0], rs_sem.at[0]
                ).wait_send()
            if chip > 0:
                sent = pl.ds(0, chip * pieces)
                all_of(
                    lsend.at[sent], lrecv.at[sent], ls_sem.at[0], ls_sem.at[0]
                ).wait_send()
    tail.__exit__(None, None, None)


def body(attention_output, residual, output_weight, down_factors, up_factors, adapter_index):
    groups = lax.axis_size("dp")
    members = lax.axis_size("tensor")
    rows, depth = attention_output.shape
    owned, _, rank = down_factors.shape
    width = output_weight.shape[1] // members
    cap = 2 * rows // groups
    chips = members // 2
    halves = 2 if cap % 32 == 0 else 1
    part = cap // halves
    slots = groups * part
    pieces = max(1, min(PIECES, width // 256))
    piece = width // pieces
    down = jnp.swapaxes(down_factors, 1, 2).reshape(owned * rank, depth)
    up = up_factors.reshape(owned * rank, width)
    vmem = pl.BlockSpec(memory_space=pltpu.VMEM)
    hbm = pl.BlockSpec(memory_space=pl.ANY)
    dma = pltpu.SemaphoreType.DMA
    hops = chips * pieces
    return pl.pallas_call(
        functools.partial(kernel, groups, members, rank, owned, halves, pieces),
        out_shape=pltpu.VMEM((rows, width), BF16),
        in_specs=[hbm] * 6,
        out_specs=vmem,
        scratch_shapes=[
            pltpu.VMEM((rows, depth), BF16),
            pltpu.VMEM((1, rows), jnp.int32),
            pltpu.VMEM((members, depth, width), BF16),
            pltpu.VMEM((owned * rank, depth), BF16),
            pltpu.VMEM((owned * rank, width), BF16),
            pltpu.VMEM((rows, width), BF16),
            pltpu.VMEM((hops, rows, piece), F32),
            pltpu.VMEM((hops, rows, piece), BF16),
            pltpu.VMEM((hops, rows, piece), BF16),
            pltpu.VMEM((hops, rows, piece), BF16),
            pltpu.VMEM((hops, rows, piece), BF16),
            pltpu.VMEM((hops, rows, piece), BF16),
            pltpu.VMEM((hops, rows, piece), BF16),
            pltpu.VMEM((halves, groups, part, depth + LANES), BF16),
            pltpu.VMEM((halves, groups, part, depth + LANES), BF16),
            pltpu.VMEM((halves, rank, slots), F32),
            pltpu.VMEM((halves, rank, slots), F32),
            pltpu.VMEM((halves, chips, rank, slots), F32),
            pltpu.VMEM((halves, groups, part, width), BF16),
            pltpu.VMEM((halves, groups, part, width), BF16),
            dma((AHEAD,)), dma((3,)), dma((1,)), dma((hops,)),
            dma((1,)), dma((1,)), dma((hops + pieces,)),
            dma((1,)), dma((halves,)), dma((1,)), dma((halves,)),
            dma((1,)), dma((halves,)), dma((1,)), dma((halves,)),
            pltpu.SemaphoreType.REGULAR((max(1, groups.bit_length() - 2),)),
            pltpu.SemaphoreType.REGULAR((2,)),
        ],
        compiler_params=pltpu.CompilerParams(
            collective_id=0, has_side_effects=True, vmem_limit_bytes=60 * 1024 * 1024
        ),
    )(attention_output, residual, adapter_index.reshape(1, rows), output_weight, down, up)


def solution(mesh):
    return jax.shard_map(
        body,
        mesh=mesh,
        in_specs=(
            P("dp", "tensor"),
            P("dp", "tensor"),
            P("tensor", None),
            P("dp", "tensor", None),
            P("dp", None, "tensor"),
            P("dp"),
        ),
        out_specs=P("dp", "tensor"),
        check_vma=False,
    )
```

```python
import contextlib
import functools

import jax
import jax.numpy as jnp
from jax import lax
from jax.experimental import pallas as pl
from jax.experimental.pallas import tpu as pltpu
from jax.sharding import PartitionSpec as P

MESH = pl.DeviceIdType.MESH
F32 = jnp.float32
BF16 = jnp.bfloat16
LANES = 128
PIECES = 4
AHEAD = 4
FIRST = 2
ORDER = (
    ("near", 0), ("project", 0, 1), ("project", 0, 2), ("settle", 0, 0), ("far", 0),
    ("project", 0, 3), ("settle", 0, 1), ("place", 1), ("far", 1), ("near", 1), ("factors",),
    ("project", 0, 4), ("settle", 0, 2), ("project", 0, 5), ("settle", 0, 3),
    ("project", 0, 6), ("settle", 0, 4), ("project", 0, 7), ("settle", 0, 5),
    ("project", 1, 0), ("settle", 0, 6), ("settle", 0, 7), ("requests",), ("greet",),
    ("on", 0, 1, 0), ("on", 0, 1, 1), ("on", 0, 1, 2), ("on", 0, 1, 3),
    ("shrink", 0), ("project", 1, 1), ("project", 1, 2),
    ("meet",), ("sum", 0), ("project", 1, 3),
    ("settle", 1, 0), ("settle", 1, 1), ("first", 1, 0, 0),
    ("shrink", 1), ("project", 1, 4), ("sum", 1),
    ("first", 1, 0, 1), ("first", 1, 0, 2), ("first", 1, 0, 3),
    ("project", 1, 5), ("project", 1, 6), ("project", 1, 7),
    ("settle", 1, 2), ("settle", 1, 3),
    ("first", 1, 1, 0), ("first", 1, 1, 1), ("first", 1, 1, 2), ("first", 1, 1, 3),
    ("settle", 1, 4), ("settle", 1, 5),
    ("first", 1, 2, 0), ("first", 1, 2, 1), ("first", 1, 2, 2), ("first", 1, 2, 3),
    ("settle", 1, 6), ("settle", 1, 7),
    ("on", 0, 2, 0), ("on", 0, 2, 1), ("on", 0, 2, 2), ("on", 0, 2, 3),
    ("long", 0, 2, 0), ("long", 0, 2, 1), ("on", 1, 1, 0),
    ("expand", 0), ("long", 0, 2, 2), ("long", 0, 2, 3),
    ("on", 1, 1, 1), ("on", 1, 1, 2), ("on", 1, 1, 3), ("expand", 1),
    ("long", 1, 2, 0), ("on", 1, 2, 0), ("long", 1, 2, 1), ("on", 1, 2, 1),
    ("long", 1, 2, 2), ("on", 1, 2, 2), ("long", 1, 2, 3), ("on", 1, 2, 3),
)
scope = contextlib.nullcontext


def kernel(
    groups, members, rank, owned, halves, pieces,
    x_hbm, res_ref, idx_hbm, w_ref, down_ref, up_ref, out_ref,
    x_ref, idx_ref, idx_all, wbuf, dbuf, ubuf, rbuf, own, psend, precv, rrecv, lrecv, rsend, lsend,
    xsend, xrecv, wants, packed, arp, arz, esend, eback,
    w_sem, d_sem, ps_sem, pr_sem, rs_sem, ls_sem, hr_sem,
    xs_sem, xr_sem, as_sem, ar_sem, zs_sem, zr_sem, es_sem, er_sem, dp_sem, z_sem, is_sem, ir_sem,
):
    chips = members // 2
    g = lax.axis_index("dp")
    t = lax.axis_index("tensor")
    z = t // 2
    c = lax.rem(t, 2)
    partner = z * 2 + (1 - c)
    rows, depth = x_ref.shape
    width = out_ref.shape[1]
    part = xrecv.shape[2]
    slots = groups * part
    low = z < chips // 2
    high = jnp.logical_not(low)
    piece = width // pieces
    last_chip = chips - 1

    def core_of(chip):
        return (g, chip * 2 + c)

    bits = groups.bit_length() - 1
    cube = groups == 1 << bits

    def peer(k):
        if not cube:
            return lax.rem(g + k, groups)
        to = g
        for b in range(bits):
            if k >> b & 1:
                to = to + (1 << b) * (1 - 2 * lax.rem(g // (1 << b), 2))
        return to

    def source_of(k):
        return peer(k) if cube else lax.rem(g + groups - k, groups)

    near = [1 << b for b in range(bits)] if cube else list(range(1, groups))
    far = [k for k in range(1, groups) if k not in near]
    rounds = bits - 1 if far else 0

    barrier = pltpu.get_barrier_semaphore()
    pl.semaphore_signal(barrier, inc=1, device_id=(g, partner), device_id_type=MESH)

    @pl.when(z > 0)
    def _():
        pl.semaphore_signal(barrier, inc=1, device_id=core_of(z - 1), device_id_type=MESH)

    @pl.when(z < last_chip)
    def _():
        pl.semaphore_signal(barrier, inc=1, device_id=core_of(z + 1), device_id_type=MESH)

    for k in near:
        pl.semaphore_signal(barrier, inc=1, device_id=(peer(k), t), device_id_type=MESH)

    def block_chip(i):
        return jnp.where(low, chips - 1 - i, i)

    blocks = [(n, 0, width) for n in range(members)]
    if pieces % 2 == 0:
        blocks[:1] = [(0, p * width // 2, width // 2) for p in range(2)]
    chunks = len(blocks)
    loaded = set()

    def weight_copy(j):
        n, offset, size = blocks[j]
        column = block_chip(n % chips) * 2 + n // chips
        start = pl.multiple_of(column * width + offset, LANES)
        return pltpu.make_async_copy(
            w_ref.at[:, pl.ds(start, size)], wbuf.at[n, :, pl.ds(offset, size)],
            w_sem.at[j % AHEAD],
        )

    def weights(n, column):
        for j in range(chunks):
            if j not in loaded and blocks[j][:2] <= (n, column) and blocks[j][0] == n:
                weight_copy(j).wait()
                loaded.add(j)
                if j + AHEAD < chunks:
                    weight_copy(j + AHEAD).start()

    down_copy = pltpu.make_async_copy(down_ref, dbuf, d_sem.at[0])
    up_copy = pltpu.make_async_copy(up_ref, ubuf, d_sem.at[1])
    res_copy = pltpu.make_async_copy(res_ref, rbuf, d_sem.at[2])
    x_copy = pltpu.make_async_copy(x_hbm, x_ref, d_sem.at[0])
    idx_copy = pltpu.make_async_copy(idx_hbm, idx_ref, d_sem.at[1])
    idx_copy.start()
    x_copy.start()
    for j in range(min(FIRST, chunks)):
        weight_copy(j).start()

    def enter():
        near_chips = jnp.where(z > 0, 1, 0) + jnp.where(z < last_chip, 1, 0)
        pl.semaphore_wait(barrier, 1 + len(near) + near_chips)

    def tell(b):
        pl.semaphore_signal(
            dp_sem.at[b], inc=1, device_id=(peer(1 << b), t), device_id_type=MESH
        )

    def tell_chip(n, to):
        pl.semaphore_signal(z_sem.at[n], inc=1, device_id=core_of(to), device_id_type=MESH)

    def greet_far():
        for b in range(rounds):
            pl.semaphore_wait(dp_sem.at[b], 1)
            if b + 1 < rounds:
                tell(b + 1)

    def greet_ends():
        if chips < 3:
            return

        @pl.when(z == 0)
        def _():
            tell_chip(0, z + 1)

        @pl.when(z == last_chip)
        def _():
            tell_chip(1, z - 1)

    def greet_chips():
        if chips < 3:
            return

        @pl.when((z > 0) & low)
        def _():
            pl.semaphore_wait(z_sem.at[0], 1)
            tell_chip(0, z + 1)
            pl.semaphore_wait(z_sem.at[1], 1)
            tell_chip(1, z - 1)

        @pl.when((z < last_chip) & jnp.logical_not(low))
        def _():
            pl.semaphore_wait(z_sem.at[1], 1)
            tell_chip(1, z - 1)
            pl.semaphore_wait(z_sem.at[0], 1)
            tell_chip(0, z + 1)

    def meet_chips():
        if chips < 3:
            return

        @pl.when(z == 0)
        def _():
            pl.semaphore_wait(z_sem.at[1], 1)

        @pl.when(z == last_chip)
        def _():
            pl.semaphore_wait(z_sem.at[0], 1)

    idx_copy.wait()
    for j in range(FIRST, min(AHEAD, chunks)):
        weight_copy(j).start()
    idx_row = idx_ref[...]
    r_i = lax.broadcasted_iota(jnp.int32, (rows, rows), 0)
    c_i = lax.broadcasted_iota(jnp.int32, (rows, rows), 1)
    idx_full = jnp.broadcast_to(idx_row, (rows, rows))
    idx_col = jnp.sum(jnp.where(r_i == c_i, idx_full, 0), axis=1, keepdims=True)
    own_row = idx_row // owned
    own_col = idx_col // owned
    same = own_col == own_row
    rank_row = jnp.sum(jnp.where(same & (r_i < c_i), 1, 0), axis=0, keepdims=True)
    rank_col = jnp.sum(jnp.where(same & (c_i < r_i), 1, 0), axis=1, keepdims=True)

    def slot_of(place_rank, owner, h):
        inside = place_rank - h * part
        keep = (inside >= 0) & (inside < part)
        return jnp.where(keep, owner * part + inside, -1)

    step = min(256, depth)

    def row_copy(h, k):
        to = peer(k)
        return pltpu.make_async_remote_copy(
            src_ref=xsend.at[h, to], dst_ref=xrecv.at[h, g],
            send_sem=xs_sem.at[0], recv_sem=xr_sem.at[h],
            device_id=(to, t), device_id_type=MESH,
        )

    others = pl.ds(0, groups - 1)

    def all_of(send, recv, send_sem, recv_sem):
        return pltpu.make_async_remote_copy(
            src_ref=send, dst_ref=recv, send_sem=send_sem, recv_sem=recv_sem,
            device_id=(g, partner), device_id_type=MESH,
        )

    def idx_copy_to(k):
        return pltpu.make_async_remote_copy(
            src_ref=idx_ref, dst_ref=idx_all.at[g], send_sem=is_sem.at[0],
            recv_sem=ir_sem.at[0], device_id=(peer(k), t), device_id_type=MESH,
        )

    def requests():
        idx_all[g] = idx_ref[...]
        if groups > 1:
            all_of(
                idx_all.at[others], idx_all.at[others], is_sem.at[0], ir_sem.at[0]
            ).wait_recv()
        every_row = jnp.concatenate([idx_all[k] for k in range(groups)], axis=0)
        chosen = every_row // owned == g
        earlier = jnp.where(r_i < c_i, 1.0, 0.0).astype(BF16)
        ahead = jnp.dot(
            jnp.where(chosen, 1.0, 0.0).astype(BF16), earlier, preferred_element_type=F32
        ).astype(jnp.int32)
        slot = jnp.where(chosen, ahead, -1)
        number = lax.rem(every_row, owned) + 1
        for h in range(halves):
            for k in range(groups):
                place = lax.broadcasted_iota(jnp.int32, (part, rows), 0) + h * part
                asked = jnp.where(place == slot[k:k + 1], number[k:k + 1], 0)
                wants[h, k * part:(k + 1) * part] = jnp.broadcast_to(
                    jnp.sum(asked, axis=1, keepdims=True).astype(F32), (part, LANES)
                )

    def rows_wait(h):
        all_of(
            xsend.at[h, others], xrecv.at[h, others], xs_sem.at[0], xr_sem.at[h]
        ).wait_recv()

    def place_rows(h):
        slot_row = slot_of(rank_row, own_row, h)
        placing = lax.broadcasted_iota(jnp.int32, (slots, rows), 0) == slot_row
        place = jnp.where(placing, 1.0, 0.0).astype(BF16)
        for j in range(depth // step):
            moved = jnp.dot(
                place, x_ref[:, j * step:(j + 1) * step], preferred_element_type=F32
            ).astype(BF16)
            for k in range(groups):
                xsend[h, k, :, j * step:(j + 1) * step] = moved[k * part:(k + 1) * part]
        xrecv[h, g] = xsend[h, g]

    tile = min(256, piece)
    tiles = piece // tile

    def pair_copy(chip, q):
        k = chip * pieces + q
        return pltpu.make_async_remote_copy(
            src_ref=psend.at[k], dst_ref=precv.at[k], send_sem=ps_sem.at[0],
            recv_sem=pr_sem.at[k], device_id=(g, partner), device_id_type=MESH,
        )

    strip = 16

    def hop(chip, q, to, send, recv, s_sem, shift):
        k = chip * pieces + q
        return pltpu.make_async_remote_copy(
            src_ref=send.at[k], dst_ref=recv.at[k], send_sem=s_sem.at[0],
            recv_sem=hr_sem.at[k + shift * pieces], device_id=(g, to * 2 + c),
            device_id_type=MESH,
        )

    right = functools.partial(hop, send=rsend, recv=rrecv, s_sem=rs_sem, shift=1)
    left = functools.partial(hop, send=lsend, recv=lrecv, s_sem=ls_sem, shift=0)

    def pass_on(chip, q, first, to, make, send, recv):
        k = chip * pieces + q
        if not first:
            make(chip, q, to).wait_recv()

        @pl.loop(0, rows // strip)
        def _(n):
            at = pl.ds(pl.multiple_of(n * strip, strip), strip)
            value = own[k, at] + precv[k, at].astype(F32)
            if not first:
                value = value + recv[k, at].astype(F32)
            send[k, at] = value.astype(BF16)

        make(chip, q, to).start()

    sent = set()

    def send_first(core, turn, q):
        if turn >= last_chip or ("first", core, turn, q) in sent:
            return
        sent.add(("first", core, turn, q))

        @pl.when((c == core) & (z == 0))
        def _():
            pass_on(chips - 1 - turn, q, True, z + 1, right, rsend, rrecv)

        @pl.when((c == core) & (z == last_chip))
        def _():
            pass_on(turn, q, True, z - 1, left, lsend, lrecv)

    def send_on(core, turn, q):
        if turn == 0 or turn >= last_chip or ("on", core, turn, q) in sent:
            return
        sent.add(("on", core, turn, q))

        @pl.when((c == core) & low & (z > 0) & (z <= turn))
        def _():
            pass_on(chips - 1 - turn + z, q, False, z + 1, right, rsend, rrecv)

        @pl.when((c == core) & high & (z < last_chip) & (last_chip - z <= turn))
        def _():
            pass_on(turn - chips + 1 + z, q, False, z - 1, left, lsend, lrecv)

    def send_long(core, turn, q):
        if turn < chips - chips // 2 or turn >= last_chip or ("long", core, turn, q) in sent:
            return
        sent.add(("long", core, turn, q))

        @pl.when((c == core) & high & (z <= turn))
        def _():
            pass_on(chips - 1 - turn + z, q, False, z + 1, right, rsend, rrecv)

        @pl.when((c == core) & low & (last_chip - z <= turn))
        def _():
            pass_on(turn - chips + 1 + z, q, False, z - 1, left, lsend, lrecv)

    wave = 2 if pieces % 2 == 0 else 1

    steps = [(i, q) for i in range(chips) for q in range(0, pieces, wave)]

    def product(n, q, into, k):
        for m in range(tiles * wave):
            at = q * piece + m * tile
            into[k + m // tiles, :, m % tiles * tile:(m % tiles + 1) * tile] = jnp.dot(
                x_ref[...], wbuf[n, :, at:at + tile], preferred_element_type=F32
            ).astype(into.dtype)

    def project(phase, n):
        i, q = steps[n]
        block = phase * chips + i
        k = block_chip(i) * pieces + q
        weights(block, q * piece)

        @pl.when(c == phase)
        def _():
            product(block, q, own, k)

        @pl.when(c != phase)
        def _():
            product(block, q, psend, k)
            if phase + n > 0:
                send_other(n)

    def send_other(n):
        i, q = steps[n]
        for p in range(wave):
            pair_copy(block_chip(i), q + p).start()

    def settle(phase, n):
        i, first = steps[n]
        for q in range(first, first + wave):
            @pl.when(c == phase)
            def _():
                pair_copy(block_chip(i), q).wait_recv()

            if phase == 0:
                send_first(0, i, q)

    lane_number = (lax.broadcasted_iota(jnp.int32, (slots, LANES), 1) // rank + 1).astype(F32)
    per_tile = LANES // rank
    tile_count = owned * rank // LANES
    chunk = min(512, owned * rank)

    def term_pair(h):
        return pltpu.make_async_remote_copy(
            src_ref=packed.at[h], dst_ref=arp.at[h], send_sem=as_sem.at[0],
            recv_sem=ar_sem.at[h], device_id=(g, partner), device_id_type=MESH,
        )

    def term_copy(h, k, core):
        to = lax.rem(z + jnp.where(low, chips - k, k), chips)
        return pltpu.make_async_remote_copy(
            src_ref=arz.at[h, z], dst_ref=arz.at[h, z], send_sem=zs_sem.at[0],
            recv_sem=zr_sem.at[h], device_id=(g, to * 2 + core), device_id_type=MESH,
        )

    def terms_wait(h):
        @pl.when(c == 0)
        def _():
            all_of(arz.at[h], arz.at[h], zs_sem.at[0], zr_sem.at[h]).wait_recv()

        if chips > 1:
            @pl.when(c == 1)
            def _():
                far_chips = pl.ds(0, chips - 1)
                all_of(
                    arz.at[h, far_chips], arz.at[h, far_chips], zs_sem.at[0], zr_sem.at[h]
                ).wait_recv()

    def wanted_of(h):
        return wants[h]

    def shrink_rows(h):
        rows_wait(h)
        if h == 0:
            down_copy.wait()
        wanted = wanted_of(h).T[:rank]
        flat = xrecv[h].reshape(slots, depth)
        mine = jnp.zeros((rank, slots), F32)
        for first in range(0, owned * rank, chunk):
            every = lax.dot_general(
                dbuf[first:first + chunk, :], flat, (((1,), (1,)), ((), ())),
                preferred_element_type=F32,
            )
            for p in range(chunk // rank):
                number = float(first // rank + p + 1)
                mine = jnp.where(wanted == number, every[p * rank:(p + 1) * rank], mine)
        packed[h] = mine

        @pl.when(c == 0)
        def _():
            term_pair(h).start()

    def sum_send(h):
        @pl.when(c == 1)
        def _():
            term_pair(h).wait_recv()
            arz[h, z] = packed[h] + arp[h]
            term_copy(h, 0, 0).start()
            for k in range(1, chips):
                for core in range(2):
                    term_copy(h, k, core).start()

    def back_copy(h, k):
        to = peer(k)
        return pltpu.make_async_remote_copy(
            src_ref=esend.at[h, to], dst_ref=eback.at[h, g],
            send_sem=es_sem.at[0], recv_sem=er_sem.at[h],
            device_id=(to, t), device_id_type=MESH,
        )

    def back_wait(h):
        all_of(
            esend.at[h, others], eback.at[h, others], es_sem.at[0], er_sem.at[h]
        ).wait_recv()

    wide = min(512, width)

    def expand_rows(h):
        terms_wait(h)
        total = arz[h, 0]
        for k in range(1, chips):
            total = total + arz[h, k]
        total = total.astype(BF16).astype(F32)
        if h == 0:
            up_copy.wait()
        wanted = wanted_of(h)
        shrink = jnp.concatenate([total] * per_tile, axis=0).T
        spread = jnp.concatenate(
            [
                jnp.where(wanted == lane_number + float(m * per_tile), shrink, 0.0).astype(BF16)
                for m in range(tile_count)
            ],
            axis=1,
        )

        @pl.loop(0, width // wide)
        def _(n):
            cols = pl.ds(pl.multiple_of(n * wide, LANES), wide)
            grown = jnp.dot(spread, ubuf[:, cols], preferred_element_type=F32).astype(BF16)
            for k in range(groups):
                esend[h, k, :, cols] = grown[k * part:(k + 1) * part]

        for k in far + near:
            back_copy(h, k).start()
        eback[h, g] = esend[h, g]

    with scope("x"):
        x_copy.wait()
    with scope("place0"):
        place_rows(0)
    with scope("project0_0"):
        project(0, 0)
    with scope("enter"):
        enter()

    @pl.when(c == 1)
    def _():
        send_other(0)

    if rounds:
        tell(0)
    greet_ends()

    def near_rows(h):
        for k in near:
            if h == 0:
                idx_copy_to(k).start()
            row_copy(h, k).start()

    def far_rows(h):
        if h == 0:
            greet_far()
        for k in far:
            if h == 0:
                idx_copy_to(k).start()
            row_copy(h, k).start()

    def load_factors():
        down_copy.start()
        up_copy.start()
        res_copy.start()

    stages = {
        "project": project, "settle": settle, "place": place_rows, "near": near_rows,
        "far": far_rows, "greet": greet_chips, "meet": meet_chips, "factors": load_factors,
        "shrink": shrink_rows, "sum": sum_send, "expand": expand_rows,
        "first": send_first, "on": send_on, "long": send_long, "requests": requests,
    }
    for name, *at in ORDER:
        if name in ("first", "on", "long"):
            if at[2] >= pieces:
                continue
        elif name in ("project", "settle"):
            if at[1] >= len(steps):
                continue
        elif at and at[0] >= halves:
            continue
        with scope(name + "_".join(str(v) for v in at)):
            stages[name](*at)
    for turn in range(last_chip):
        for q in range(pieces):
            for core in range(2):
                send_first(core, turn, q)
                send_long(core, turn, q)
                send_on(core, turn, q)

    res_copy.wait()

    def branch_of(h, q, n):
        slot_col = slot_of(rank_col, own_col, h)
        unplace = jnp.where(
            lax.broadcasted_iota(jnp.int32, (rows, slots), 1) == slot_col, 1.0, 0.0
        ).astype(BF16)
        first = q * piece + n * tile
        back = eback[h, :, :, first:first + tile].reshape(slots, tile)
        return jnp.dot(unplace, back, preferred_element_type=F32)

    for h in range(halves):
        with scope("backwait%d" % h):
            back_wait(h)
        for q in range(pieces):
            for n in range(tiles):
                cols = slice(n * tile, (n + 1) * tile)
                first = q * piece + n * tile
                value = own[z * pieces + q, :, cols] + branch_of(h, q, n)
                if h == 0:
                    value = (
                        value + precv[z * pieces + q, :, cols].astype(F32)
                        + rbuf[:, first:first + tile].astype(F32)
                    )
                own[z * pieces + q, :, cols] = value

    for q in range(pieces):
        mine_at = z * pieces + q
        mark = scope("fin%d" % q)
        mark.__enter__()

        def finish(use_right, use_left):
            @pl.loop(0, rows // strip)
            def _(n):
                at = pl.ds(pl.multiple_of(n * strip, strip), strip)
                value = own[mine_at, at]
                if use_right:
                    value = value + rrecv[mine_at, at].astype(F32)
                if use_left:
                    value = value + lrecv[mine_at, at].astype(F32)
                out_ref[at, q * piece:(q + 1) * piece] = value.astype(BF16)

        if chips == 1:
            finish(False, False)
        else:
            @pl.when(z == 0)
            def _():
                left(z, q, z).wait_recv()
                finish(False, True)

            @pl.when(z == chips - 1)
            def _():
                right(z, q, z).wait_recv()
                finish(True, False)

            @pl.when((z > 0) & (z < chips - 1))
            def _():
                right(z, q, z).wait_recv()
                left(z, q, z).wait_recv()
                finish(True, True)
        mark.__exit__(None, None, None)

    tail = scope("tail")
    tail.__enter__()
    all_of(psend, precv, ps_sem.at[0], ps_sem.at[0]).wait_send()

    @pl.when(c == 0)
    def _():
        all_of(packed, arp, as_sem.at[0], as_sem.at[0]).wait_send()

    @pl.when(c == 1)
    def _():
        all_of(arz, arz, zs_sem.at[0], zs_sem.at[0]).wait_send()
        if chips > 1:
            far_chips = pl.ds(0, chips - 1)
            all_of(
                arz.at[:, far_chips], arz.at[:, far_chips], zs_sem.at[0], zs_sem.at[0]
            ).wait_send()

    if groups > 1:
        all_of(
            xsend.at[:, others], xrecv.at[:, others], xs_sem.at[0], xs_sem.at[0]
        ).wait_send()
        all_of(
            esend.at[:, others], eback.at[:, others], es_sem.at[0], es_sem.at[0]
        ).wait_send()
        all_of(idx_all.at[others], idx_all.at[others], is_sem.at[0], is_sem.at[0]).wait_send()
    for chip in range(chips):
        @pl.when(z == chip)
        def _():
            if chip < last_chip:
                sent = pl.ds(0, (last_chip - chip) * pieces)
                all_of(
                    rsend.at[sent], rrecv.at[sent], rs_sem.at[0], rs_sem.at[0]
                ).wait_send()
            if chip > 0:
                sent = pl.ds(0, chip * pieces)
                all_of(
                    lsend.at[sent], lrecv.at[sent], ls_sem.at[0], ls_sem.at[0]
                ).wait_send()
    tail.__exit__(None, None, None)


def body(attention_output, residual, output_weight, down_factors, up_factors, adapter_index):
    groups = lax.axis_size("dp")
    members = lax.axis_size("tensor")
    rows, depth = attention_output.shape
    owned, _, rank = down_factors.shape
    width = output_weight.shape[1] // members
    cap = 2 * rows // groups
    chips = members // 2
    halves = 2 if cap % 32 == 0 else 1
    part = cap // halves
    slots = groups * part
    pieces = max(1, min(PIECES, width // 256))
    piece = width // pieces
    down = jnp.swapaxes(down_factors, 1, 2).reshape(owned * rank, depth)
    up = up_factors.reshape(owned * rank, width)
    vmem = pl.BlockSpec(memory_space=pltpu.VMEM)
    hbm = pl.BlockSpec(memory_space=pl.ANY)
    dma = pltpu.SemaphoreType.DMA
    hops = chips * pieces
    return pl.pallas_call(
        functools.partial(kernel, groups, members, rank, owned, halves, pieces),
        out_shape=pltpu.VMEM((rows, width), BF16),
        in_specs=[hbm] * 6,
        out_specs=vmem,
        scratch_shapes=[
            pltpu.VMEM((rows, depth), BF16),
            pltpu.VMEM((1, rows), jnp.int32),
            pltpu.VMEM((groups, 1, rows), jnp.int32),
            pltpu.VMEM((members, depth, width), BF16),
            pltpu.VMEM((owned * rank, depth), BF16),
            pltpu.VMEM((owned * rank, width), BF16),
            pltpu.VMEM((rows, width), BF16),
            pltpu.VMEM((hops, rows, piece), F32),
            pltpu.VMEM((hops, rows, piece), BF16),
            pltpu.VMEM((hops, rows, piece), BF16),
            pltpu.VMEM((hops, rows, piece), BF16),
            pltpu.VMEM((hops, rows, piece), BF16),
            pltpu.VMEM((hops, rows, piece), BF16),
            pltpu.VMEM((hops, rows, piece), BF16),
            pltpu.VMEM((halves, groups, part, depth), BF16),
            pltpu.VMEM((halves, groups, part, depth), BF16),
            pltpu.VMEM((halves, slots, LANES), F32),
            pltpu.VMEM((halves, rank, slots), F32),
            pltpu.VMEM((halves, rank, slots), F32),
            pltpu.VMEM((halves, chips, rank, slots), F32),
            pltpu.VMEM((halves, groups, part, width), BF16),
            pltpu.VMEM((halves, groups, part, width), BF16),
            dma((AHEAD,)), dma((3,)), dma((1,)), dma((hops,)),
            dma((1,)), dma((1,)), dma((hops + pieces,)),
            dma((1,)), dma((halves,)), dma((1,)), dma((halves,)),
            dma((1,)), dma((halves,)), dma((1,)), dma((halves,)),
            pltpu.SemaphoreType.REGULAR((max(1, groups.bit_length() - 2),)),
            pltpu.SemaphoreType.REGULAR((2,)),
            dma((1,)), dma((1,)),
        ],
        compiler_params=pltpu.CompilerParams(
            collective_id=0, has_side_effects=True, vmem_limit_bytes=60 * 1024 * 1024
        ),
    )(attention_output, residual, adapter_index.reshape(1, rows), output_weight, down, up)


def solution(mesh):
    return jax.shard_map(
        body,
        mesh=mesh,
        in_specs=(
            P("dp", "tensor"),
            P("dp", "tensor"),
            P("tensor", None),
            P("dp", "tensor", None),
            P("dp", None, "tensor"),
            P("dp"),
        ),
        out_specs=P("dp", "tensor"),
        check_vma=False,
    )
```

```python
import contextlib
import functools

import jax
import jax.numpy as jnp
from jax import lax
from jax.experimental import pallas as pl
from jax.experimental.pallas import tpu as pltpu
from jax.sharding import PartitionSpec as P

MESH = pl.DeviceIdType.MESH
F32 = jnp.float32
BF16 = jnp.bfloat16
LANES = 128
PIECES = 4
AHEAD = 4
FIRST = 2
HELD = 2
ORDER = (
    ("near", 0), ("project", 0, 0), ("project", 0, 1), ("project", 0, 2), ("settle", 0, 0),
    ("far", 0), ("project", 0, 3), ("settle", 0, 1), ("place", 1), ("factors",),
    ("project", 0, 4), ("settle", 0, 2), ("project", 0, 5), ("settle", 0, 3),
    ("far", 1), ("near", 1),
    ("project", 1, 0), ("project", 0, 6), ("settle", 0, 4), ("greet",), ("project", 0, 7),
    ("settle", 0, 5), ("settle", 0, 6), ("settle", 0, 7),
    ("relay", 0, 2, 0), ("relay", 0, 2, 1), ("relay", 0, 2, 2), ("relay", 0, 2, 3),
    ("requests",), ("relay", 0, 1, 0), ("relay", 0, 1, 1),
    ("shrink", 0), ("settle", 1, 0), ("first", 1, 0, 0), ("first", 0, 2, 0), ("first", 0, 2, 1),
    ("relay", 0, 1, 2), ("relay", 0, 1, 3),
    ("project", 1, 1), ("low", 0, 0), ("low", 0, 1), ("project", 1, 2),
    ("meet",), ("sum", 0), ("project", 1, 3),
    ("first", 1, 0, 1), ("settle", 1, 1), ("first", 1, 0, 2),
    ("shrink", 1), ("project", 1, 4), ("sum", 1),
    ("low", 0, 2), ("low", 0, 3), ("first", 1, 0, 3), ("project", 1, 5),
    ("relay", 1, 1, 0), ("project", 1, 6), ("project", 1, 7),
    ("settle", 1, 2), ("settle", 1, 3),
    ("first", 1, 1, 0), ("first", 1, 1, 1), ("first", 1, 1, 2), ("first", 1, 1, 3),
    ("settle", 1, 4), ("settle", 1, 5),
    ("first", 1, 2, 0), ("first", 1, 2, 1), ("first", 1, 2, 2), ("first", 1, 2, 3),
    ("settle", 1, 6), ("settle", 1, 7),
    ("expand", 0), ("high", 0, 0), ("high", 0, 1), ("high", 0, 2), ("high", 0, 3),
    ("relay", 1, 1, 1), ("relay", 1, 1, 2),
    ("relay", 1, 2, 0), ("relay", 1, 2, 1), ("relay", 1, 2, 2), ("relay", 1, 2, 3),
    ("expand", 1), ("relay", 1, 1, 3), ("first", 0, 2, 2), ("first", 0, 2, 3),
    ("low", 1, 0), ("high", 1, 0), ("low", 1, 1), ("high", 1, 1),
    ("low", 1, 2), ("high", 1, 2), ("low", 1, 3), ("high", 1, 3),
)
scope = contextlib.nullcontext


def kernel(
    groups, members, rank, owned, halves, pieces,
    x_hbm, res_ref, idx_hbm, w_ref, down_ref, up_ref, out_ref,
    x_ref, idx_ref, idx_all, wbuf, dbuf, ubuf, rbuf, own, psend, precv, rrecv, lrecv, rsend, lsend, jrecv, klrecv,
    xsend, xrecv, wants, packed, arp, arz, esend, eback,
    w_sem, d_sem, ps_sem, pr_sem, rs_sem, ls_sem, hr_sem, j_sem,
    xs_sem, xr_sem, as_sem, ar_sem, zs_sem, zr_sem, es_sem, er_sem, dp_sem, z_sem, is_sem, ir_sem,
):
    chips = members // 2
    g = lax.axis_index("dp")
    t = lax.axis_index("tensor")
    z = t // 2
    c = lax.rem(t, 2)
    partner = z * 2 + (1 - c)
    rows, depth = x_ref.shape
    width = out_ref.shape[1]
    part = xrecv.shape[2]
    slots = groups * part
    low = z < chips // 2
    high = jnp.logical_not(low)
    piece = width // pieces
    last_chip = chips - 1
    wave = 2 if pieces % 2 == 0 else 1

    def core_of(chip):
        return (g, chip * 2 + c)

    bits = groups.bit_length() - 1
    cube = groups == 1 << bits

    def peer(k):
        if not cube:
            return lax.rem(g + k, groups)
        to = g
        for b in range(bits):
            if k >> b & 1:
                to = to + (1 << b) * (1 - 2 * lax.rem(g // (1 << b), 2))
        return to

    def source_of(k):
        return peer(k) if cube else lax.rem(g + groups - k, groups)

    near = [1 << b for b in range(bits)] if cube else list(range(1, groups))
    far = [k for k in range(1, groups) if k not in near]
    rounds = bits - 1 if far else 0

    barrier = pltpu.get_barrier_semaphore()
    pl.semaphore_signal(barrier, inc=1, device_id=(g, partner), device_id_type=MESH)

    @pl.when(z > 0)
    def _():
        pl.semaphore_signal(barrier, inc=1, device_id=core_of(z - 1), device_id_type=MESH)

    @pl.when(z < last_chip)
    def _():
        pl.semaphore_signal(barrier, inc=1, device_id=core_of(z + 1), device_id_type=MESH)

    for k in near:
        pl.semaphore_signal(barrier, inc=1, device_id=(peer(k), t), device_id_type=MESH)

    def block_chip(i):
        return jnp.where(low, chips - 1 - i, i)

    blocks = [(n, 0, width) for n in range(members)]
    if pieces % 2 == 0:
        blocks[:1] = [(0, p * width // 2, width // 2) for p in range(2)]
    chunks = len(blocks)
    loaded = set()

    def weight_copy(j):
        n, offset, size = blocks[j]
        column = block_chip(n % chips) * 2 + n // chips
        start = pl.multiple_of(column * width + offset, LANES)
        return pltpu.make_async_copy(
            w_ref.at[:, pl.ds(start, size)], wbuf.at[n, :, pl.ds(offset, size)],
            w_sem.at[j % AHEAD],
        )

    def weights(n, column):
        for j in range(chunks):
            if j not in loaded and blocks[j][:2] <= (n, column) and blocks[j][0] == n:
                weight_copy(j).wait()
                loaded.add(j)
                if j + AHEAD < chunks:
                    weight_copy(j + AHEAD).start()

    down_copy = pltpu.make_async_copy(down_ref, dbuf, d_sem.at[0])
    up_copy = pltpu.make_async_copy(up_ref, ubuf, d_sem.at[1])
    res_copy = pltpu.make_async_copy(res_ref, rbuf, d_sem.at[2])
    x_copy = pltpu.make_async_copy(x_hbm, x_ref, d_sem.at[0])
    idx_copy = pltpu.make_async_copy(idx_hbm, idx_ref, d_sem.at[1])
    idx_copy.start()
    x_copy.start()
    for j in range(min(FIRST, chunks)):
        weight_copy(j).start()

    def enter():
        near_chips = jnp.where(z > 0, 1, 0) + jnp.where(z < last_chip, 1, 0)
        pl.semaphore_wait(barrier, 1 + len(near) + near_chips)

    def tell(b):
        pl.semaphore_signal(
            dp_sem.at[b], inc=1, device_id=(peer(1 << b), t), device_id_type=MESH
        )

    def tell_chip(n, to):
        pl.semaphore_signal(z_sem.at[n], inc=1, device_id=core_of(to), device_id_type=MESH)

    def greet_far():
        for b in range(rounds):
            pl.semaphore_wait(dp_sem.at[b], 1)
            if b + 1 < rounds:
                tell(b + 1)

    def greet_ends():
        if chips < 3:
            return

        @pl.when(z == 0)
        def _():
            tell_chip(0, z + 1)

        @pl.when(z == last_chip)
        def _():
            tell_chip(1, z - 1)

    def greet_chips():
        if chips < 3:
            return

        @pl.when((z > 0) & low)
        def _():
            pl.semaphore_wait(z_sem.at[0], 1)
            tell_chip(0, z + 1)
            pl.semaphore_wait(z_sem.at[1], 1)
            tell_chip(1, z - 1)

        @pl.when((z < last_chip) & jnp.logical_not(low))
        def _():
            pl.semaphore_wait(z_sem.at[1], 1)
            tell_chip(1, z - 1)
            pl.semaphore_wait(z_sem.at[0], 1)
            tell_chip(0, z + 1)

    def meet_chips():
        if chips < 3:
            return

        @pl.when(z == 0)
        def _():
            pl.semaphore_wait(z_sem.at[1], 1)

        @pl.when(z == last_chip)
        def _():
            pl.semaphore_wait(z_sem.at[0], 1)

    idx_copy.wait()
    for j in range(FIRST, min(AHEAD, chunks)):
        weight_copy(j).start()
    idx_row = idx_ref[...]
    r_i = lax.broadcasted_iota(jnp.int32, (rows, rows), 0)
    c_i = lax.broadcasted_iota(jnp.int32, (rows, rows), 1)
    idx_full = jnp.broadcast_to(idx_row, (rows, rows))
    idx_col = jnp.sum(jnp.where(r_i == c_i, idx_full, 0), axis=1, keepdims=True)
    own_row = idx_row // owned
    own_col = idx_col // owned
    same = own_col == own_row
    rank_row = jnp.sum(jnp.where(same & (r_i < c_i), 1, 0), axis=0, keepdims=True)
    rank_col = jnp.sum(jnp.where(same & (c_i < r_i), 1, 0), axis=1, keepdims=True)

    def slot_of(place_rank, owner, h):
        inside = place_rank - h * part
        keep = (inside >= 0) & (inside < part)
        return jnp.where(keep, owner * part + inside, -1)

    step = min(256, depth)

    def row_copy(h, k):
        to = peer(k)
        return pltpu.make_async_remote_copy(
            src_ref=xsend.at[h, to], dst_ref=xrecv.at[h, g],
            send_sem=xs_sem.at[0], recv_sem=xr_sem.at[h],
            device_id=(to, t), device_id_type=MESH,
        )

    others = pl.ds(0, groups - 1)

    def all_of(send, recv, send_sem, recv_sem):
        return pltpu.make_async_remote_copy(
            src_ref=send, dst_ref=recv, send_sem=send_sem, recv_sem=recv_sem,
            device_id=(g, partner), device_id_type=MESH,
        )

    def idx_copy_to(k):
        return pltpu.make_async_remote_copy(
            src_ref=idx_ref, dst_ref=idx_all.at[g], send_sem=is_sem.at[0],
            recv_sem=ir_sem.at[0], device_id=(peer(k), t), device_id_type=MESH,
        )

    def requests():
        idx_all[g] = idx_ref[...]
        if groups > 1:
            all_of(
                idx_all.at[others], idx_all.at[others], is_sem.at[0], ir_sem.at[0]
            ).wait_recv()
        every_row = jnp.concatenate([idx_all[k] for k in range(groups)], axis=0)
        chosen = every_row // owned == g
        earlier = jnp.where(r_i < c_i, 1.0, 0.0).astype(BF16)
        ahead = jnp.dot(
            jnp.where(chosen, 1.0, 0.0).astype(BF16), earlier, preferred_element_type=F32
        ).astype(jnp.int32)
        slot = jnp.where(chosen, ahead, -1)
        number = lax.rem(every_row, owned) + 1
        for h in range(halves):
            for k in range(groups):
                place = lax.broadcasted_iota(jnp.int32, (part, rows), 0) + h * part
                asked = jnp.where(place == slot[k:k + 1], number[k:k + 1], 0)
                wants[h, k * part:(k + 1) * part] = jnp.broadcast_to(
                    jnp.sum(asked, axis=1, keepdims=True).astype(F32), (part, LANES)
                )

    def rows_wait(h):
        all_of(
            xsend.at[h, others], xrecv.at[h, others], xs_sem.at[0], xr_sem.at[h]
        ).wait_recv()

    def place_rows(h):
        slot_row = slot_of(rank_row, own_row, h)
        placing = lax.broadcasted_iota(jnp.int32, (slots, rows), 0) == slot_row
        place = jnp.where(placing, 1.0, 0.0).astype(BF16)
        for j in range(depth // step):
            moved = jnp.dot(
                place, x_ref[:, j * step:(j + 1) * step], preferred_element_type=F32
            ).astype(BF16)
            for k in range(groups):
                xsend[h, k, :, j * step:(j + 1) * step] = moved[k * part:(k + 1) * part]
        xrecv[h, g] = xsend[h, g]

    tile = min(256, piece)
    tiles = piece // tile

    def pair_copy(chip, q):
        k = chip * pieces + q
        return pltpu.make_async_remote_copy(
            src_ref=psend.at[k], dst_ref=precv.at[k], send_sem=ps_sem.at[0],
            recv_sem=pr_sem.at[chip * (pieces // wave) + q // wave],
            device_id=(g, partner), device_id_type=MESH,
        )

    strip = 16

    sent = set()

    def leaps(core, b):
        return chips > 2 and b in (0, last_chip)

    def hop(core, a, b, q):
        k = b * pieces + q
        to_right = b > a
        jump = leaps(core, b) and abs(b - a) == 2
        to = b if jump else (a + 1 if to_right else a - 1)
        if jump:
            landing = (jrecv if to_right else klrecv).at[q]
            arrival = j_sem.at[q + (0 if to_right else pieces)]
        else:
            landing = (rrecv if to_right else lrecv).at[k]
            arrival = hr_sem.at[k + (pieces if to_right else 0)]
        return pltpu.make_async_remote_copy(
            src_ref=(rsend if to_right else lsend).at[k], dst_ref=landing,
            send_sem=(rs_sem if to_right else ls_sem).at[0], recv_sem=arrival,
            device_id=(g, to * 2 + c), device_id_type=MESH,
        ), landing

    def send(core, a, b, q):
        if (core, a, b, q) in sent:
            return
        sent.add((core, a, b, q))
        before = a - 1 if b > a else a + 1
        joins = 0 <= before < chips and not (leaps(core, b) and abs(b - a) == 1)

        @pl.when((c == core) & (z == a))
        def _():
            k = b * pieces + q
            if joins:
                copy, landed = hop(core, before, b, q)
                copy.wait_recv()
            out = rsend if b > a else lsend

            @pl.loop(0, rows // strip)
            def _(n):
                at = pl.ds(pl.multiple_of(n * strip, strip), strip)
                value = own[k, at] + precv[k, at].astype(F32)
                if joins:
                    value = value + landed[at].astype(F32)
                out[k, at] = value.astype(BF16)

            hop(core, a, b, q)[0].start()

    def send_first(core, turn, q):
        if turn < last_chip:
            send(core, 0, last_chip - turn, q)
            send(core, last_chip, turn, q)

    def send_relay(core, d, q):
        if 0 < d < last_chip:
            send(core, d, last_chip, q)
            send(core, last_chip - d, 0, q)

    def send_low(core, q):
        if chips > 3:
            send(core, 1, 2, q)

    def send_high(core, q):
        if chips > 3:
            send(core, last_chip - 1, last_chip - 2, q)

    steps = [(i, q) for i in range(chips) for q in range(0, pieces, wave)]

    def product(n, q, into, k):
        for m in range(tiles * wave):
            at = q * piece + m * tile
            into[k + m // tiles, :, m % tiles * tile:(m % tiles + 1) * tile] = jnp.dot(
                x_ref[...], wbuf[n, :, at:at + tile], preferred_element_type=F32
            ).astype(into.dtype)

    def project(phase, n):
        i, q = steps[n]
        block = phase * chips + i
        k = block_chip(i) * pieces + q
        weights(block, q * piece)

        @pl.when(c == phase)
        def _():
            product(block, q, own, k)

        @pl.when(c != phase)
        def _():
            product(block, q, psend, k)
            send_other(n)

    def send_other(n):
        i, q = steps[n]
        for p in range(wave):
            pair_copy(block_chip(i), q + p).start()

    def settle(phase, n):
        i, first = steps[n]
        both = pl.ds(block_chip(i) * pieces + first, wave)

        @pl.when(c == phase)
        def _():
            all_of(
                psend.at[both], precv.at[both], ps_sem.at[0],
                pr_sem.at[block_chip(i) * (pieces // wave) + first // wave],
            ).wait_recv()

        if phase == 0 and i < HELD:
            for q in range(first, first + wave):
                send_first(0, i, q)

    lane_number = (lax.broadcasted_iota(jnp.int32, (slots, LANES), 1) // rank + 1).astype(F32)
    per_tile = LANES // rank
    tile_count = owned * rank // LANES
    chunk = min(512, owned * rank)

    def term_pair(h):
        return pltpu.make_async_remote_copy(
            src_ref=packed.at[h], dst_ref=arp.at[h], send_sem=as_sem.at[0],
            recv_sem=ar_sem.at[h], device_id=(g, partner), device_id_type=MESH,
        )

    def term_copy(h, k, core):
        to = lax.rem(z + jnp.where(low, chips - k, k), chips)
        return pltpu.make_async_remote_copy(
            src_ref=arz.at[h, z], dst_ref=arz.at[h, z], send_sem=zs_sem.at[0],
            recv_sem=zr_sem.at[h], device_id=(g, to * 2 + core), device_id_type=MESH,
        )

    def terms_wait(h):
        @pl.when(c == 0)
        def _():
            all_of(arz.at[h], arz.at[h], zs_sem.at[0], zr_sem.at[h]).wait_recv()

        if chips > 1:
            @pl.when(c == 1)
            def _():
                far_chips = pl.ds(0, chips - 1)
                all_of(
                    arz.at[h, far_chips], arz.at[h, far_chips], zs_sem.at[0], zr_sem.at[h]
                ).wait_recv()

    def wanted_of(h):
        return wants[h]

    def shrink_rows(h):
        rows_wait(h)
        if h == 0:
            down_copy.wait()
        wanted = wanted_of(h).T[:rank]
        flat = xrecv[h].reshape(slots, depth)
        mine = jnp.zeros((rank, slots), F32)
        for first in range(0, owned * rank, chunk):
            every = lax.dot_general(
                dbuf[first:first + chunk, :], flat, (((1,), (1,)), ((), ())),
                preferred_element_type=F32,
            )
            for p in range(chunk // rank):
                number = float(first // rank + p + 1)
                mine = jnp.where(wanted == number, every[p * rank:(p + 1) * rank], mine)
        packed[h] = mine

        @pl.when(c == 0)
        def _():
            term_pair(h).start()

    def sum_send(h):
        @pl.when(c == 1)
        def _():
            term_pair(h).wait_recv()
            arz[h, z] = (packed[h] + arp[h]).astype(BF16)
            term_copy(h, 0, 0).start()
            for k in range(1, chips):
                for core in range(2):
                    term_copy(h, k, core).start()

    def back_copy(h, k):
        to = peer(k)
        return pltpu.make_async_remote_copy(
            src_ref=esend.at[h, to], dst_ref=eback.at[h, g],
            send_sem=es_sem.at[0], recv_sem=er_sem.at[h],
            device_id=(to, t), device_id_type=MESH,
        )

    def back_wait(h):
        all_of(
            esend.at[h, others], eback.at[h, others], es_sem.at[0], er_sem.at[h]
        ).wait_recv()

    wide = min(512, width)

    def expand_rows(h):
        terms_wait(h)
        total = arz[h, 0].astype(F32)
        for k in range(1, chips):
            total = total + arz[h, k].astype(F32)
        total = total.astype(BF16).astype(F32)
        if h == 0:
            up_copy.wait()
        wanted = wanted_of(h)
        shrink = jnp.concatenate([total] * per_tile, axis=0).T
        spread = jnp.concatenate(
            [
                jnp.where(wanted == lane_number + float(m * per_tile), shrink, 0.0).astype(BF16)
                for m in range(tile_count)
            ],
            axis=1,
        )

        @pl.loop(0, width // wide)
        def _(n):
            cols = pl.ds(pl.multiple_of(n * wide, LANES), wide)
            grown = jnp.dot(spread, ubuf[:, cols], preferred_element_type=F32).astype(BF16)
            for k in range(groups):
                esend[h, k, :, cols] = grown[k * part:(k + 1) * part]

        for k in far + near:
            back_copy(h, k).start()
        eback[h, g] = esend[h, g]

    with scope("x"):
        x_copy.wait()
    with scope("place0"):
        place_rows(0)
    with scope("enter"):
        enter()
    if rounds:
        tell(0)
    greet_ends()

    def near_rows(h):
        for k in near:
            if h == 0:
                idx_copy_to(k).start()
            row_copy(h, k).start()

    def far_rows(h):
        if h == 0:
            greet_far()
        for k in far:
            if h == 0:
                idx_copy_to(k).start()
            row_copy(h, k).start()

    def load_factors():
        down_copy.start()
        up_copy.start()
        res_copy.start()

    stages = {
        "project": project, "settle": settle, "place": place_rows, "near": near_rows,
        "far": far_rows, "greet": greet_chips, "meet": meet_chips, "factors": load_factors,
        "shrink": shrink_rows, "sum": sum_send, "expand": expand_rows,
        "first": send_first, "relay": send_relay, "low": send_low, "high": send_high, "requests": requests,
    }
    for name, *at in ORDER:
        if name in ("first", "relay", "low", "high"):
            if at[-1] >= pieces:
                continue
        elif name in ("project", "settle"):
            if at[1] >= len(steps):
                continue
        elif at and at[0] >= halves:
            continue
        with scope(name + "_".join(str(v) for v in at)):
            stages[name](*at)
    for b in range(chips):
        for a in list(range(b)) + list(range(last_chip, b, -1)):
            for core in range(2):
                for q in range(pieces):
                    send(core, a, b, q)

    res_copy.wait()

    def branch_of(h, q, n):
        slot_col = slot_of(rank_col, own_col, h)
        unplace = jnp.where(
            lax.broadcasted_iota(jnp.int32, (rows, slots), 1) == slot_col, 1.0, 0.0
        ).astype(BF16)
        first = q * piece + n * tile
        back = eback[h, :, :, first:first + tile].reshape(slots, tile)
        return jnp.dot(unplace, back, preferred_element_type=F32)

    def close(core, q, into):
        for a in range(chips):
            @pl.when((c == core) & (z == a))
            def _():
                landed = []
                for step in (1, 2):
                    for source in (a - step, a + step):
                        if 0 <= source < chips and (step == 1 or leaps(core, a)):
                            copy, ref = hop(core, source, a, q)
                            copy.wait_recv()
                            landed.append(ref)

                @pl.loop(0, rows // strip)
                def _(n):
                    at = pl.ds(pl.multiple_of(n * strip, strip), strip)
                    value = own[a * pieces + q, at]
                    for ref in landed:
                        value = value + ref[at].astype(F32)
                    if into is own:
                        own[a * pieces + q, at] = value
                    else:
                        out_ref[at, q * piece:(q + 1) * piece] = value.astype(BF16)

    with scope("close0"):
        for q in range(pieces):
            close(0, q, own)

    for h in range(halves):
        with scope("backwait%d" % h):
            back_wait(h)
        for q in range(pieces):
            for n in range(tiles):
                cols = slice(n * tile, (n + 1) * tile)
                first = q * piece + n * tile
                value = own[z * pieces + q, :, cols] + branch_of(h, q, n)
                if h == 0:
                    value = (
                        value + precv[z * pieces + q, :, cols].astype(F32)
                        + rbuf[:, first:first + tile].astype(F32)
                    )
                own[z * pieces + q, :, cols] = value
                if h == halves - 1:
                    out_ref[:, first:first + tile] = value.astype(BF16)

    for q in range(pieces):
        with scope("fin%d" % q):
            close(1, q, out_ref)

    tail = scope("tail")
    tail.__enter__()
    all_of(psend, precv, ps_sem.at[0], ps_sem.at[0]).wait_send()

    @pl.when(c == 0)
    def _():
        all_of(packed, arp, as_sem.at[0], as_sem.at[0]).wait_send()

    @pl.when(c == 1)
    def _():
        all_of(arz, arz, zs_sem.at[0], zs_sem.at[0]).wait_send()
        if chips > 1:
            far_chips = pl.ds(0, chips - 1)
            all_of(
                arz.at[:, far_chips], arz.at[:, far_chips], zs_sem.at[0], zs_sem.at[0]
            ).wait_send()

    if groups > 1:
        all_of(
            xsend.at[:, others], xrecv.at[:, others], xs_sem.at[0], xs_sem.at[0]
        ).wait_send()
        all_of(
            esend.at[:, others], eback.at[:, others], es_sem.at[0], es_sem.at[0]
        ).wait_send()
        all_of(idx_all.at[others], idx_all.at[others], is_sem.at[0], is_sem.at[0]).wait_send()
    for chip in range(chips):
        @pl.when(z == chip)
        def _():
            if chip < last_chip:
                sent = pl.ds(0, (last_chip - chip) * pieces)
                all_of(
                    rsend.at[sent], rrecv.at[sent], rs_sem.at[0], rs_sem.at[0]
                ).wait_send()
            if chip > 0:
                sent = pl.ds(0, chip * pieces)
                all_of(
                    lsend.at[sent], lrecv.at[sent], ls_sem.at[0], ls_sem.at[0]
                ).wait_send()
    tail.__exit__(None, None, None)


def body(attention_output, residual, output_weight, down_factors, up_factors, adapter_index):
    groups = lax.axis_size("dp")
    members = lax.axis_size("tensor")
    rows, depth = attention_output.shape
    owned, _, rank = down_factors.shape
    width = output_weight.shape[1] // members
    cap = 2 * rows // groups
    chips = members // 2
    halves = 2 if cap % 32 == 0 else 1
    part = cap // halves
    slots = groups * part
    pieces = max(1, min(PIECES, width // 256))
    piece = width // pieces
    down = jnp.swapaxes(down_factors, 1, 2).reshape(owned * rank, depth)
    up = up_factors.reshape(owned * rank, width)
    vmem = pl.BlockSpec(memory_space=pltpu.VMEM)
    hbm = pl.BlockSpec(memory_space=pl.ANY)
    dma = pltpu.SemaphoreType.DMA
    hops = chips * pieces
    return pl.pallas_call(
        functools.partial(kernel, groups, members, rank, owned, halves, pieces),
        out_shape=pltpu.VMEM((rows, width), BF16),
        in_specs=[hbm] * 6,
        out_specs=vmem,
        scratch_shapes=[
            pltpu.VMEM((rows, depth), BF16),
            pltpu.VMEM((1, rows), jnp.int32),
            pltpu.VMEM((groups, 1, rows), jnp.int32),
            pltpu.VMEM((members, depth, width), BF16),
            pltpu.VMEM((owned * rank, depth), BF16),
            pltpu.VMEM((owned * rank, width), BF16),
            pltpu.VMEM((rows, width), BF16),
            pltpu.VMEM((hops, rows, piece), F32),
            pltpu.VMEM((hops, rows, piece), BF16),
            pltpu.VMEM((hops, rows, piece), BF16),
            pltpu.VMEM((hops, rows, piece), BF16),
            pltpu.VMEM((hops, rows, piece), BF16),
            pltpu.VMEM((hops, rows, piece), BF16),
            pltpu.VMEM((hops, rows, piece), BF16),
            pltpu.VMEM((pieces, rows, piece), BF16),
            pltpu.VMEM((pieces, rows, piece), BF16),
            pltpu.VMEM((halves, groups, part, depth), BF16),
            pltpu.VMEM((halves, groups, part, depth), BF16),
            pltpu.VMEM((halves, slots, LANES), F32),
            pltpu.VMEM((halves, rank, slots), F32),
            pltpu.VMEM((halves, rank, slots), F32),
            pltpu.VMEM((halves, chips, rank, slots), BF16),
            pltpu.VMEM((halves, groups, part, width), BF16),
            pltpu.VMEM((halves, groups, part, width), BF16),
            dma((AHEAD,)), dma((3,)), dma((1,)), dma((hops // (2 if pieces % 2 == 0 else 1),)),
            dma((1,)), dma((1,)), dma((hops + pieces,)), dma((2 * pieces,)),
            dma((1,)), dma((halves,)), dma((1,)), dma((halves,)),
            dma((1,)), dma((halves,)), dma((1,)), dma((halves,)),
            pltpu.SemaphoreType.REGULAR((max(1, groups.bit_length() - 2),)),
            pltpu.SemaphoreType.REGULAR((2,)),
            dma((1,)), dma((1,)),
        ],
        compiler_params=pltpu.CompilerParams(
            collective_id=0, has_side_effects=True, vmem_limit_bytes=60 * 1024 * 1024
        ),
    )(attention_output, residual, adapter_index.reshape(1, rows), output_weight, down, up)


def solution(mesh):
    return jax.shard_map(
        body,
        mesh=mesh,
        in_specs=(
            P("dp", "tensor"),
            P("dp", "tensor"),
            P("tensor", None),
            P("dp", "tensor", None),
            P("dp", None, "tensor"),
            P("dp"),
        ),
        out_specs=P("dp", "tensor"),
        check_vma=False,
    )
```

```python
import contextlib
import functools

import jax
import jax.numpy as jnp
from jax import lax
from jax.experimental import pallas as pl
from jax.experimental.pallas import tpu as pltpu
from jax.sharding import PartitionSpec as P

MESH = pl.DeviceIdType.MESH
F32 = jnp.float32
BF16 = jnp.bfloat16
LANES = 128
PIECES = 4
AHEAD = 4
FIRST = 2
HELD = 2
ORDER = (
    ("near", 0), ("project", 0, 0), ("project", 0, 1), ("project", 0, 2), ("settle", 0, 0),
    ("far", 0), ("project", 0, 3), ("settle", 0, 1), ("place", 1), ("factors",),
    ("project", 0, 4), ("settle", 0, 2), ("project", 0, 5), ("settle", 0, 3), ("far", 1),
    ("near", 1), ("project", 1, 0), ("project", 0, 6), ("settle", 0, 4), ("greet",),
    ("project", 0, 7), ("settle", 0, 5), ("settle", 0, 6), ("settle", 0, 7), ("relay", 0, 2, 0),
    ("relay", 0, 2, 1), ("relay", 0, 2, 2), ("relay", 0, 2, 3), ("requests",), ("relay", 0, 1, 0),
    ("relay", 0, 1, 1), ("shrink", 0), ("settle", 1, 0), ("first", 1, 0, 0), ("first", 0, 2, 0),
    ("first", 0, 2, 1), ("relay", 0, 1, 2), ("relay", 0, 1, 3), ("project", 1, 1), ("low", 0, 0),
    ("low", 0, 1), ("project", 1, 2), ("meet",), ("sum", 0), ("project", 1, 3), ("settle", 1, 1),
    ("first", 1, 0, 1), ("first", 1, 0, 2), ("shrink", 1), ("project", 1, 4), ("high", 0, 0),
    ("high", 0, 1), ("sum", 1), ("low", 0, 2), ("low", 0, 3), ("first", 1, 0, 3),
    ("settle", 1, 2), ("first", 1, 1, 0), ("first", 1, 1, 1), ("settle", 1, 3), ("project", 1, 5),
    ("relay", 1, 1, 0), ("project", 1, 6), ("project", 1, 7), ("high", 0, 2), ("high", 0, 3),
    ("first", 1, 1, 2), ("first", 1, 1, 3), ("settle", 1, 4), ("settle", 1, 5),
    ("first", 1, 2, 0), ("first", 1, 2, 1), ("first", 1, 2, 2), ("first", 1, 2, 3),
    ("settle", 1, 6), ("settle", 1, 7), ("expand", 0), ("relay", 1, 1, 1), ("relay", 1, 1, 2),
    ("relay", 1, 2, 0), ("relay", 1, 2, 1), ("relay", 1, 2, 2), ("relay", 1, 2, 3), ("expand", 1),
    ("relay", 1, 1, 3), ("first", 0, 2, 2), ("first", 0, 2, 3), ("low", 1, 0), ("high", 1, 0),
    ("low", 1, 1), ("high", 1, 1), ("low", 1, 2), ("high", 1, 2), ("low", 1, 3), ("high", 1, 3),
)
scope = contextlib.nullcontext


def kernel(
    groups, members, rank, owned, halves, pieces,
    x_hbm, res_ref, idx_hbm, w_ref, down_ref, up_ref, out_ref,
    x_ref, idx_ref, idx_all, wbuf, dbuf, ubuf, rbuf, own, psend, precv, rrecv, lrecv, rsend, lsend, jrecv, klrecv,
    xsend, xrecv, wants, packed, arp, arz, esend, eback,
    w_sem, d_sem, ps_sem, pr_sem, rs_sem, ls_sem, hr_sem, j_sem,
    xs_sem, xr_sem, as_sem, ar_sem, zs_sem, zr_sem, es_sem, er_sem, dp_sem, z_sem, is_sem, ir_sem,
):
    chips = members // 2
    g = lax.axis_index("dp")
    t = lax.axis_index("tensor")
    z = t // 2
    c = lax.rem(t, 2)
    partner = z * 2 + (1 - c)
    rows, depth = x_ref.shape
    width = out_ref.shape[1]
    part = xrecv.shape[2]
    slots = groups * part
    low = z < chips // 2
    high = jnp.logical_not(low)
    piece = width // pieces
    last_chip = chips - 1
    wave = 2 if pieces % 2 == 0 else 1

    def core_of(chip):
        return (g, chip * 2 + c)

    bits = groups.bit_length() - 1
    cube = groups == 1 << bits

    def peer(k):
        if not cube:
            return lax.rem(g + k, groups)
        to = g
        for b in range(bits):
            if k >> b & 1:
                to = to + (1 << b) * (1 - 2 * lax.rem(g // (1 << b), 2))
        return to

    def source_of(k):
        return peer(k) if cube else lax.rem(g + groups - k, groups)

    near = [1 << b for b in range(bits)] if cube else list(range(1, groups))
    far = [k for k in range(1, groups) if k not in near]
    rounds = bits - 1 if far else 0

    barrier = pltpu.get_barrier_semaphore()
    pl.semaphore_signal(barrier, inc=1, device_id=(g, partner), device_id_type=MESH)

    @pl.when(z > 0)
    def _():
        pl.semaphore_signal(barrier, inc=1, device_id=core_of(z - 1), device_id_type=MESH)

    @pl.when(z < last_chip)
    def _():
        pl.semaphore_signal(barrier, inc=1, device_id=core_of(z + 1), device_id_type=MESH)

    for k in near:
        pl.semaphore_signal(barrier, inc=1, device_id=(peer(k), t), device_id_type=MESH)

    def block_chip(i):
        return jnp.where(low, chips - 1 - i, i)

    blocks = [(n, 0, width) for n in range(members)]
    if pieces % 2 == 0:
        blocks[:1] = [(0, p * width // 2, width // 2) for p in range(2)]
    chunks = len(blocks)
    loaded = set()

    def weight_copy(j):
        n, offset, size = blocks[j]
        column = block_chip(n % chips) * 2 + n // chips
        start = pl.multiple_of(column * width + offset, LANES)
        return pltpu.make_async_copy(
            w_ref.at[:, pl.ds(start, size)], wbuf.at[n, :, pl.ds(offset, size)],
            w_sem.at[j % AHEAD],
        )

    def weights(n, column):
        for j in range(chunks):
            if j not in loaded and blocks[j][:2] <= (n, column) and blocks[j][0] == n:
                weight_copy(j).wait()
                loaded.add(j)
                if j + AHEAD < chunks:
                    weight_copy(j + AHEAD).start()

    down_copy = pltpu.make_async_copy(down_ref, dbuf, d_sem.at[0])
    up_copy = pltpu.make_async_copy(up_ref, ubuf, d_sem.at[1])
    res_copy = pltpu.make_async_copy(res_ref, rbuf, d_sem.at[2])
    x_copy = pltpu.make_async_copy(x_hbm, x_ref, d_sem.at[0])
    idx_copy = pltpu.make_async_copy(idx_hbm, idx_ref, d_sem.at[1])
    idx_copy.start()
    x_copy.start()
    for j in range(min(FIRST, chunks)):
        weight_copy(j).start()

    def enter():
        near_chips = jnp.where(z > 0, 1, 0) + jnp.where(z < last_chip, 1, 0)
        pl.semaphore_wait(barrier, 1 + len(near) + near_chips)

    def tell(b):
        pl.semaphore_signal(
            dp_sem.at[b], inc=1, device_id=(peer(1 << b), t), device_id_type=MESH
        )

    def tell_chip(n, to):
        pl.semaphore_signal(z_sem.at[n], inc=1, device_id=core_of(to), device_id_type=MESH)

    def greet_far():
        for b in range(rounds):
            pl.semaphore_wait(dp_sem.at[b], 1)
            if b + 1 < rounds:
                tell(b + 1)

    def greet_ends():
        if chips < 3:
            return

        @pl.when(z == 0)
        def _():
            tell_chip(0, z + 1)

        @pl.when(z == last_chip)
        def _():
            tell_chip(1, z - 1)

    def greet_chips():
        if chips < 3:
            return

        @pl.when((z > 0) & low)
        def _():
            pl.semaphore_wait(z_sem.at[0], 1)
            tell_chip(0, z + 1)
            pl.semaphore_wait(z_sem.at[1], 1)
            tell_chip(1, z - 1)

        @pl.when((z < last_chip) & jnp.logical_not(low))
        def _():
            pl.semaphore_wait(z_sem.at[1], 1)
            tell_chip(1, z - 1)
            pl.semaphore_wait(z_sem.at[0], 1)
            tell_chip(0, z + 1)

    def meet_chips():
        if chips < 3:
            return

        @pl.when(z == 0)
        def _():
            pl.semaphore_wait(z_sem.at[1], 1)

        @pl.when(z == last_chip)
        def _():
            pl.semaphore_wait(z_sem.at[0], 1)

    idx_copy.wait()
    for j in range(FIRST, min(AHEAD, chunks)):
        weight_copy(j).start()
    idx_row = idx_ref[...]
    r_i = lax.broadcasted_iota(jnp.int32, (rows, rows), 0)
    c_i = lax.broadcasted_iota(jnp.int32, (rows, rows), 1)
    idx_full = jnp.broadcast_to(idx_row, (rows, rows))
    idx_col = jnp.sum(jnp.where(r_i == c_i, idx_full, 0), axis=1, keepdims=True)
    own_row = idx_row // owned
    own_col = idx_col // owned
    same = own_col == own_row
    rank_row = jnp.sum(jnp.where(same & (r_i < c_i), 1, 0), axis=0, keepdims=True)
    rank_col = jnp.sum(jnp.where(same & (c_i < r_i), 1, 0), axis=1, keepdims=True)

    def slot_of(place_rank, owner, h):
        inside = place_rank - h * part
        keep = (inside >= 0) & (inside < part)
        return jnp.where(keep, owner * part + inside, -1)

    step = min(256, depth)

    def row_copy(h, k):
        to = peer(k)
        return pltpu.make_async_remote_copy(
            src_ref=xsend.at[h, to], dst_ref=xrecv.at[h, g],
            send_sem=xs_sem.at[0], recv_sem=xr_sem.at[h],
            device_id=(to, t), device_id_type=MESH,
        )

    others = pl.ds(0, groups - 1)

    def all_of(send, recv, send_sem, recv_sem):
        return pltpu.make_async_remote_copy(
            src_ref=send, dst_ref=recv, send_sem=send_sem, recv_sem=recv_sem,
            device_id=(g, partner), device_id_type=MESH,
        )

    def idx_copy_to(k):
        return pltpu.make_async_remote_copy(
            src_ref=idx_ref, dst_ref=idx_all.at[g], send_sem=is_sem.at[0],
            recv_sem=ir_sem.at[0], device_id=(peer(k), t), device_id_type=MESH,
        )

    def requests():
        idx_all[g] = idx_ref[...]
        if groups > 1:
            all_of(
                idx_all.at[others], idx_all.at[others], is_sem.at[0], ir_sem.at[0]
            ).wait_recv()
        every_row = jnp.concatenate([idx_all[k] for k in range(groups)], axis=0)
        chosen = every_row // owned == g
        earlier = jnp.where(r_i < c_i, 1.0, 0.0).astype(BF16)
        ahead = jnp.dot(
            jnp.where(chosen, 1.0, 0.0).astype(BF16), earlier, preferred_element_type=F32
        ).astype(jnp.int32)
        slot = jnp.where(chosen, ahead, -1)
        number = lax.rem(every_row, owned) + 1
        for h in range(halves):
            for k in range(groups):
                place = lax.broadcasted_iota(jnp.int32, (part, rows), 0) + h * part
                asked = jnp.where(place == slot[k:k + 1], number[k:k + 1], 0)
                wants[h, k * part:(k + 1) * part] = jnp.broadcast_to(
                    jnp.sum(asked, axis=1, keepdims=True).astype(F32), (part, LANES)
                )

    def rows_wait(h):
        all_of(
            xsend.at[h, others], xrecv.at[h, others], xs_sem.at[0], xr_sem.at[h]
        ).wait_recv()

    def place_rows(h):
        slot_row = slot_of(rank_row, own_row, h)
        placing = lax.broadcasted_iota(jnp.int32, (slots, rows), 0) == slot_row
        place = jnp.where(placing, 1.0, 0.0).astype(BF16)
        for j in range(depth // step):
            moved = jnp.dot(
                place, x_ref[:, j * step:(j + 1) * step], preferred_element_type=F32
            ).astype(BF16)
            for k in range(groups):
                xsend[h, k, :, j * step:(j + 1) * step] = moved[k * part:(k + 1) * part]
        xrecv[h, g] = xsend[h, g]

    tile = min(256, piece)
    tiles = piece // tile

    def pair_copy(chip, q):
        k = chip * pieces + q
        return pltpu.make_async_remote_copy(
            src_ref=psend.at[k], dst_ref=precv.at[k], send_sem=ps_sem.at[0],
            recv_sem=pr_sem.at[chip * (pieces // wave) + q // wave],
            device_id=(g, partner), device_id_type=MESH,
        )

    strip = 16

    sent = set()

    def leaps(core, b):
        return chips > 2 and b in (0, last_chip)

    def hop(core, a, b, q):
        k = b * pieces + q
        to_right = b > a
        jump = leaps(core, b) and abs(b - a) == 2
        to = b if jump else (a + 1 if to_right else a - 1)
        if jump:
            landing = (jrecv if to_right else klrecv).at[q]
            arrival = j_sem.at[q + (0 if to_right else pieces)]
        else:
            landing = (rrecv if to_right else lrecv).at[k]
            arrival = hr_sem.at[k + (pieces if to_right else 0)]
        return pltpu.make_async_remote_copy(
            src_ref=(rsend if to_right else lsend).at[k], dst_ref=landing,
            send_sem=(rs_sem if to_right else ls_sem).at[0], recv_sem=arrival,
            device_id=(g, to * 2 + c), device_id_type=MESH,
        ), landing

    def send(core, a, b, q):
        if (core, a, b, q) in sent:
            return
        sent.add((core, a, b, q))
        before = a - 1 if b > a else a + 1
        joins = 0 <= before < chips and not (leaps(core, b) and abs(b - a) == 1)

        @pl.when((c == core) & (z == a))
        def _():
            k = b * pieces + q
            if joins:
                copy, landed = hop(core, before, b, q)
                copy.wait_recv()
            out = rsend if b > a else lsend

            @pl.loop(0, rows // strip)
            def _(n):
                at = pl.ds(pl.multiple_of(n * strip, strip), strip)
                value = own[k, at] + precv[k, at].astype(F32)
                if joins:
                    value = value + landed[at].astype(F32)
                out[k, at] = value.astype(BF16)

            hop(core, a, b, q)[0].start()

    def send_first(core, turn, q):
        if turn < last_chip:
            send(core, 0, last_chip - turn, q)
            send(core, last_chip, turn, q)

    def send_relay(core, d, q):
        if 0 < d < last_chip:
            send(core, d, last_chip, q)
            send(core, last_chip - d, 0, q)

    def send_low(core, q):
        if chips > 3:
            send(core, 1, 2, q)

    def send_high(core, q):
        if chips > 3:
            send(core, last_chip - 1, last_chip - 2, q)

    steps = [(i, q) for i in range(chips) for q in range(0, pieces, wave)]

    def product(n, q, into, k):
        for m in range(tiles * wave):
            at = q * piece + m * tile
            into[k + m // tiles, :, m % tiles * tile:(m % tiles + 1) * tile] = jnp.dot(
                x_ref[...], wbuf[n, :, at:at + tile], preferred_element_type=F32
            ).astype(into.dtype)

    def project(phase, n):
        if phase + n == 0:
            @pl.when(c == 0)
            def _():
                product(0, 0, own, first_at)

            return
        i, q = steps[n]
        block = phase * chips + i
        k = block_chip(i) * pieces + q
        weights(block, q * piece)

        @pl.when(c == phase)
        def _():
            product(block, q, own, k)

        @pl.when(c != phase)
        def _():
            product(block, q, psend, k)
            send_other(n)

    def send_other(n):
        i, q = steps[n]
        for p in range(wave):
            pair_copy(block_chip(i), q + p).start()

    def settle(phase, n):
        i, first = steps[n]
        both = pl.ds(block_chip(i) * pieces + first, wave)

        @pl.when(c == phase)
        def _():
            all_of(
                psend.at[both], precv.at[both], ps_sem.at[0],
                pr_sem.at[block_chip(i) * (pieces // wave) + first // wave],
            ).wait_recv()

        if phase == 0 and i < HELD:
            for q in range(first, first + wave):
                send_first(0, i, q)

    lane_number = (lax.broadcasted_iota(jnp.int32, (slots, LANES), 1) // rank + 1).astype(F32)
    per_tile = LANES // rank
    tile_count = owned * rank // LANES
    chunk = min(512, owned * rank)

    def term_pair(h):
        return pltpu.make_async_remote_copy(
            src_ref=packed.at[h], dst_ref=arp.at[h], send_sem=as_sem.at[0],
            recv_sem=ar_sem.at[h], device_id=(g, partner), device_id_type=MESH,
        )

    def term_copy(h, k, core):
        to = lax.rem(z + jnp.where(low, chips - k, k), chips)
        return pltpu.make_async_remote_copy(
            src_ref=arz.at[h, z], dst_ref=arz.at[h, z], send_sem=zs_sem.at[0],
            recv_sem=zr_sem.at[h], device_id=(g, to * 2 + core), device_id_type=MESH,
        )

    def terms_wait(h):
        @pl.when(c == 0)
        def _():
            all_of(arz.at[h], arz.at[h], zs_sem.at[0], zr_sem.at[h]).wait_recv()

        if chips > 1:
            @pl.when(c == 1)
            def _():
                far_chips = pl.ds(0, chips - 1)
                all_of(
                    arz.at[h, far_chips], arz.at[h, far_chips], zs_sem.at[0], zr_sem.at[h]
                ).wait_recv()

    def wanted_of(h):
        return wants[h]

    def shrink_rows(h):
        rows_wait(h)
        if h == 0:
            down_copy.wait()
        wanted = wanted_of(h).T[:rank]
        flat = xrecv[h].reshape(slots, depth)
        mine = jnp.zeros((rank, slots), F32)
        for first in range(0, owned * rank, chunk):
            every = lax.dot_general(
                dbuf[first:first + chunk, :], flat, (((1,), (1,)), ((), ())),
                preferred_element_type=F32,
            )
            for p in range(chunk // rank):
                number = float(first // rank + p + 1)
                mine = jnp.where(wanted == number, every[p * rank:(p + 1) * rank], mine)
        packed[h] = mine

        @pl.when(c == 0)
        def _():
            term_pair(h).start()

    def sum_send(h):
        @pl.when(c == 1)
        def _():
            term_pair(h).wait_recv()
            arz[h, z] = (packed[h] + arp[h]).astype(BF16)
            term_copy(h, 0, 0).start()
            for k in range(1, chips):
                for core in range(2):
                    term_copy(h, k, core).start()

    def back_copy(h, k, cols):
        to = peer(k)
        return pltpu.make_async_remote_copy(
            src_ref=esend.at[h, to, :, cols], dst_ref=eback.at[h, g, :, cols],
            send_sem=es_sem.at[0], recv_sem=er_sem.at[h],
            device_id=(to, t), device_id_type=MESH,
        )

    def back_wait(h):
        all_of(
            esend.at[h, others], eback.at[h, others], es_sem.at[0], er_sem.at[h]
        ).wait_recv()

    wide = min(512, width)

    def expand_rows(h):
        terms_wait(h)
        total = arz[h, 0].astype(F32)
        for k in range(1, chips):
            total = total + arz[h, k].astype(F32)
        total = total.astype(BF16).astype(F32)
        if h == 0:
            up_copy.wait()
        wanted = wanted_of(h)
        shrink = jnp.concatenate([total] * per_tile, axis=0).T
        spread = jnp.concatenate(
            [
                jnp.where(wanted == lane_number + float(m * per_tile), shrink, 0.0).astype(BF16)
                for m in range(tile_count)
            ],
            axis=1,
        )

        for n in range(width // wide):
            cols = pl.ds(n * wide, wide)
            grown = jnp.dot(
                spread, ubuf[:, n * wide:(n + 1) * wide], preferred_element_type=F32
            ).astype(BF16)
            for k in range(groups):
                esend[h, k, :, cols] = grown[k * part:(k + 1) * part]
            for k in far + near:
                back_copy(h, k, cols).start()
        eback[h, g] = esend[h, g]

    with scope("x"):
        x_copy.wait()
    first_at = block_chip(0) * pieces
    weights(0, 0)

    @pl.when(c == 1)
    def _():
        product(0, 0, psend, first_at)

    with scope("enter"):
        enter()

    @pl.when(c == 1)
    def _():
        send_other(0)

    with scope("place0"):
        place_rows(0)
    if rounds:
        tell(0)
    greet_ends()

    def near_rows(h):
        for k in near:
            if h == 0:
                idx_copy_to(k).start()
            row_copy(h, k).start()

    def far_rows(h):
        if h == 0:
            greet_far()
        for k in far:
            if h == 0:
                idx_copy_to(k).start()
            row_copy(h, k).start()

    def load_factors():
        down_copy.start()
        up_copy.start()
        res_copy.start()

    stages = {
        "project": project, "settle": settle, "place": place_rows, "near": near_rows,
        "far": far_rows, "greet": greet_chips, "meet": meet_chips, "factors": load_factors,
        "shrink": shrink_rows, "sum": sum_send, "expand": expand_rows,
        "first": send_first, "relay": send_relay, "low": send_low, "high": send_high, "requests": requests,
    }
    for name, *at in ORDER:
        if name in ("first", "relay", "low", "high"):
            if at[-1] >= pieces:
                continue
        elif name in ("project", "settle"):
            if at[1] >= len(steps):
                continue
        elif at and at[0] >= halves:
            continue
        with scope(name + "_".join(str(v) for v in at)):
            stages[name](*at)
    for b in range(chips):
        for a in list(range(b)) + list(range(last_chip, b, -1)):
            for core in range(2):
                for q in range(pieces):
                    send(core, a, b, q)

    res_copy.wait()

    def branch_of(h, q, n):
        slot_col = slot_of(rank_col, own_col, h)
        unplace = jnp.where(
            lax.broadcasted_iota(jnp.int32, (rows, slots), 1) == slot_col, 1.0, 0.0
        ).astype(BF16)
        first = q * piece + n * tile
        back = eback[h, :, :, first:first + tile].reshape(slots, tile)
        return jnp.dot(unplace, back, preferred_element_type=F32)

    def close(core, q, into):
        for a in range(chips):
            @pl.when((c == core) & (z == a))
            def _():
                landed = []
                for step in (1, 2):
                    for source in (a - step, a + step):
                        if 0 <= source < chips and (step == 1 or leaps(core, a)):
                            copy, ref = hop(core, source, a, q)
                            copy.wait_recv()
                            landed.append(ref)

                @pl.loop(0, rows // strip)
                def _(n):
                    at = pl.ds(pl.multiple_of(n * strip, strip), strip)
                    value = own[a * pieces + q, at]
                    for ref in landed:
                        value = value + ref[at].astype(F32)
                    if into is own:
                        own[a * pieces + q, at] = value
                    else:
                        out_ref[at, q * piece:(q + 1) * piece] = value.astype(BF16)

    with scope("close0"):
        for q in range(pieces):
            close(0, q, own)

    for h in range(halves):
        with scope("backwait%d" % h):
            back_wait(h)
        for q in range(pieces):
            for n in range(tiles):
                cols = slice(n * tile, (n + 1) * tile)
                first = q * piece + n * tile
                value = own[z * pieces + q, :, cols] + branch_of(h, q, n)
                if h == 0:
                    value = (
                        value + precv[z * pieces + q, :, cols].astype(F32)
                        + rbuf[:, first:first + tile].astype(F32)
                    )
                own[z * pieces + q, :, cols] = value
                if h == halves - 1:
                    out_ref[:, first:first + tile] = value.astype(BF16)

    for q in range(pieces):
        with scope("fin%d" % q):
            close(1, q, out_ref)

    tail = scope("tail")
    tail.__enter__()
    all_of(psend, precv, ps_sem.at[0], ps_sem.at[0]).wait_send()

    @pl.when(c == 0)
    def _():
        all_of(packed, arp, as_sem.at[0], as_sem.at[0]).wait_send()

    @pl.when(c == 1)
    def _():
        all_of(arz, arz, zs_sem.at[0], zs_sem.at[0]).wait_send()
        if chips > 1:
            far_chips = pl.ds(0, chips - 1)
            all_of(
                arz.at[:, far_chips], arz.at[:, far_chips], zs_sem.at[0], zs_sem.at[0]
            ).wait_send()

    if groups > 1:
        all_of(
            xsend.at[:, others], xrecv.at[:, others], xs_sem.at[0], xs_sem.at[0]
        ).wait_send()
        all_of(
            esend.at[:, others], eback.at[:, others], es_sem.at[0], es_sem.at[0]
        ).wait_send()
        all_of(idx_all.at[others], idx_all.at[others], is_sem.at[0], is_sem.at[0]).wait_send()
    for chip in range(chips):
        @pl.when(z == chip)
        def _():
            if chip < last_chip:
                sent = pl.ds(0, (last_chip - chip) * pieces)
                all_of(
                    rsend.at[sent], rrecv.at[sent], rs_sem.at[0], rs_sem.at[0]
                ).wait_send()
            if chip > 0:
                sent = pl.ds(0, chip * pieces)
                all_of(
                    lsend.at[sent], lrecv.at[sent], ls_sem.at[0], ls_sem.at[0]
                ).wait_send()
    tail.__exit__(None, None, None)


def body(attention_output, residual, output_weight, down_factors, up_factors, adapter_index):
    groups = lax.axis_size("dp")
    members = lax.axis_size("tensor")
    rows, depth = attention_output.shape
    owned, _, rank = down_factors.shape
    width = output_weight.shape[1] // members
    cap = 2 * rows // groups
    chips = members // 2
    halves = 2 if cap % 32 == 0 else 1
    part = cap // halves
    slots = groups * part
    pieces = max(1, min(PIECES, width // 256))
    piece = width // pieces
    down = jnp.swapaxes(down_factors, 1, 2).reshape(owned * rank, depth)
    up = up_factors.reshape(owned * rank, width)
    vmem = pl.BlockSpec(memory_space=pltpu.VMEM)
    hbm = pl.BlockSpec(memory_space=pl.ANY)
    dma = pltpu.SemaphoreType.DMA
    hops = chips * pieces
    return pl.pallas_call(
        functools.partial(kernel, groups, members, rank, owned, halves, pieces),
        out_shape=pltpu.VMEM((rows, width), BF16),
        in_specs=[hbm] * 6,
        out_specs=vmem,
        scratch_shapes=[
            pltpu.VMEM((rows, depth), BF16),
            pltpu.VMEM((1, rows), jnp.int32),
            pltpu.VMEM((groups, 1, rows), jnp.int32),
            pltpu.VMEM((members, depth, width), BF16),
            pltpu.VMEM((owned * rank, depth), BF16),
            pltpu.VMEM((owned * rank, width), BF16),
            pltpu.VMEM((rows, width), BF16),
            pltpu.VMEM((hops, rows, piece), F32),
            pltpu.VMEM((hops, rows, piece), BF16),
            pltpu.VMEM((hops, rows, piece), BF16),
            pltpu.VMEM((hops, rows, piece), BF16),
            pltpu.VMEM((hops, rows, piece), BF16),
            pltpu.VMEM((hops, rows, piece), BF16),
            pltpu.VMEM((hops, rows, piece), BF16),
            pltpu.VMEM((pieces, rows, piece), BF16),
            pltpu.VMEM((pieces, rows, piece), BF16),
            pltpu.VMEM((halves, groups, part, depth), BF16),
            pltpu.VMEM((halves, groups, part, depth), BF16),
            pltpu.VMEM((halves, slots, LANES), F32),
            pltpu.VMEM((halves, rank, slots), F32),
            pltpu.VMEM((halves, rank, slots), F32),
            pltpu.VMEM((halves, chips, rank, slots), BF16),
            pltpu.VMEM((halves, groups, part, width), BF16),
            pltpu.VMEM((halves, groups, part, width), BF16),
            dma((AHEAD,)), dma((3,)), dma((1,)), dma((hops // (2 if pieces % 2 == 0 else 1),)),
            dma((1,)), dma((1,)), dma((hops + pieces,)), dma((2 * pieces,)),
            dma((1,)), dma((halves,)), dma((1,)), dma((halves,)),
            dma((1,)), dma((halves,)), dma((1,)), dma((halves,)),
            pltpu.SemaphoreType.REGULAR((max(1, groups.bit_length() - 2),)),
            pltpu.SemaphoreType.REGULAR((2,)),
            dma((1,)), dma((1,)),
        ],
        compiler_params=pltpu.CompilerParams(
            collective_id=0, has_side_effects=True, vmem_limit_bytes=60 * 1024 * 1024
        ),
    )(attention_output, residual, adapter_index.reshape(1, rows), output_weight, down, up)


def solution(mesh):
    return jax.shard_map(
        body,
        mesh=mesh,
        in_specs=(
            P("dp", "tensor"),
            P("dp", "tensor"),
            P("tensor", None),
            P("dp", "tensor", None),
            P("dp", None, "tensor"),
            P("dp"),
        ),
        out_specs=P("dp", "tensor"),
        check_vma=False,
    )
```

```python
import contextlib
import functools

import jax
import jax.numpy as jnp
from jax import lax
from jax.experimental import pallas as pl
from jax.experimental.pallas import tpu as pltpu
from jax.sharding import PartitionSpec as P

MESH = pl.DeviceIdType.MESH
F32 = jnp.float32
BF16 = jnp.bfloat16
LANES = 128
PIECES = 4
AHEAD = 4
FIRST = 2
HELD = 2
ORDER = (
    ("near", 0), ("project", 0, 0), ("project", 0, 1), ("project", 0, 2), ("settle", 0, 0),
    ("far", 0), ("project", 0, 3), ("settle", 0, 1), ("place", 1), ("factors",),
    ("project", 0, 4), ("settle", 0, 2), ("project", 0, 5), ("settle", 0, 3), ("far", 1),
    ("near", 1), ("project", 1, 0), ("project", 0, 6), ("settle", 0, 4), ("greet",),
    ("project", 0, 7), ("settle", 0, 5), ("settle", 0, 6), ("settle", 0, 7), ("relay", 0, 2, 0),
    ("relay", 0, 2, 1), ("relay", 0, 2, 2), ("relay", 0, 2, 3), ("requests",), ("relay", 0, 1, 0),
    ("relay", 0, 1, 1), ("shrink", 0), ("settle", 1, 0), ("first", 1, 0, 0), ("first", 0, 2, 0),
    ("first", 0, 2, 1), ("relay", 0, 1, 2), ("relay", 0, 1, 3), ("project", 1, 1), ("low", 0, 0),
    ("low", 0, 1), ("project", 1, 2), ("meet",), ("sum", 0), ("project", 1, 3), ("settle", 1, 1),
    ("first", 1, 0, 1), ("first", 1, 0, 2), ("shrink", 1), ("project", 1, 4), ("high", 0, 0),
    ("high", 0, 1), ("sum", 1), ("low", 0, 2), ("low", 0, 3), ("first", 1, 0, 3),
    ("settle", 1, 2), ("first", 1, 1, 0), ("first", 1, 1, 1), ("settle", 1, 3), ("project", 1, 5),
    ("relay", 1, 1, 0), ("project", 1, 6), ("project", 1, 7), ("high", 0, 2), ("high", 0, 3),
    ("first", 1, 1, 2), ("first", 1, 1, 3), ("settle", 1, 4), ("settle", 1, 5),
    ("first", 1, 2, 0), ("first", 1, 2, 1), ("first", 1, 2, 2), ("first", 1, 2, 3),
    ("settle", 1, 6), ("settle", 1, 7), ("expand", 0), ("relay", 1, 1, 1), ("relay", 1, 1, 2),
    ("relay", 1, 2, 0), ("relay", 1, 2, 1), ("relay", 1, 2, 2), ("relay", 1, 2, 3), ("expand", 1),
    ("relay", 1, 1, 3), ("first", 0, 2, 2), ("first", 0, 2, 3), ("low", 1, 0), ("high", 1, 0),
    ("low", 1, 1), ("high", 1, 1), ("low", 1, 2), ("high", 1, 2), ("low", 1, 3), ("high", 1, 3),
)
scope = contextlib.nullcontext


def kernel(
    groups, members, rank, owned, halves, pieces,
    x_hbm, res_ref, idx_hbm, w_ref, down_ref, up_ref, out_ref,
    x_ref, idx_ref, idx_all, wbuf, dbuf, ubuf, rbuf, own, psend, precv, rrecv, lrecv, rsend, lsend, jrecv,
    xsend, xrecv, wants, packed, arp, arz, esend, eback,
    w_sem, d_sem, ps_sem, pr_sem, rs_sem, ls_sem, hr_sem, j_sem,
    xs_sem, xr_sem, as_sem, ar_sem, zs_sem, zr_sem, es_sem, er_sem, dp_sem, z_sem, is_sem, ir_sem,
):
    chips = members // 2
    g = lax.axis_index("dp")
    t = lax.axis_index("tensor")
    z = t // 2
    c = lax.rem(t, 2)
    partner = z * 2 + (1 - c)
    rows, depth = x_ref.shape
    width = out_ref.shape[1]
    part = xrecv.shape[2]
    slots = groups * part
    low = z < chips // 2
    high = jnp.logical_not(low)
    piece = width // pieces
    last_chip = chips - 1
    wave = 2 if pieces % 2 == 0 else 1

    def core_of(chip):
        return (g, chip * 2 + c)

    bits = groups.bit_length() - 1
    cube = groups == 1 << bits

    def peer(k):
        if not cube:
            return lax.rem(g + k, groups)
        to = g
        for b in range(bits):
            if k >> b & 1:
                to = to + (1 << b) * (1 - 2 * lax.rem(g // (1 << b), 2))
        return to

    def source_of(k):
        return peer(k) if cube else lax.rem(g + groups - k, groups)

    near = [1 << b for b in range(bits)] if cube else list(range(1, groups))
    far = [k for k in range(1, groups) if k not in near]
    rounds = bits - 1 if far else 0

    barrier = pltpu.get_barrier_semaphore()
    pl.semaphore_signal(barrier, inc=1, device_id=(g, partner), device_id_type=MESH)

    @pl.when(z > 0)
    def _():
        pl.semaphore_signal(barrier, inc=1, device_id=core_of(z - 1), device_id_type=MESH)

    @pl.when(z < last_chip)
    def _():
        pl.semaphore_signal(barrier, inc=1, device_id=core_of(z + 1), device_id_type=MESH)

    for k in near:
        pl.semaphore_signal(barrier, inc=1, device_id=(peer(k), t), device_id_type=MESH)

    def block_chip(i):
        return jnp.where(low, chips - 1 - i, i)

    blocks = [(n, 0, width) for n in range(members)]
    if pieces % 2 == 0:
        blocks[:1] = [(0, p * width // 2, width // 2) for p in range(2)]
    chunks = len(blocks)
    loaded = set()

    def weight_copy(j):
        n, offset, size = blocks[j]
        column = block_chip(n % chips) * 2 + n // chips
        start = pl.multiple_of(column * width + offset, LANES)
        return pltpu.make_async_copy(
            w_ref.at[:, pl.ds(start, size)], wbuf.at[n, :, pl.ds(offset, size)],
            w_sem.at[j % AHEAD],
        )

    def weights(n, column):
        for j in range(chunks):
            if j not in loaded and blocks[j][:2] <= (n, column) and blocks[j][0] == n:
                weight_copy(j).wait()
                loaded.add(j)
                if j + AHEAD < chunks:
                    weight_copy(j + AHEAD).start()

    down_copy = pltpu.make_async_copy(down_ref, dbuf, d_sem.at[0])
    up_copy = pltpu.make_async_copy(up_ref, ubuf, d_sem.at[1])
    res_copy = pltpu.make_async_copy(res_ref, rbuf, d_sem.at[2])
    x_copy = pltpu.make_async_copy(x_hbm, x_ref, d_sem.at[0])
    idx_copy = pltpu.make_async_copy(idx_hbm, idx_ref, d_sem.at[1])
    idx_copy.start()
    x_copy.start()
    for j in range(min(FIRST, chunks)):
        weight_copy(j).start()

    def enter():
        near_chips = jnp.where(z > 0, 1, 0) + jnp.where(z < last_chip, 1, 0)
        pl.semaphore_wait(barrier, 1 + len(near) + near_chips)

    def tell(b):
        pl.semaphore_signal(
            dp_sem.at[b], inc=1, device_id=(peer(1 << b), t), device_id_type=MESH
        )

    def tell_chip(n, to):
        pl.semaphore_signal(z_sem.at[n], inc=1, device_id=core_of(to), device_id_type=MESH)

    def greet_far():
        for b in range(rounds):
            pl.semaphore_wait(dp_sem.at[b], 1)
            if b + 1 < rounds:
                tell(b + 1)

    def greet_ends():
        if chips < 3:
            return

        @pl.when(z == 0)
        def _():
            tell_chip(0, z + 1)

        @pl.when(z == last_chip)
        def _():
            tell_chip(1, z - 1)

    def greet_chips():
        if chips < 3:
            return

        @pl.when((z > 0) & low)
        def _():
            pl.semaphore_wait(z_sem.at[0], 1)
            tell_chip(0, z + 1)
            pl.semaphore_wait(z_sem.at[1], 1)
            tell_chip(1, z - 1)

        @pl.when((z < last_chip) & jnp.logical_not(low))
        def _():
            pl.semaphore_wait(z_sem.at[1], 1)
            tell_chip(1, z - 1)
            pl.semaphore_wait(z_sem.at[0], 1)
            tell_chip(0, z + 1)

    def meet_chips():
        if chips < 3:
            return

        @pl.when(z == 0)
        def _():
            pl.semaphore_wait(z_sem.at[1], 1)

        @pl.when(z == last_chip)
        def _():
            pl.semaphore_wait(z_sem.at[0], 1)

    idx_copy.wait()
    for j in range(FIRST, min(AHEAD, chunks)):
        weight_copy(j).start()
    idx_row = idx_ref[...]
    r_i = lax.broadcasted_iota(jnp.int32, (rows, rows), 0)
    c_i = lax.broadcasted_iota(jnp.int32, (rows, rows), 1)
    idx_full = jnp.broadcast_to(idx_row, (rows, rows))
    idx_col = jnp.sum(jnp.where(r_i == c_i, idx_full, 0), axis=1, keepdims=True)
    own_row = idx_row // owned
    own_col = idx_col // owned
    same = own_col == own_row
    rank_row = jnp.sum(jnp.where(same & (r_i < c_i), 1, 0), axis=0, keepdims=True)
    rank_col = jnp.sum(jnp.where(same & (c_i < r_i), 1, 0), axis=1, keepdims=True)

    def slot_of(place_rank, owner, h):
        inside = place_rank - h * part
        keep = (inside >= 0) & (inside < part)
        return jnp.where(keep, owner * part + inside, -1)

    step = min(256, depth)

    def row_copy(h, k):
        to = peer(k)
        return pltpu.make_async_remote_copy(
            src_ref=xsend.at[h, to], dst_ref=xrecv.at[h, g],
            send_sem=xs_sem.at[0], recv_sem=xr_sem.at[h],
            device_id=(to, t), device_id_type=MESH,
        )

    others = pl.ds(0, groups - 1)

    def all_of(send, recv, send_sem, recv_sem):
        return pltpu.make_async_remote_copy(
            src_ref=send, dst_ref=recv, send_sem=send_sem, recv_sem=recv_sem,
            device_id=(g, partner), device_id_type=MESH,
        )

    def idx_copy_to(k):
        return pltpu.make_async_remote_copy(
            src_ref=idx_ref, dst_ref=idx_all.at[g], send_sem=is_sem.at[0],
            recv_sem=ir_sem.at[0], device_id=(peer(k), t), device_id_type=MESH,
        )

    def requests():
        idx_all[g] = idx_ref[...]
        if groups > 1:
            all_of(
                idx_all.at[others], idx_all.at[others], is_sem.at[0], ir_sem.at[0]
            ).wait_recv()
        every_row = jnp.concatenate([idx_all[k] for k in range(groups)], axis=0)
        chosen = every_row // owned == g
        earlier = jnp.where(r_i < c_i, 1.0, 0.0).astype(BF16)
        ahead = jnp.dot(
            jnp.where(chosen, 1.0, 0.0).astype(BF16), earlier, preferred_element_type=F32
        ).astype(jnp.int32)
        slot = jnp.where(chosen, ahead, -1)
        number = lax.rem(every_row, owned) + 1
        for h in range(halves):
            for k in range(groups):
                place = lax.broadcasted_iota(jnp.int32, (part, rows), 0) + h * part
                asked = jnp.where(place == slot[k:k + 1], number[k:k + 1], 0)
                wants[h, k * part:(k + 1) * part] = jnp.broadcast_to(
                    jnp.sum(asked, axis=1, keepdims=True).astype(F32), (part, LANES)
                )

    def rows_wait(h):
        all_of(
            xsend.at[h, others], xrecv.at[h, others], xs_sem.at[0], xr_sem.at[h]
        ).wait_recv()

    def place_rows(h):
        slot_row = slot_of(rank_row, own_row, h)
        placing = lax.broadcasted_iota(jnp.int32, (slots, rows), 0) == slot_row
        place = jnp.where(placing, 1.0, 0.0).astype(BF16)
        for j in range(depth // step):
            moved = jnp.dot(
                place, x_ref[:, j * step:(j + 1) * step], preferred_element_type=F32
            ).astype(BF16)
            for k in range(groups):
                xsend[h, k, :, j * step:(j + 1) * step] = moved[k * part:(k + 1) * part]
        xrecv[h, g] = xsend[h, g]

    tile = min(256, piece)
    tiles = piece // tile

    def pair_copy(chip, q):
        k = chip * pieces + q
        return pltpu.make_async_remote_copy(
            src_ref=psend.at[k], dst_ref=precv.at[k], send_sem=ps_sem.at[0],
            recv_sem=pr_sem.at[chip * (pieces // wave) + q // wave],
            device_id=(g, partner), device_id_type=MESH,
        )

    strip = 16

    sent = set()

    def leaps(core, b):
        return chips > 2 and b in (0, last_chip)

    def hop(core, a, b, q):
        k = b * pieces + q
        to_right = b > a
        jump = leaps(core, b) and abs(b - a) == 2
        to = b if jump else (a + 1 if to_right else a - 1)
        if jump:
            landing = jrecv.at[q]
            arrival = j_sem.at[q]
        else:
            landing = (rrecv if to_right else lrecv).at[k]
            arrival = hr_sem.at[k + (pieces if to_right else 0)]
        return pltpu.make_async_remote_copy(
            src_ref=(rsend if to_right else lsend).at[k], dst_ref=landing,
            send_sem=(rs_sem if to_right else ls_sem).at[0], recv_sem=arrival,
            device_id=(g, to * 2 + c), device_id_type=MESH,
        ), landing

    def send(core, a, b, q):
        if (core, a, b, q) in sent:
            return
        sent.add((core, a, b, q))
        before = a - 1 if b > a else a + 1
        joins = 0 <= before < chips and not (leaps(core, b) and abs(b - a) == 1)

        @pl.when((c == core) & (z == a))
        def _():
            k = b * pieces + q
            if joins:
                copy, landed = hop(core, before, b, q)
                copy.wait_recv()
            out = rsend if b > a else lsend

            @pl.loop(0, rows // strip)
            def _(n):
                at = pl.ds(pl.multiple_of(n * strip, strip), strip)
                value = own[k, at] + precv[k, at].astype(F32)
                if joins:
                    value = value + landed[at].astype(F32)
                out[k, at] = value.astype(BF16)

            hop(core, a, b, q)[0].start()

    def send_first(core, turn, q):
        if turn < last_chip:
            send(core, 0, last_chip - turn, q)
            send(core, last_chip, turn, q)

    def send_relay(core, d, q):
        if 0 < d < last_chip:
            send(core, d, last_chip, q)
            send(core, last_chip - d, 0, q)

    def send_low(core, q):
        if chips > 3:
            send(core, 1, 2, q)

    def send_high(core, q):
        if chips > 3:
            send(core, last_chip - 1, last_chip - 2, q)

    steps = [(i, q) for i in range(chips) for q in range(0, pieces, wave)]

    def product(n, q, into, k):
        for m in range(tiles * wave):
            at = q * piece + m * tile
            into[k + m // tiles, :, m % tiles * tile:(m % tiles + 1) * tile] = jnp.dot(
                x_ref[...], wbuf[n, :, at:at + tile], preferred_element_type=F32
            ).astype(into.dtype)

    def project(phase, n):
        if phase + n == 0:
            @pl.when(c == 0)
            def _():
                product(0, 0, own, first_at)

            return
        i, q = steps[n]
        block = phase * chips + i
        k = block_chip(i) * pieces + q
        weights(block, q * piece)

        @pl.when(c == phase)
        def _():
            product(block, q, own, k)

        @pl.when(c != phase)
        def _():
            product(block, q, psend, k)
            send_other(n)

    def send_other(n):
        i, q = steps[n]
        for p in range(wave):
            pair_copy(block_chip(i), q + p).start()

    def settle(phase, n):
        i, first = steps[n]
        both = pl.ds(block_chip(i) * pieces + first, wave)

        @pl.when(c == phase)
        def _():
            all_of(
                psend.at[both], precv.at[both], ps_sem.at[0],
                pr_sem.at[block_chip(i) * (pieces // wave) + first // wave],
            ).wait_recv()

        if phase == 0 and i < HELD:
            for q in range(first, first + wave):
                send_first(0, i, q)

    lane_number = (lax.broadcasted_iota(jnp.int32, (slots, LANES), 1) // rank + 1).astype(F32)
    per_tile = LANES // rank
    tile_count = owned * rank // LANES
    chunk = min(512, owned * rank)

    def term_pair(h):
        return pltpu.make_async_remote_copy(
            src_ref=packed.at[h], dst_ref=arp.at[h], send_sem=as_sem.at[0],
            recv_sem=ar_sem.at[h], device_id=(g, partner), device_id_type=MESH,
        )

    def term_copy(h, k, core):
        to = lax.rem(z + jnp.where(low, chips - k, k), chips)
        return pltpu.make_async_remote_copy(
            src_ref=arz.at[h, z], dst_ref=arz.at[h, z], send_sem=zs_sem.at[0],
            recv_sem=zr_sem.at[h], device_id=(g, to * 2 + core), device_id_type=MESH,
        )

    def terms_wait(h):
        @pl.when(c == 0)
        def _():
            all_of(arz.at[h], arz.at[h], zs_sem.at[0], zr_sem.at[h]).wait_recv()

        if chips > 1:
            @pl.when(c == 1)
            def _():
                far_chips = pl.ds(0, chips - 1)
                all_of(
                    arz.at[h, far_chips], arz.at[h, far_chips], zs_sem.at[0], zr_sem.at[h]
                ).wait_recv()

    def wanted_of(h):
        return wants[h]

    def shrink_rows(h):
        rows_wait(h)
        if h == 0:
            down_copy.wait()
        wanted = wanted_of(h).T[:rank]
        flat = xrecv[h].reshape(slots, depth)
        mine = jnp.zeros((rank, slots), F32)
        for first in range(0, owned * rank, chunk):
            every = lax.dot_general(
                dbuf[first:first + chunk, :], flat, (((1,), (1,)), ((), ())),
                preferred_element_type=F32,
            )
            for p in range(chunk // rank):
                number = float(first // rank + p + 1)
                mine = jnp.where(wanted == number, every[p * rank:(p + 1) * rank], mine)
        packed[h] = mine

        @pl.when(c == 0)
        def _():
            term_pair(h).start()

    def sum_send(h):
        @pl.when(c == 1)
        def _():
            term_pair(h).wait_recv()
            arz[h, z] = (packed[h] + arp[h]).astype(BF16)
            term_copy(h, 0, 0).start()
            for k in range(1, chips):
                for core in range(2):
                    term_copy(h, k, core).start()

    def back_copy(h, k, cols):
        to = peer(k)
        return pltpu.make_async_remote_copy(
            src_ref=esend.at[h, to, :, cols], dst_ref=eback.at[h, g, :, cols],
            send_sem=es_sem.at[0], recv_sem=er_sem.at[h],
            device_id=(to, t), device_id_type=MESH,
        )

    def back_wait(h):
        all_of(
            esend.at[h, others], eback.at[h, others], es_sem.at[0], er_sem.at[h]
        ).wait_recv()

    wide = min(512, width)

    def expand_rows(h):
        terms_wait(h)
        total = arz[h, 0].astype(F32)
        for k in range(1, chips):
            total = total + arz[h, k].astype(F32)
        total = total.astype(BF16).astype(F32)
        if h == 0:
            up_copy.wait()
        wanted = wanted_of(h)
        shrink = jnp.concatenate([total] * per_tile, axis=0).T
        spread = jnp.concatenate(
            [
                jnp.where(wanted == lane_number + float(m * per_tile), shrink, 0.0).astype(BF16)
                for m in range(tile_count)
            ],
            axis=1,
        )

        for n in range(width // wide):
            cols = pl.ds(n * wide, wide)
            grown = jnp.dot(
                spread, ubuf[:, n * wide:(n + 1) * wide], preferred_element_type=F32
            ).astype(BF16)
            for k in range(groups):
                esend[h, k, :, cols] = grown[k * part:(k + 1) * part]
            for k in far + near:
                back_copy(h, k, cols).start()
        eback[h, g] = esend[h, g]

    with scope("x"):
        x_copy.wait()
    first_at = block_chip(0) * pieces
    weights(0, 0)

    @pl.when(c == 1)
    def _():
        product(0, 0, psend, first_at)

    with scope("enter"):
        enter()

    @pl.when(c == 1)
    def _():
        send_other(0)

    with scope("place0"):
        place_rows(0)
    if rounds:
        tell(0)
    greet_ends()

    def near_rows(h):
        for k in near:
            if h == 0:
                idx_copy_to(k).start()
            row_copy(h, k).start()

    def far_rows(h):
        if h == 0:
            greet_far()
        for k in far:
            if h == 0:
                idx_copy_to(k).start()
            row_copy(h, k).start()

    def load_factors():
        down_copy.start()
        up_copy.start()
        res_copy.start()

    stages = {
        "project": project, "settle": settle, "place": place_rows, "near": near_rows,
        "far": far_rows, "greet": greet_chips, "meet": meet_chips, "factors": load_factors,
        "shrink": shrink_rows, "sum": sum_send, "expand": expand_rows,
        "first": send_first, "relay": send_relay, "low": send_low, "high": send_high, "requests": requests,
    }
    for name, *at in ORDER:
        if name in ("first", "relay", "low", "high"):
            if at[-1] >= pieces:
                continue
        elif name in ("project", "settle"):
            if at[1] >= len(steps):
                continue
        elif at and at[0] >= halves:
            continue
        with scope(name + "_".join(str(v) for v in at)):
            stages[name](*at)
    for b in range(chips):
        for a in list(range(b)) + list(range(last_chip, b, -1)):
            for core in range(2):
                for q in range(pieces):
                    send(core, a, b, q)

    res_copy.wait()

    def branch_of(h, q, n):
        slot_col = slot_of(rank_col, own_col, h)
        unplace = jnp.where(
            lax.broadcasted_iota(jnp.int32, (rows, slots), 1) == slot_col, 1.0, 0.0
        ).astype(BF16)
        first = q * piece + n * tile
        back = eback[h, :, :, first:first + tile].reshape(slots, tile)
        return jnp.dot(unplace, back, preferred_element_type=F32)

    def close(core, q, into):
        for a in range(chips):
            @pl.when((c == core) & (z == a))
            def _():
                landed = []
                for step in (1, 2):
                    for source in (a - step, a + step):
                        if 0 <= source < chips and (step == 1 or leaps(core, a)):
                            copy, ref = hop(core, source, a, q)
                            copy.wait_recv()
                            landed.append(ref)

                @pl.loop(0, rows // strip)
                def _(n):
                    at = pl.ds(pl.multiple_of(n * strip, strip), strip)
                    value = own[a * pieces + q, at]
                    for ref in landed:
                        value = value + ref[at].astype(F32)
                    if into is own:
                        own[a * pieces + q, at] = value
                    else:
                        out_ref[at, q * piece:(q + 1) * piece] = value.astype(BF16)

    with scope("close0"):
        for q in range(pieces):
            close(0, q, own)

    for h in range(halves):
        with scope("backwait%d" % h):
            back_wait(h)
        for q in range(pieces):
            for n in range(tiles):
                cols = slice(n * tile, (n + 1) * tile)
                first = q * piece + n * tile
                value = own[z * pieces + q, :, cols] + branch_of(h, q, n)
                if h == 0:
                    value = (
                        value + precv[z * pieces + q, :, cols].astype(F32)
                        + rbuf[:, first:first + tile].astype(F32)
                    )
                own[z * pieces + q, :, cols] = value
                if h == halves - 1:
                    out_ref[:, first:first + tile] = value.astype(BF16)

    for q in range(pieces):
        with scope("fin%d" % q):
            close(1, q, out_ref)

    tail = scope("tail")
    tail.__enter__()
    all_of(psend, precv, ps_sem.at[0], ps_sem.at[0]).wait_send()

    @pl.when(c == 0)
    def _():
        all_of(packed, arp, as_sem.at[0], as_sem.at[0]).wait_send()

    @pl.when(c == 1)
    def _():
        all_of(arz, arz, zs_sem.at[0], zs_sem.at[0]).wait_send()
        if chips > 1:
            far_chips = pl.ds(0, chips - 1)
            all_of(
                arz.at[:, far_chips], arz.at[:, far_chips], zs_sem.at[0], zs_sem.at[0]
            ).wait_send()

    if groups > 1:
        all_of(
            xsend.at[:, others], xrecv.at[:, others], xs_sem.at[0], xs_sem.at[0]
        ).wait_send()
        all_of(
            esend.at[:, others], eback.at[:, others], es_sem.at[0], es_sem.at[0]
        ).wait_send()
        all_of(idx_all.at[others], idx_all.at[others], is_sem.at[0], is_sem.at[0]).wait_send()
    for chip in range(chips):
        @pl.when(z == chip)
        def _():
            if chip < last_chip:
                sent = pl.ds(0, (last_chip - chip) * pieces)
                all_of(
                    rsend.at[sent], rrecv.at[sent], rs_sem.at[0], rs_sem.at[0]
                ).wait_send()
            if chip > 0:
                sent = pl.ds(0, chip * pieces)
                all_of(
                    lsend.at[sent], lrecv.at[sent], ls_sem.at[0], ls_sem.at[0]
                ).wait_send()
    tail.__exit__(None, None, None)


def body(attention_output, residual, output_weight, down_factors, up_factors, adapter_index):
    groups = lax.axis_size("dp")
    members = lax.axis_size("tensor")
    rows, depth = attention_output.shape
    owned, _, rank = down_factors.shape
    width = output_weight.shape[1] // members
    cap = 2 * rows // groups
    chips = members // 2
    halves = 2 if cap % 32 == 0 else 1
    part = cap // halves
    slots = groups * part
    pieces = max(1, min(PIECES, width // 256))
    piece = width // pieces
    down = jnp.swapaxes(down_factors, 1, 2).reshape(owned * rank, depth)
    up = up_factors.reshape(owned * rank, width)
    vmem = pl.BlockSpec(memory_space=pltpu.VMEM)
    hbm = pl.BlockSpec(memory_space=pl.ANY)
    dma = pltpu.SemaphoreType.DMA
    hops = chips * pieces
    return pl.pallas_call(
        functools.partial(kernel, groups, members, rank, owned, halves, pieces),
        out_shape=pltpu.VMEM((rows, width), BF16),
        in_specs=[hbm] * 6,
        out_specs=vmem,
        scratch_shapes=[
            pltpu.VMEM((rows, depth), BF16),
            pltpu.VMEM((1, rows), jnp.int32),
            pltpu.VMEM((groups, 1, rows), jnp.int32),
            pltpu.VMEM((members, depth, width), BF16),
            pltpu.VMEM((owned * rank, depth), BF16),
            pltpu.VMEM((owned * rank, width), BF16),
            pltpu.VMEM((rows, width), BF16),
            pltpu.VMEM((hops, rows, piece), F32),
            pltpu.VMEM((hops, rows, piece), BF16),
            pltpu.VMEM((hops, rows, piece), BF16),
            pltpu.VMEM((hops, rows, piece), BF16),
            pltpu.VMEM((hops, rows, piece), BF16),
            pltpu.VMEM((hops, rows, piece), BF16),
            pltpu.VMEM((hops, rows, piece), BF16),
            pltpu.VMEM((pieces, rows, piece), BF16),
            pltpu.VMEM((halves, groups, part, depth), BF16),
            pltpu.VMEM((halves, groups, part, depth), BF16),
            pltpu.VMEM((halves, slots, LANES), F32),
            pltpu.VMEM((halves, rank, slots), F32),
            pltpu.VMEM((halves, rank, slots), F32),
            pltpu.VMEM((halves, chips, rank, slots), BF16),
            pltpu.VMEM((halves, groups, part, width), BF16),
            pltpu.VMEM((halves, groups, part, width), BF16),
            dma((AHEAD,)), dma((3,)), dma((1,)), dma((hops // (2 if pieces % 2 == 0 else 1),)),
            dma((1,)), dma((1,)), dma((hops + pieces,)), dma((pieces,)),
            dma((1,)), dma((halves,)), dma((1,)), dma((halves,)),
            dma((1,)), dma((halves,)), dma((1,)), dma((halves,)),
            pltpu.SemaphoreType.REGULAR((max(1, groups.bit_length() - 2),)),
            pltpu.SemaphoreType.REGULAR((2,)),
            dma((1,)), dma((1,)),
        ],
        compiler_params=pltpu.CompilerParams(
            collective_id=0, has_side_effects=True, vmem_limit_bytes=60 * 1024 * 1024
        ),
    )(attention_output, residual, adapter_index.reshape(1, rows), output_weight, down, up)


def solution(mesh):
    return jax.shard_map(
        body,
        mesh=mesh,
        in_specs=(
            P("dp", "tensor"),
            P("dp", "tensor"),
            P("tensor", None),
            P("dp", "tensor", None),
            P("dp", None, "tensor"),
            P("dp"),
        ),
        out_specs=P("dp", "tensor"),
        check_vma=False,
    )
```

```python
import contextlib
import functools

import jax
import jax.numpy as jnp
from jax import lax
from jax.experimental import pallas as pl
from jax.experimental.pallas import tpu as pltpu
from jax.sharding import PartitionSpec as P

MESH = pl.DeviceIdType.MESH
F32 = jnp.float32
BF16 = jnp.bfloat16
LANES = 128
PIECES = 4
AHEAD = 4
FIRST = 2
HELD = 2
ORDER = (
    ("near", 0), ("project", 0, 0), ("project", 0, 1), ("project", 0, 2), ("settle", 0, 0),
    ("far", 0), ("project", 0, 3), ("settle", 0, 1), ("place", 1), ("factors",),
    ("project", 0, 4), ("settle", 0, 2), ("project", 0, 5), ("settle", 0, 3), ("far", 1),
    ("near", 1), ("project", 1, 0), ("project", 0, 6), ("settle", 0, 4), ("greet",),
    ("project", 0, 7), ("settle", 0, 5), ("settle", 0, 6), ("settle", 0, 7), ("relay", 0, 2, 0),
    ("relay", 0, 2, 1), ("relay", 0, 2, 2), ("relay", 0, 2, 3), ("requests",), ("relay", 0, 1, 0),
    ("relay", 0, 1, 1), ("shrink", 0), ("settle", 1, 0), ("first", 1, 0, 0), ("first", 0, 2, 0),
    ("first", 0, 2, 1), ("relay", 0, 1, 2), ("relay", 0, 1, 3), ("project", 1, 1), ("low", 0, 0),
    ("low", 0, 1), ("project", 1, 2), ("meet",), ("sum", 0), ("project", 1, 3), ("settle", 1, 1),
    ("first", 1, 0, 1), ("shrink", 1), ("project", 1, 4), ("high", 0, 0), ("high", 0, 1),
    ("sum", 1), ("first", 1, 0, 2), ("low", 0, 2), ("low", 0, 3), ("first", 1, 0, 3),
    ("settle", 1, 2), ("first", 1, 1, 0), ("first", 1, 1, 1), ("settle", 1, 3), ("project", 1, 5),
    ("relay", 1, 1, 0), ("project", 1, 6), ("project", 1, 7), ("high", 0, 2), ("high", 0, 3),
    ("first", 1, 1, 2), ("first", 1, 1, 3), ("settle", 1, 4), ("settle", 1, 5),
    ("first", 1, 2, 0), ("first", 1, 2, 1), ("first", 1, 2, 2), ("first", 1, 2, 3),
    ("settle", 1, 6), ("settle", 1, 7), ("expand", 0), ("relay", 1, 1, 1), ("relay", 1, 1, 2),
    ("relay", 1, 2, 0), ("relay", 1, 2, 1), ("relay", 1, 2, 2), ("relay", 1, 2, 3), ("expand", 1),
    ("relay", 1, 1, 3), ("first", 0, 2, 2), ("first", 0, 2, 3), ("low", 1, 0), ("high", 1, 0),
    ("low", 1, 1), ("high", 1, 1), ("low", 1, 2), ("high", 1, 2), ("low", 1, 3), ("high", 1, 3),
)
scope = contextlib.nullcontext


def kernel(
    groups, members, rank, owned, halves, pieces,
    x_hbm, res_ref, idx_hbm, w_ref, down_ref, up_ref, out_ref,
    x_ref, idx_ref, idx_all, wbuf, dbuf, ubuf, rbuf, own, psend, precv, rrecv, lrecv, rsend, lsend, jrecv,
    xsend, xrecv, wants, packed, arp, arz, esend, eback,
    w_sem, d_sem, ps_sem, pr_sem, rs_sem, ls_sem, hr_sem, j_sem,
    xs_sem, xr_sem, as_sem, ar_sem, zs_sem, zr_sem, es_sem, er_sem, dp_sem, z_sem, is_sem, ir_sem,
):
    chips = members // 2
    g = lax.axis_index("dp")
    t = lax.axis_index("tensor")
    z = t // 2
    c = lax.rem(t, 2)
    partner = z * 2 + (1 - c)
    rows, depth = x_ref.shape
    width = out_ref.shape[1]
    part = xrecv.shape[2]
    slots = groups * part
    low = z < chips // 2
    high = jnp.logical_not(low)
    piece = width // pieces
    last_chip = chips - 1
    wave = 2 if pieces % 2 == 0 else 1

    def core_of(chip):
        return (g, chip * 2 + c)

    bits = groups.bit_length() - 1
    cube = groups == 1 << bits

    def peer(k):
        if not cube:
            return lax.rem(g + k, groups)
        to = g
        for b in range(bits):
            if k >> b & 1:
                to = to + (1 << b) * (1 - 2 * lax.rem(g // (1 << b), 2))
        return to

    def source_of(k):
        return peer(k) if cube else lax.rem(g + groups - k, groups)

    near = [1 << b for b in range(bits)] if cube else list(range(1, groups))
    far = [k for k in range(1, groups) if k not in near]
    rounds = bits - 1 if far else 0

    barrier = pltpu.get_barrier_semaphore()
    pl.semaphore_signal(barrier, inc=1, device_id=(g, partner), device_id_type=MESH)

    @pl.when(z > 0)
    def _():
        pl.semaphore_signal(barrier, inc=1, device_id=core_of(z - 1), device_id_type=MESH)

    @pl.when(z < last_chip)
    def _():
        pl.semaphore_signal(barrier, inc=1, device_id=core_of(z + 1), device_id_type=MESH)

    for k in near:
        pl.semaphore_signal(barrier, inc=1, device_id=(peer(k), t), device_id_type=MESH)

    def block_chip(i):
        return jnp.where(low, chips - 1 - i, i)

    blocks = [(n, 0, width) for n in range(members)]
    if pieces % 2 == 0:
        blocks[:1] = [(0, p * width // 2, width // 2) for p in range(2)]
    chunks = len(blocks)
    loaded = set()

    def weight_copy(j):
        n, offset, size = blocks[j]
        column = block_chip(n % chips) * 2 + n // chips
        start = pl.multiple_of(column * width + offset, LANES)
        return pltpu.make_async_copy(
            w_ref.at[:, pl.ds(start, size)], wbuf.at[n, :, pl.ds(offset, size)],
            w_sem.at[j % AHEAD],
        )

    def weights(n, column):
        for j in range(chunks):
            if j not in loaded and blocks[j][:2] <= (n, column) and blocks[j][0] == n:
                weight_copy(j).wait()
                loaded.add(j)
                if j + AHEAD < chunks:
                    weight_copy(j + AHEAD).start()

    down_copy = pltpu.make_async_copy(down_ref, dbuf, d_sem.at[0])
    up_copy = pltpu.make_async_copy(up_ref, ubuf, d_sem.at[1])
    res_copy = pltpu.make_async_copy(res_ref, rbuf, d_sem.at[2])
    x_copy = pltpu.make_async_copy(x_hbm, x_ref, d_sem.at[0])
    idx_copy = pltpu.make_async_copy(idx_hbm, idx_ref, d_sem.at[1])
    idx_copy.start()
    x_copy.start()
    for j in range(min(FIRST, chunks)):
        weight_copy(j).start()

    def enter():
        near_chips = jnp.where(z > 0, 1, 0) + jnp.where(z < last_chip, 1, 0)
        pl.semaphore_wait(barrier, 1 + len(near) + near_chips)

    def tell(b):
        pl.semaphore_signal(
            dp_sem.at[b], inc=1, device_id=(peer(1 << b), t), device_id_type=MESH
        )

    def tell_chip(n, to):
        pl.semaphore_signal(z_sem.at[n], inc=1, device_id=core_of(to), device_id_type=MESH)

    def greet_far():
        for b in range(rounds):
            pl.semaphore_wait(dp_sem.at[b], 1)
            if b + 1 < rounds:
                tell(b + 1)

    def greet_ends():
        if chips < 3:
            return

        @pl.when(z == 0)
        def _():
            tell_chip(0, z + 1)

        @pl.when(z == last_chip)
        def _():
            tell_chip(1, z - 1)

    def greet_chips():
        if chips < 3:
            return

        @pl.when((z > 0) & low)
        def _():
            pl.semaphore_wait(z_sem.at[0], 1)
            tell_chip(0, z + 1)
            pl.semaphore_wait(z_sem.at[1], 1)
            tell_chip(1, z - 1)

        @pl.when((z < last_chip) & jnp.logical_not(low))
        def _():
            pl.semaphore_wait(z_sem.at[1], 1)
            tell_chip(1, z - 1)
            pl.semaphore_wait(z_sem.at[0], 1)
            tell_chip(0, z + 1)

    def meet_chips():
        if chips < 3:
            return

        @pl.when(z == 0)
        def _():
            pl.semaphore_wait(z_sem.at[1], 1)

        @pl.when(z == last_chip)
        def _():
            pl.semaphore_wait(z_sem.at[0], 1)

    idx_copy.wait()
    for j in range(FIRST, min(AHEAD, chunks)):
        weight_copy(j).start()
    idx_row = idx_ref[...]
    r_i = lax.broadcasted_iota(jnp.int32, (rows, rows), 0)
    c_i = lax.broadcasted_iota(jnp.int32, (rows, rows), 1)
    idx_full = jnp.broadcast_to(idx_row, (rows, rows))
    idx_col = jnp.sum(jnp.where(r_i == c_i, idx_full, 0), axis=1, keepdims=True)
    own_row = idx_row // owned
    own_col = idx_col // owned
    same = own_col == own_row
    rank_row = jnp.sum(jnp.where(same & (r_i < c_i), 1, 0), axis=0, keepdims=True)
    rank_col = jnp.sum(jnp.where(same & (c_i < r_i), 1, 0), axis=1, keepdims=True)

    def slot_of(place_rank, owner, h):
        inside = place_rank - h * part
        keep = (inside >= 0) & (inside < part)
        return jnp.where(keep, owner * part + inside, -1)

    step = min(256, depth)

    def row_copy(h, k):
        to = peer(k)
        return pltpu.make_async_remote_copy(
            src_ref=xsend.at[h, to], dst_ref=xrecv.at[h, g],
            send_sem=xs_sem.at[0], recv_sem=xr_sem.at[h],
            device_id=(to, t), device_id_type=MESH,
        )

    others = pl.ds(0, groups - 1)

    def all_of(send, recv, send_sem, recv_sem):
        return pltpu.make_async_remote_copy(
            src_ref=send, dst_ref=recv, send_sem=send_sem, recv_sem=recv_sem,
            device_id=(g, partner), device_id_type=MESH,
        )

    def idx_copy_to(k):
        return pltpu.make_async_remote_copy(
            src_ref=idx_ref, dst_ref=idx_all.at[g], send_sem=is_sem.at[0],
            recv_sem=ir_sem.at[0], device_id=(peer(k), t), device_id_type=MESH,
        )

    def requests():
        idx_all[g] = idx_ref[...]
        if groups > 1:
            all_of(
                idx_all.at[others], idx_all.at[others], is_sem.at[0], ir_sem.at[0]
            ).wait_recv()
        every_row = jnp.concatenate([idx_all[k] for k in range(groups)], axis=0)
        chosen = every_row // owned == g
        earlier = jnp.where(r_i < c_i, 1.0, 0.0).astype(BF16)
        ahead = jnp.dot(
            jnp.where(chosen, 1.0, 0.0).astype(BF16), earlier, preferred_element_type=F32
        ).astype(jnp.int32)
        slot = jnp.where(chosen, ahead, -1)
        number = lax.rem(every_row, owned) + 1
        for h in range(halves):
            for k in range(groups):
                place = lax.broadcasted_iota(jnp.int32, (part, rows), 0) + h * part
                asked = jnp.where(place == slot[k:k + 1], number[k:k + 1], 0)
                wants[h, k * part:(k + 1) * part] = jnp.broadcast_to(
                    jnp.sum(asked, axis=1, keepdims=True).astype(F32), (part, LANES)
                )

    def rows_wait(h):
        all_of(
            xsend.at[h, others], xrecv.at[h, others], xs_sem.at[0], xr_sem.at[h]
        ).wait_recv()

    def place_rows(h):
        slot_row = slot_of(rank_row, own_row, h)
        placing = lax.broadcasted_iota(jnp.int32, (slots, rows), 0) == slot_row
        place = jnp.where(placing, 1.0, 0.0).astype(BF16)
        for j in range(depth // step):
            moved = jnp.dot(
                place, x_ref[:, j * step:(j + 1) * step], preferred_element_type=F32
            ).astype(BF16)
            for k in range(groups):
                xsend[h, k, :, j * step:(j + 1) * step] = moved[k * part:(k + 1) * part]
        xrecv[h, g] = xsend[h, g]

    tile = min(256, piece)
    tiles = piece // tile

    def pair_copy(chip, q):
        k = chip * pieces + q
        return pltpu.make_async_remote_copy(
            src_ref=psend.at[k], dst_ref=precv.at[k], send_sem=ps_sem.at[0],
            recv_sem=pr_sem.at[chip * (pieces // wave) + q // wave],
            device_id=(g, partner), device_id_type=MESH,
        )

    strip = 16

    sent = set()

    def leaps(core, b):
        return chips > 2 and b in (0, last_chip)

    def hop(core, a, b, q):
        k = b * pieces + q
        to_right = b > a
        jump = leaps(core, b) and abs(b - a) == 2
        to = b if jump else (a + 1 if to_right else a - 1)
        if jump:
            landing = jrecv.at[q]
            arrival = j_sem.at[q]
        else:
            landing = (rrecv if to_right else lrecv).at[k]
            arrival = hr_sem.at[k + (pieces if to_right else 0)]
        return pltpu.make_async_remote_copy(
            src_ref=(rsend if to_right else lsend).at[k], dst_ref=landing,
            send_sem=(rs_sem if to_right else ls_sem).at[0], recv_sem=arrival,
            device_id=(g, to * 2 + c), device_id_type=MESH,
        ), landing

    def send(core, a, b, q):
        if (core, a, b, q) in sent:
            return
        sent.add((core, a, b, q))
        before = a - 1 if b > a else a + 1
        joins = 0 <= before < chips and not (leaps(core, b) and abs(b - a) == 1)

        @pl.when((c == core) & (z == a))
        def _():
            k = b * pieces + q
            if joins:
                copy, landed = hop(core, before, b, q)
                copy.wait_recv()
            out = rsend if b > a else lsend

            @pl.loop(0, rows // strip)
            def _(n):
                at = pl.ds(pl.multiple_of(n * strip, strip), strip)
                value = own[k, at] + precv[k, at].astype(F32)
                if joins:
                    value = value + landed[at].astype(F32)
                out[k, at] = value.astype(BF16)

            hop(core, a, b, q)[0].start()

    def send_first(core, turn, q):
        if turn < last_chip:
            send(core, 0, last_chip - turn, q)
            send(core, last_chip, turn, q)

    def send_relay(core, d, q):
        if 0 < d < last_chip:
            send(core, d, last_chip, q)
            send(core, last_chip - d, 0, q)

    def send_low(core, q):
        if chips > 3:
            send(core, 1, 2, q)

    def send_high(core, q):
        if chips > 3:
            send(core, last_chip - 1, last_chip - 2, q)

    steps = [(i, q) for i in range(chips) for q in range(0, pieces, wave)]

    def product(n, q, into, k):
        for m in range(tiles * wave):
            at = q * piece + m * tile
            into[k + m // tiles, :, m % tiles * tile:(m % tiles + 1) * tile] = jnp.dot(
                x_ref[...], wbuf[n, :, at:at + tile], preferred_element_type=F32
            ).astype(into.dtype)

    def project(phase, n):
        if phase + n == 0:
            @pl.when(c == 0)
            def _():
                product(0, 0, own, first_at)

            return
        i, q = steps[n]
        block = phase * chips + i
        k = block_chip(i) * pieces + q
        weights(block, q * piece)

        @pl.when(c == phase)
        def _():
            product(block, q, own, k)

        @pl.when(c != phase)
        def _():
            product(block, q, psend, k)
            send_other(n)

    def send_other(n):
        i, q = steps[n]
        for p in range(wave):
            pair_copy(block_chip(i), q + p).start()

    def settle(phase, n):
        i, first = steps[n]
        both = pl.ds(block_chip(i) * pieces + first, wave)

        @pl.when(c == phase)
        def _():
            all_of(
                psend.at[both], precv.at[both], ps_sem.at[0],
                pr_sem.at[block_chip(i) * (pieces // wave) + first // wave],
            ).wait_recv()

        if phase == 0 and i < HELD:
            for q in range(first, first + wave):
                send_first(0, i, q)

    lane_number = (lax.broadcasted_iota(jnp.int32, (slots, LANES), 1) // rank + 1).astype(F32)
    per_tile = LANES // rank
    tile_count = owned * rank // LANES
    chunk = min(512, owned * rank)

    def term_pair(h):
        return pltpu.make_async_remote_copy(
            src_ref=packed.at[h], dst_ref=arp.at[h], send_sem=as_sem.at[0],
            recv_sem=ar_sem.at[h], device_id=(g, partner), device_id_type=MESH,
        )

    def term_copy(h, k, core):
        to = lax.rem(z + jnp.where(low, chips - k, k), chips)
        return pltpu.make_async_remote_copy(
            src_ref=arz.at[h, z], dst_ref=arz.at[h, z], send_sem=zs_sem.at[0],
            recv_sem=zr_sem.at[h], device_id=(g, to * 2 + core), device_id_type=MESH,
        )

    def terms_wait(h):
        @pl.when(c == 0)
        def _():
            all_of(arz.at[h], arz.at[h], zs_sem.at[0], zr_sem.at[h]).wait_recv()

        if chips > 1:
            @pl.when(c == 1)
            def _():
                far_chips = pl.ds(0, chips - 1)
                all_of(
                    arz.at[h, far_chips], arz.at[h, far_chips], zs_sem.at[0], zr_sem.at[h]
                ).wait_recv()

    def wanted_of(h):
        return wants[h]

    def shrink_rows(h):
        rows_wait(h)
        if h == 0:
            down_copy.wait()
        wanted = wanted_of(h).T[:rank]
        flat = xrecv[h].reshape(slots, depth)
        mine = jnp.zeros((rank, slots), F32)
        for first in range(0, owned * rank, chunk):
            every = lax.dot_general(
                dbuf[first:first + chunk, :], flat, (((1,), (1,)), ((), ())),
                preferred_element_type=F32,
            )
            for p in range(chunk // rank):
                number = float(first // rank + p + 1)
                mine = jnp.where(wanted == number, every[p * rank:(p + 1) * rank], mine)
        packed[h] = mine

        @pl.when(c == 0)
        def _():
            term_pair(h).start()

    def sum_send(h):
        @pl.when(c == 1)
        def _():
            term_pair(h).wait_recv()
            arz[h, z] = (packed[h] + arp[h]).astype(BF16)
            for core in range(2):
                for k in range(1, chips):
                    term_copy(h, k, core).start()
            term_copy(h, 0, 0).start()

    def back_copy(h, k, cols):
        to = peer(k)
        return pltpu.make_async_remote_copy(
            src_ref=esend.at[h, to, :, cols], dst_ref=eback.at[h, g, :, cols],
            send_sem=es_sem.at[0], recv_sem=er_sem.at[h],
            device_id=(to, t), device_id_type=MESH,
        )

    def back_wait(h):
        all_of(
            esend.at[h, others], eback.at[h, others], es_sem.at[0], er_sem.at[h]
        ).wait_recv()

    wide = min(512, width)

    def expand_rows(h):
        terms_wait(h)
        total = arz[h, 0].astype(F32)
        for k in range(1, chips):
            total = total + arz[h, k].astype(F32)
        total = total.astype(BF16).astype(F32)
        if h == 0:
            up_copy.wait()
        wanted = wanted_of(h)
        shrink = jnp.concatenate([total] * per_tile, axis=0).T
        spread = jnp.concatenate(
            [
                jnp.where(wanted == lane_number + float(m * per_tile), shrink, 0.0).astype(BF16)
                for m in range(tile_count)
            ],
            axis=1,
        )

        for n in range(width // wide):
            cols = pl.ds(n * wide, wide)
            grown = jnp.dot(
                spread, ubuf[:, n * wide:(n + 1) * wide], preferred_element_type=F32
            ).astype(BF16)
            for k in range(groups):
                esend[h, k, :, cols] = grown[k * part:(k + 1) * part]
            for k in far + near:
                back_copy(h, k, cols).start()
        eback[h, g] = esend[h, g]

    with scope("x"):
        x_copy.wait()
    first_at = block_chip(0) * pieces
    weights(0, 0)

    @pl.when(c == 1)
    def _():
        product(0, 0, psend, first_at)

    with scope("enter"):
        enter()

    @pl.when(c == 1)
    def _():
        send_other(0)

    with scope("place0"):
        place_rows(0)
    if rounds:
        tell(0)
    greet_ends()

    def near_rows(h):
        for k in near:
            if h == 0:
                idx_copy_to(k).start()
            row_copy(h, k).start()

    def far_rows(h):
        if h == 0:
            greet_far()
        for k in far:
            if h == 0:
                idx_copy_to(k).start()
            row_copy(h, k).start()

    def load_factors():
        down_copy.start()
        up_copy.start()
        res_copy.start()

    stages = {
        "project": project, "settle": settle, "place": place_rows, "near": near_rows,
        "far": far_rows, "greet": greet_chips, "meet": meet_chips, "factors": load_factors,
        "shrink": shrink_rows, "sum": sum_send, "expand": expand_rows,
        "first": send_first, "relay": send_relay, "low": send_low, "high": send_high, "requests": requests,
    }
    for name, *at in ORDER:
        if name in ("first", "relay", "low", "high"):
            if at[-1] >= pieces:
                continue
        elif name in ("project", "settle"):
            if at[1] >= len(steps):
                continue
        elif at and at[0] >= halves:
            continue
        with scope(name + "_".join(str(v) for v in at)):
            stages[name](*at)
    for b in range(chips):
        for a in list(range(b)) + list(range(last_chip, b, -1)):
            for core in range(2):
                for q in range(pieces):
                    send(core, a, b, q)

    res_copy.wait()

    def branch_of(h, q, n):
        slot_col = slot_of(rank_col, own_col, h)
        unplace = jnp.where(
            lax.broadcasted_iota(jnp.int32, (rows, slots), 1) == slot_col, 1.0, 0.0
        ).astype(BF16)
        first = q * piece + n * tile
        back = eback[h, :, :, first:first + tile].reshape(slots, tile)
        return jnp.dot(unplace, back, preferred_element_type=F32)

    def close(core, q, into):
        for a in range(chips):
            @pl.when((c == core) & (z == a))
            def _():
                landed = []
                for step in (1, 2):
                    for source in (a - step, a + step):
                        if 0 <= source < chips and (step == 1 or leaps(core, a)):
                            copy, ref = hop(core, source, a, q)
                            copy.wait_recv()
                            landed.append(ref)

                @pl.loop(0, rows // strip)
                def _(n):
                    at = pl.ds(pl.multiple_of(n * strip, strip), strip)
                    value = own[a * pieces + q, at]
                    for ref in landed:
                        value = value + ref[at].astype(F32)
                    if into is own:
                        own[a * pieces + q, at] = value
                    else:
                        out_ref[at, q * piece:(q + 1) * piece] = value.astype(BF16)

    with scope("close0"):
        for q in range(pieces):
            close(0, q, own)

    for h in range(halves):
        with scope("backwait%d" % h):
            back_wait(h)
        for q in range(pieces):
            for n in range(tiles):
                cols = slice(n * tile, (n + 1) * tile)
                first = q * piece + n * tile
                value = own[z * pieces + q, :, cols] + branch_of(h, q, n)
                if h == 0:
                    value = (
                        value + precv[z * pieces + q, :, cols].astype(F32)
                        + rbuf[:, first:first + tile].astype(F32)
                    )
                own[z * pieces + q, :, cols] = value
                if h == halves - 1:
                    out_ref[:, first:first + tile] = value.astype(BF16)

    for q in range(pieces):
        with scope("fin%d" % q):
            close(1, q, out_ref)

    tail = scope("tail")
    tail.__enter__()
    all_of(psend, precv, ps_sem.at[0], ps_sem.at[0]).wait_send()

    @pl.when(c == 0)
    def _():
        all_of(packed, arp, as_sem.at[0], as_sem.at[0]).wait_send()

    @pl.when(c == 1)
    def _():
        all_of(arz, arz, zs_sem.at[0], zs_sem.at[0]).wait_send()
        if chips > 1:
            far_chips = pl.ds(0, chips - 1)
            all_of(
                arz.at[:, far_chips], arz.at[:, far_chips], zs_sem.at[0], zs_sem.at[0]
            ).wait_send()

    if groups > 1:
        all_of(
            xsend.at[:, others], xrecv.at[:, others], xs_sem.at[0], xs_sem.at[0]
        ).wait_send()
        all_of(
            esend.at[:, others], eback.at[:, others], es_sem.at[0], es_sem.at[0]
        ).wait_send()
        all_of(idx_all.at[others], idx_all.at[others], is_sem.at[0], is_sem.at[0]).wait_send()
    for chip in range(chips):
        @pl.when(z == chip)
        def _():
            if chip < last_chip:
                sent = pl.ds(0, (last_chip - chip) * pieces)
                all_of(
                    rsend.at[sent], rrecv.at[sent], rs_sem.at[0], rs_sem.at[0]
                ).wait_send()
            if chip > 0:
                sent = pl.ds(0, chip * pieces)
                all_of(
                    lsend.at[sent], lrecv.at[sent], ls_sem.at[0], ls_sem.at[0]
                ).wait_send()
    tail.__exit__(None, None, None)


def body(attention_output, residual, output_weight, down_factors, up_factors, adapter_index):
    groups = lax.axis_size("dp")
    members = lax.axis_size("tensor")
    rows, depth = attention_output.shape
    owned, _, rank = down_factors.shape
    width = output_weight.shape[1] // members
    cap = 2 * rows // groups
    chips = members // 2
    halves = 2 if cap % 32 == 0 else 1
    part = cap // halves
    slots = groups * part
    pieces = max(1, min(PIECES, width // 256))
    piece = width // pieces
    down = jnp.swapaxes(down_factors, 1, 2).reshape(owned * rank, depth)
    up = up_factors.reshape(owned * rank, width)
    vmem = pl.BlockSpec(memory_space=pltpu.VMEM)
    hbm = pl.BlockSpec(memory_space=pl.ANY)
    dma = pltpu.SemaphoreType.DMA
    hops = chips * pieces
    return pl.pallas_call(
        functools.partial(kernel, groups, members, rank, owned, halves, pieces),
        out_shape=pltpu.VMEM((rows, width), BF16),
        in_specs=[hbm] * 6,
        out_specs=vmem,
        scratch_shapes=[
            pltpu.VMEM((rows, depth), BF16),
            pltpu.VMEM((1, rows), jnp.int32),
            pltpu.VMEM((groups, 1, rows), jnp.int32),
            pltpu.VMEM((members, depth, width), BF16),
            pltpu.VMEM((owned * rank, depth), BF16),
            pltpu.VMEM((owned * rank, width), BF16),
            pltpu.VMEM((rows, width), BF16),
            pltpu.VMEM((hops, rows, piece), F32),
            pltpu.VMEM((hops, rows, piece), BF16),
            pltpu.VMEM((hops, rows, piece), BF16),
            pltpu.VMEM((hops, rows, piece), BF16),
            pltpu.VMEM((hops, rows, piece), BF16),
            pltpu.VMEM((hops, rows, piece), BF16),
            pltpu.VMEM((hops, rows, piece), BF16),
            pltpu.VMEM((pieces, rows, piece), BF16),
            pltpu.VMEM((halves, groups, part, depth), BF16),
            pltpu.VMEM((halves, groups, part, depth), BF16),
            pltpu.VMEM((halves, slots, LANES), F32),
            pltpu.VMEM((halves, rank, slots), F32),
            pltpu.VMEM((halves, rank, slots), F32),
            pltpu.VMEM((halves, chips, rank, slots), BF16),
            pltpu.VMEM((halves, groups, part, width), BF16),
            pltpu.VMEM((halves, groups, part, width), BF16),
            dma((AHEAD,)), dma((3,)), dma((1,)), dma((hops // (2 if pieces % 2 == 0 else 1),)),
            dma((1,)), dma((1,)), dma((hops + pieces,)), dma((pieces,)),
            dma((1,)), dma((halves,)), dma((1,)), dma((halves,)),
            dma((1,)), dma((halves,)), dma((1,)), dma((halves,)),
            pltpu.SemaphoreType.REGULAR((max(1, groups.bit_length() - 2),)),
            pltpu.SemaphoreType.REGULAR((2,)),
            dma((1,)), dma((1,)),
        ],
        compiler_params=pltpu.CompilerParams(
            collective_id=0, has_side_effects=True, vmem_limit_bytes=60 * 1024 * 1024
        ),
    )(attention_output, residual, adapter_index.reshape(1, rows), output_weight, down, up)


def solution(mesh):
    return jax.shard_map(
        body,
        mesh=mesh,
        in_specs=(
            P("dp", "tensor"),
            P("dp", "tensor"),
            P("tensor", None),
            P("dp", "tensor", None),
            P("dp", None, "tensor"),
            P("dp"),
        ),
        out_specs=P("dp", "tensor"),
        check_vma=False,
    )
```

```python
import contextlib
import functools

import jax
import jax.numpy as jnp
from jax import lax
from jax.experimental import pallas as pl
from jax.experimental.pallas import tpu as pltpu
from jax.sharding import PartitionSpec as P

MESH = pl.DeviceIdType.MESH
F32 = jnp.float32
BF16 = jnp.bfloat16
LANES = 128
PIECES = 4
AHEAD = 4
FIRST = 2
HELD = 2
ORDER = (
    ("near", 0), ("project", 0, 0), ("project", 0, 1), ("project", 0, 2), ("settle", 0, 0),
    ("far", 0), ("project", 0, 3), ("settle", 0, 1), ("place", 1), ("factors",),
    ("project", 0, 4), ("settle", 0, 2), ("project", 0, 5), ("settle", 0, 3), ("far", 1),
    ("near", 1), ("project", 1, 0), ("project", 0, 6), ("settle", 0, 4), ("greet",),
    ("project", 0, 7), ("settle", 0, 5), ("settle", 0, 6), ("settle", 0, 7), ("relay", 0, 2, 0),
    ("relay", 0, 2, 1), ("relay", 0, 2, 2), ("relay", 0, 2, 3), ("requests",), ("relay", 0, 1, 0),
    ("relay", 0, 1, 1), ("shrink", 0), ("settle", 1, 0), ("first", 1, 0, 0), ("first", 0, 2, 0),
    ("first", 0, 2, 1), ("relay", 0, 1, 2), ("relay", 0, 1, 3), ("project", 1, 1), ("low", 0, 0),
    ("low", 0, 1), ("project", 1, 2), ("meet",), ("sum", 0), ("first", 1, 0, 1),
    ("project", 1, 3), ("settle", 1, 1), ("shrink", 1), ("project", 1, 4), ("high", 0, 0),
    ("high", 0, 1), ("sum", 1), ("first", 1, 0, 2), ("low", 0, 2), ("low", 0, 3),
    ("first", 1, 0, 3), ("settle", 1, 2), ("first", 1, 1, 0), ("first", 1, 1, 1),
    ("settle", 1, 3), ("project", 1, 5), ("relay", 1, 1, 0), ("project", 1, 6), ("project", 1, 7),
    ("high", 0, 2), ("high", 0, 3), ("first", 1, 1, 2), ("first", 1, 1, 3), ("settle", 1, 4),
    ("settle", 1, 5), ("first", 1, 2, 0), ("first", 1, 2, 1), ("first", 1, 2, 2),
    ("first", 1, 2, 3), ("settle", 1, 6), ("settle", 1, 7), ("expand", 0), ("relay", 1, 1, 1),
    ("relay", 1, 1, 2), ("relay", 1, 2, 0), ("relay", 1, 2, 1), ("relay", 1, 2, 2),
    ("relay", 1, 2, 3), ("expand", 1), ("relay", 1, 1, 3), ("first", 0, 2, 2), ("first", 0, 2, 3),
    ("low", 1, 0), ("high", 1, 0), ("low", 1, 1), ("high", 1, 1), ("low", 1, 2), ("high", 1, 2),
    ("low", 1, 3), ("high", 1, 3),
)
scope = contextlib.nullcontext


def kernel(
    groups, members, rank, owned, halves, pieces,
    x_hbm, res_ref, idx_hbm, w_ref, down_ref, up_ref, out_ref,
    x_ref, idx_ref, idx_all, wbuf, dbuf, ubuf, rbuf, own, psend, precv, rrecv, lrecv, rsend, lsend, jrecv,
    xsend, xrecv, wants, packed, arp, arz, esend, eback,
    w_sem, d_sem, ps_sem, pr_sem, rs_sem, ls_sem, hr_sem, j_sem,
    xs_sem, xr_sem, as_sem, ar_sem, zs_sem, zr_sem, es_sem, er_sem, dp_sem, z_sem, is_sem, ir_sem,
):
    chips = members // 2
    g = lax.axis_index("dp")
    t = lax.axis_index("tensor")
    z = t // 2
    c = lax.rem(t, 2)
    partner = z * 2 + (1 - c)
    rows, depth = x_ref.shape
    width = out_ref.shape[1]
    part = xrecv.shape[2]
    slots = groups * part
    low = z < chips // 2
    high = jnp.logical_not(low)
    piece = width // pieces
    last_chip = chips - 1
    wave = 2 if pieces % 2 == 0 else 1

    def core_of(chip):
        return (g, chip * 2 + c)

    bits = groups.bit_length() - 1
    cube = groups == 1 << bits

    def peer(k):
        if not cube:
            return lax.rem(g + k, groups)
        to = g
        for b in range(bits):
            if k >> b & 1:
                to = to + (1 << b) * (1 - 2 * lax.rem(g // (1 << b), 2))
        return to

    def source_of(k):
        return peer(k) if cube else lax.rem(g + groups - k, groups)

    near = [1 << b for b in range(bits)] if cube else list(range(1, groups))
    far = [k for k in range(1, groups) if k not in near]
    rounds = bits - 1 if far else 0

    barrier = pltpu.get_barrier_semaphore()
    pl.semaphore_signal(barrier, inc=1, device_id=(g, partner), device_id_type=MESH)

    @pl.when(z > 0)
    def _():
        pl.semaphore_signal(barrier, inc=1, device_id=core_of(z - 1), device_id_type=MESH)

    @pl.when(z < last_chip)
    def _():
        pl.semaphore_signal(barrier, inc=1, device_id=core_of(z + 1), device_id_type=MESH)

    for k in near:
        pl.semaphore_signal(barrier, inc=1, device_id=(peer(k), t), device_id_type=MESH)

    def block_chip(i):
        return jnp.where(low, chips - 1 - i, i)

    blocks = [(n, 0, width) for n in range(members)]
    if pieces % 2 == 0:
        blocks[:1] = [(0, p * width // 2, width // 2) for p in range(2)]
    chunks = len(blocks)
    loaded = set()

    def weight_copy(j):
        n, offset, size = blocks[j]
        column = block_chip(n % chips) * 2 + n // chips
        start = pl.multiple_of(column * width + offset, LANES)
        return pltpu.make_async_copy(
            w_ref.at[:, pl.ds(start, size)], wbuf.at[n, :, pl.ds(offset, size)],
            w_sem.at[j % AHEAD],
        )

    def weights(n, column):
        for j in range(chunks):
            if j not in loaded and blocks[j][:2] <= (n, column) and blocks[j][0] == n:
                weight_copy(j).wait()
                loaded.add(j)
                if j + AHEAD < chunks:
                    weight_copy(j + AHEAD).start()

    down_copy = pltpu.make_async_copy(down_ref, dbuf, d_sem.at[0])
    up_copy = pltpu.make_async_copy(up_ref, ubuf, d_sem.at[1])
    res_copy = pltpu.make_async_copy(res_ref, rbuf, d_sem.at[2])
    x_copy = pltpu.make_async_copy(x_hbm, x_ref, d_sem.at[0])
    idx_copy = pltpu.make_async_copy(idx_hbm, idx_ref, d_sem.at[1])
    idx_copy.start()
    x_copy.start()
    for j in range(min(FIRST, chunks)):
        weight_copy(j).start()

    def enter():
        near_chips = jnp.where(z > 0, 1, 0) + jnp.where(z < last_chip, 1, 0)
        pl.semaphore_wait(barrier, 1 + len(near) + near_chips)

    def tell(b):
        pl.semaphore_signal(
            dp_sem.at[b], inc=1, device_id=(peer(1 << b), t), device_id_type=MESH
        )

    def tell_chip(n, to):
        pl.semaphore_signal(z_sem.at[n], inc=1, device_id=core_of(to), device_id_type=MESH)

    def greet_far():
        for b in range(rounds):
            pl.semaphore_wait(dp_sem.at[b], 1)
            if b + 1 < rounds:
                tell(b + 1)

    def greet_ends():
        if chips < 3:
            return

        @pl.when(z == 0)
        def _():
            tell_chip(0, z + 1)

        @pl.when(z == last_chip)
        def _():
            tell_chip(1, z - 1)

    def greet_chips():
        if chips < 3:
            return

        @pl.when((z > 0) & low)
        def _():
            pl.semaphore_wait(z_sem.at[0], 1)
            tell_chip(0, z + 1)
            pl.semaphore_wait(z_sem.at[1], 1)
            tell_chip(1, z - 1)

        @pl.when((z < last_chip) & jnp.logical_not(low))
        def _():
            pl.semaphore_wait(z_sem.at[1], 1)
            tell_chip(1, z - 1)
            pl.semaphore_wait(z_sem.at[0], 1)
            tell_chip(0, z + 1)

    def meet_chips():
        if chips < 3:
            return

        @pl.when(z == 0)
        def _():
            pl.semaphore_wait(z_sem.at[1], 1)

        @pl.when(z == last_chip)
        def _():
            pl.semaphore_wait(z_sem.at[0], 1)

    idx_copy.wait()
    for j in range(FIRST, min(AHEAD, chunks)):
        weight_copy(j).start()
    idx_row = idx_ref[...]
    r_i = lax.broadcasted_iota(jnp.int32, (rows, rows), 0)
    c_i = lax.broadcasted_iota(jnp.int32, (rows, rows), 1)
    idx_full = jnp.broadcast_to(idx_row, (rows, rows))
    idx_col = jnp.sum(jnp.where(r_i == c_i, idx_full, 0), axis=1, keepdims=True)
    own_row = idx_row // owned
    own_col = idx_col // owned
    same = own_col == own_row
    rank_row = jnp.sum(jnp.where(same & (r_i < c_i), 1, 0), axis=0, keepdims=True)
    rank_col = jnp.sum(jnp.where(same & (c_i < r_i), 1, 0), axis=1, keepdims=True)

    def slot_of(place_rank, owner, h):
        inside = place_rank - h * part
        keep = (inside >= 0) & (inside < part)
        return jnp.where(keep, owner * part + inside, -1)

    step = min(256, depth)

    def row_copy(h, k):
        to = peer(k)
        return pltpu.make_async_remote_copy(
            src_ref=xsend.at[h, to], dst_ref=xrecv.at[h, g],
            send_sem=xs_sem.at[0], recv_sem=xr_sem.at[h],
            device_id=(to, t), device_id_type=MESH,
        )

    others = pl.ds(0, groups - 1)

    def all_of(send, recv, send_sem, recv_sem):
        return pltpu.make_async_remote_copy(
            src_ref=send, dst_ref=recv, send_sem=send_sem, recv_sem=recv_sem,
            device_id=(g, partner), device_id_type=MESH,
        )

    def idx_copy_to(k):
        return pltpu.make_async_remote_copy(
            src_ref=idx_ref, dst_ref=idx_all.at[g], send_sem=is_sem.at[0],
            recv_sem=ir_sem.at[0], device_id=(peer(k), t), device_id_type=MESH,
        )

    def requests():
        idx_all[g] = idx_ref[...]
        if groups > 1:
            all_of(
                idx_all.at[others], idx_all.at[others], is_sem.at[0], ir_sem.at[0]
            ).wait_recv()
        every_row = jnp.concatenate([idx_all[k] for k in range(groups)], axis=0)
        chosen = every_row // owned == g
        earlier = jnp.where(r_i < c_i, 1.0, 0.0).astype(BF16)
        ahead = jnp.dot(
            jnp.where(chosen, 1.0, 0.0).astype(BF16), earlier, preferred_element_type=F32
        ).astype(jnp.int32)
        slot = jnp.where(chosen, ahead, -1)
        number = lax.rem(every_row, owned) + 1
        for h in range(halves):
            for k in range(groups):
                place = lax.broadcasted_iota(jnp.int32, (part, rows), 0) + h * part
                asked = jnp.where(place == slot[k:k + 1], number[k:k + 1], 0)
                wants[h, k * part:(k + 1) * part] = jnp.broadcast_to(
                    jnp.sum(asked, axis=1, keepdims=True).astype(F32), (part, LANES)
                )

    def rows_wait(h):
        all_of(
            xsend.at[h, others], xrecv.at[h, others], xs_sem.at[0], xr_sem.at[h]
        ).wait_recv()

    def place_rows(h):
        slot_row = slot_of(rank_row, own_row, h)
        placing = lax.broadcasted_iota(jnp.int32, (slots, rows), 0) == slot_row
        place = jnp.where(placing, 1.0, 0.0).astype(BF16)
        for j in range(depth // step):
            moved = jnp.dot(
                place, x_ref[:, j * step:(j + 1) * step], preferred_element_type=F32
            ).astype(BF16)
            for k in range(groups):
                xsend[h, k, :, j * step:(j + 1) * step] = moved[k * part:(k + 1) * part]
        xrecv[h, g] = xsend[h, g]

    tile = min(256, piece)
    tiles = piece // tile

    def pair_copy(chip, q):
        k = chip * pieces + q
        return pltpu.make_async_remote_copy(
            src_ref=psend.at[k], dst_ref=precv.at[k], send_sem=ps_sem.at[0],
            recv_sem=pr_sem.at[chip * (pieces // wave) + q // wave],
            device_id=(g, partner), device_id_type=MESH,
        )

    strip = 16

    sent = set()

    def leaps(core, b):
        return chips > 2 and b in (0, last_chip)

    def hop(core, a, b, q):
        k = b * pieces + q
        to_right = b > a
        jump = leaps(core, b) and abs(b - a) == 2
        to = b if jump else (a + 1 if to_right else a - 1)
        if jump:
            landing = jrecv.at[q]
            arrival = j_sem.at[q]
        else:
            landing = (rrecv if to_right else lrecv).at[k]
            arrival = hr_sem.at[k + (pieces if to_right else 0)]
        return pltpu.make_async_remote_copy(
            src_ref=(rsend if to_right else lsend).at[k], dst_ref=landing,
            send_sem=(rs_sem if to_right else ls_sem).at[0], recv_sem=arrival,
            device_id=(g, to * 2 + c), device_id_type=MESH,
        ), landing

    def send(core, a, b, q):
        if (core, a, b, q) in sent:
            return
        sent.add((core, a, b, q))
        before = a - 1 if b > a else a + 1
        joins = 0 <= before < chips and not (leaps(core, b) and abs(b - a) == 1)

        @pl.when((c == core) & (z == a))
        def _():
            k = b * pieces + q
            if joins:
                copy, landed = hop(core, before, b, q)
                copy.wait_recv()
            out = rsend if b > a else lsend

            @pl.loop(0, rows // strip)
            def _(n):
                at = pl.ds(pl.multiple_of(n * strip, strip), strip)
                value = own[k, at] + precv[k, at].astype(F32)
                if joins:
                    value = value + landed[at].astype(F32)
                out[k, at] = value.astype(BF16)

            hop(core, a, b, q)[0].start()

    def send_first(core, turn, q):
        if turn < last_chip:
            send(core, 0, last_chip - turn, q)
            send(core, last_chip, turn, q)

    def send_relay(core, d, q):
        if 0 < d < last_chip:
            send(core, d, last_chip, q)
            send(core, last_chip - d, 0, q)

    def send_low(core, q):
        if chips > 3:
            send(core, 1, 2, q)

    def send_high(core, q):
        if chips > 3:
            send(core, last_chip - 1, last_chip - 2, q)

    steps = [(i, q) for i in range(chips) for q in range(0, pieces, wave)]

    def product(n, q, into, k):
        for m in range(tiles * wave):
            at = q * piece + m * tile
            into[k + m // tiles, :, m % tiles * tile:(m % tiles + 1) * tile] = jnp.dot(
                x_ref[...], wbuf[n, :, at:at + tile], preferred_element_type=F32
            ).astype(into.dtype)

    def project(phase, n):
        if phase + n == 0:
            @pl.when(c == 0)
            def _():
                product(0, 0, own, first_at)

            return
        i, q = steps[n]
        block = phase * chips + i
        k = block_chip(i) * pieces + q
        weights(block, q * piece)

        @pl.when(c == phase)
        def _():
            product(block, q, own, k)

        @pl.when(c != phase)
        def _():
            product(block, q, psend, k)
            send_other(n)

    def send_other(n):
        i, q = steps[n]
        for p in range(wave):
            pair_copy(block_chip(i), q + p).start()

    def settle(phase, n):
        i, first = steps[n]
        both = pl.ds(block_chip(i) * pieces + first, wave)

        @pl.when(c == phase)
        def _():
            all_of(
                psend.at[both], precv.at[both], ps_sem.at[0],
                pr_sem.at[block_chip(i) * (pieces // wave) + first // wave],
            ).wait_recv()

        if phase == 0 and i < HELD:
            for q in range(first, first + wave):
                send_first(0, i, q)

    lane_number = (lax.broadcasted_iota(jnp.int32, (slots, LANES), 1) // rank + 1).astype(F32)
    per_tile = LANES // rank
    tile_count = owned * rank // LANES
    chunk = min(512, owned * rank)

    def term_pair(h):
        return pltpu.make_async_remote_copy(
            src_ref=packed.at[h], dst_ref=arp.at[h], send_sem=as_sem.at[0],
            recv_sem=ar_sem.at[h], device_id=(g, partner), device_id_type=MESH,
        )

    def term_copy(h, k, core):
        to = lax.rem(z + jnp.where(low, chips - k, k), chips)
        return pltpu.make_async_remote_copy(
            src_ref=arz.at[h, z], dst_ref=arz.at[h, z], send_sem=zs_sem.at[0],
            recv_sem=zr_sem.at[h], device_id=(g, to * 2 + core), device_id_type=MESH,
        )

    def terms_wait(h):
        @pl.when(c == 0)
        def _():
            all_of(arz.at[h], arz.at[h], zs_sem.at[0], zr_sem.at[h]).wait_recv()

        if chips > 1:
            @pl.when(c == 1)
            def _():
                far_chips = pl.ds(0, chips - 1)
                all_of(
                    arz.at[h, far_chips], arz.at[h, far_chips], zs_sem.at[0], zr_sem.at[h]
                ).wait_recv()

    def wanted_of(h):
        return wants[h]

    def shrink_rows(h):
        rows_wait(h)
        if h == 0:
            down_copy.wait()
        wanted = wanted_of(h).T[:rank]
        flat = xrecv[h].reshape(slots, depth)
        mine = jnp.zeros((rank, slots), F32)
        for first in range(0, owned * rank, chunk):
            every = lax.dot_general(
                dbuf[first:first + chunk, :], flat, (((1,), (1,)), ((), ())),
                preferred_element_type=F32,
            )
            for p in range(chunk // rank):
                number = float(first // rank + p + 1)
                mine = jnp.where(wanted == number, every[p * rank:(p + 1) * rank], mine)
        packed[h] = mine

        @pl.when(c == 0)
        def _():
            term_pair(h).start()

    def sum_send(h):
        @pl.when(c == 1)
        def _():
            term_pair(h).wait_recv()
            arz[h, z] = (packed[h] + arp[h]).astype(BF16)
            for core in range(2):
                for k in range(1, chips):
                    term_copy(h, k, core).start()
            term_copy(h, 0, 0).start()

    def back_copy(h, k, cols):
        to = peer(k)
        return pltpu.make_async_remote_copy(
            src_ref=esend.at[h, to, :, cols], dst_ref=eback.at[h, g, :, cols],
            send_sem=es_sem.at[0], recv_sem=er_sem.at[h],
            device_id=(to, t), device_id_type=MESH,
        )

    def back_wait(h):
        all_of(
            esend.at[h, others], eback.at[h, others], es_sem.at[0], er_sem.at[h]
        ).wait_recv()

    wide = min(512, width)

    def expand_rows(h):
        terms_wait(h)
        total = arz[h, 0].astype(F32)
        for k in range(1, chips):
            total = total + arz[h, k].astype(F32)
        total = total.astype(BF16).astype(F32)
        if h == 0:
            up_copy.wait()
        wanted = wanted_of(h)
        shrink = jnp.concatenate([total] * per_tile, axis=0).T
        spread = jnp.concatenate(
            [
                jnp.where(wanted == lane_number + float(m * per_tile), shrink, 0.0).astype(BF16)
                for m in range(tile_count)
            ],
            axis=1,
        )

        for n in range(width // wide):
            cols = pl.ds(n * wide, wide)
            grown = jnp.dot(
                spread, ubuf[:, n * wide:(n + 1) * wide], preferred_element_type=F32
            ).astype(BF16)
            for k in range(groups):
                esend[h, k, :, cols] = grown[k * part:(k + 1) * part]
            for k in far + near:
                back_copy(h, k, cols).start()
        eback[h, g] = esend[h, g]

    with scope("x"):
        x_copy.wait()
    first_at = block_chip(0) * pieces
    weights(0, 0)

    @pl.when(c == 1)
    def _():
        product(0, 0, psend, first_at)

    with scope("enter"):
        enter()

    @pl.when(c == 1)
    def _():
        send_other(0)

    with scope("place0"):
        place_rows(0)
    if rounds:
        tell(0)
    greet_ends()

    def near_rows(h):
        for k in near:
            if h == 0:
                idx_copy_to(k).start()
            row_copy(h, k).start()

    def far_rows(h):
        if h == 0:
            greet_far()
        for k in far:
            if h == 0:
                idx_copy_to(k).start()
            row_copy(h, k).start()

    def load_factors():
        down_copy.start()
        up_copy.start()
        res_copy.start()

    stages = {
        "project": project, "settle": settle, "place": place_rows, "near": near_rows,
        "far": far_rows, "greet": greet_chips, "meet": meet_chips, "factors": load_factors,
        "shrink": shrink_rows, "sum": sum_send, "expand": expand_rows,
        "first": send_first, "relay": send_relay, "low": send_low, "high": send_high, "requests": requests,
    }
    for name, *at in ORDER:
        if name in ("first", "relay", "low", "high"):
            if at[-1] >= pieces:
                continue
        elif name in ("project", "settle"):
            if at[1] >= len(steps):
                continue
        elif at and at[0] >= halves:
            continue
        with scope(name + "_".join(str(v) for v in at)):
            stages[name](*at)
    for b in range(chips):
        for a in list(range(b)) + list(range(last_chip, b, -1)):
            for core in range(2):
                for q in range(pieces):
                    send(core, a, b, q)

    res_copy.wait()

    def branch_of(h, q, n):
        slot_col = slot_of(rank_col, own_col, h)
        unplace = jnp.where(
            lax.broadcasted_iota(jnp.int32, (rows, slots), 1) == slot_col, 1.0, 0.0
        ).astype(BF16)
        first = q * piece + n * tile
        back = eback[h, :, :, first:first + tile].reshape(slots, tile)
        return jnp.dot(unplace, back, preferred_element_type=F32)

    def close(core, q, into):
        for a in range(chips):
            @pl.when((c == core) & (z == a))
            def _():
                landed = []
                for step in (1, 2):
                    for source in (a - step, a + step):
                        if 0 <= source < chips and (step == 1 or leaps(core, a)):
                            copy, ref = hop(core, source, a, q)
                            copy.wait_recv()
                            landed.append(ref)

                @pl.loop(0, rows // strip)
                def _(n):
                    at = pl.ds(pl.multiple_of(n * strip, strip), strip)
                    value = own[a * pieces + q, at]
                    for ref in landed:
                        value = value + ref[at].astype(F32)
                    if into is own:
                        own[a * pieces + q, at] = value
                    else:
                        out_ref[at, q * piece:(q + 1) * piece] = value.astype(BF16)

    with scope("close0"):
        for q in range(pieces):
            close(0, q, own)

    for h in range(halves):
        with scope("backwait%d" % h):
            back_wait(h)
        for q in range(pieces):
            for n in range(tiles):
                cols = slice(n * tile, (n + 1) * tile)
                first = q * piece + n * tile
                value = own[z * pieces + q, :, cols] + branch_of(h, q, n)
                if h == 0:
                    value = (
                        value + precv[z * pieces + q, :, cols].astype(F32)
                        + rbuf[:, first:first + tile].astype(F32)
                    )
                own[z * pieces + q, :, cols] = value
                if h == halves - 1:
                    out_ref[:, first:first + tile] = value.astype(BF16)

    for q in range(pieces):
        with scope("fin%d" % q):
            close(1, q, out_ref)

    tail = scope("tail")
    tail.__enter__()
    all_of(psend, precv, ps_sem.at[0], ps_sem.at[0]).wait_send()

    @pl.when(c == 0)
    def _():
        all_of(packed, arp, as_sem.at[0], as_sem.at[0]).wait_send()

    @pl.when(c == 1)
    def _():
        all_of(arz, arz, zs_sem.at[0], zs_sem.at[0]).wait_send()
        if chips > 1:
            far_chips = pl.ds(0, chips - 1)
            all_of(
                arz.at[:, far_chips], arz.at[:, far_chips], zs_sem.at[0], zs_sem.at[0]
            ).wait_send()

    if groups > 1:
        all_of(
            xsend.at[:, others], xrecv.at[:, others], xs_sem.at[0], xs_sem.at[0]
        ).wait_send()
        all_of(
            esend.at[:, others], eback.at[:, others], es_sem.at[0], es_sem.at[0]
        ).wait_send()
        all_of(idx_all.at[others], idx_all.at[others], is_sem.at[0], is_sem.at[0]).wait_send()
    for chip in range(chips):
        @pl.when(z == chip)
        def _():
            if chip < last_chip:
                sent = pl.ds(0, (last_chip - chip) * pieces)
                all_of(
                    rsend.at[sent], rrecv.at[sent], rs_sem.at[0], rs_sem.at[0]
                ).wait_send()
            if chip > 0:
                sent = pl.ds(0, chip * pieces)
                all_of(
                    lsend.at[sent], lrecv.at[sent], ls_sem.at[0], ls_sem.at[0]
                ).wait_send()
    tail.__exit__(None, None, None)


def body(attention_output, residual, output_weight, down_factors, up_factors, adapter_index):
    groups = lax.axis_size("dp")
    members = lax.axis_size("tensor")
    rows, depth = attention_output.shape
    owned, _, rank = down_factors.shape
    width = output_weight.shape[1] // members
    cap = 2 * rows // groups
    chips = members // 2
    halves = 2 if cap % 32 == 0 else 1
    part = cap // halves
    slots = groups * part
    pieces = max(1, min(PIECES, width // 256))
    piece = width // pieces
    down = jnp.swapaxes(down_factors, 1, 2).reshape(owned * rank, depth)
    up = up_factors.reshape(owned * rank, width)
    vmem = pl.BlockSpec(memory_space=pltpu.VMEM)
    hbm = pl.BlockSpec(memory_space=pl.ANY)
    dma = pltpu.SemaphoreType.DMA
    hops = chips * pieces
    return pl.pallas_call(
        functools.partial(kernel, groups, members, rank, owned, halves, pieces),
        out_shape=pltpu.VMEM((rows, width), BF16),
        in_specs=[hbm] * 6,
        out_specs=vmem,
        scratch_shapes=[
            pltpu.VMEM((rows, depth), BF16),
            pltpu.VMEM((1, rows), jnp.int32),
            pltpu.VMEM((groups, 1, rows), jnp.int32),
            pltpu.VMEM((members, depth, width), BF16),
            pltpu.VMEM((owned * rank, depth), BF16),
            pltpu.VMEM((owned * rank, width), BF16),
            pltpu.VMEM((rows, width), BF16),
            pltpu.VMEM((hops, rows, piece), F32),
            pltpu.VMEM((hops, rows, piece), BF16),
            pltpu.VMEM((hops, rows, piece), BF16),
            pltpu.VMEM((hops, rows, piece), BF16),
            pltpu.VMEM((hops, rows, piece), BF16),
            pltpu.VMEM((hops, rows, piece), BF16),
            pltpu.VMEM((hops, rows, piece), BF16),
            pltpu.VMEM((pieces, rows, piece), BF16),
            pltpu.VMEM((halves, groups, part, depth), BF16),
            pltpu.VMEM((halves, groups, part, depth), BF16),
            pltpu.VMEM((halves, slots, LANES), F32),
            pltpu.VMEM((halves, rank, slots), F32),
            pltpu.VMEM((halves, rank, slots), F32),
            pltpu.VMEM((halves, chips, rank, slots), BF16),
            pltpu.VMEM((halves, groups, part, width), BF16),
            pltpu.VMEM((halves, groups, part, width), BF16),
            dma((AHEAD,)), dma((3,)), dma((1,)), dma((hops // (2 if pieces % 2 == 0 else 1),)),
            dma((1,)), dma((1,)), dma((hops + pieces,)), dma((pieces,)),
            dma((1,)), dma((halves,)), dma((1,)), dma((halves,)),
            dma((1,)), dma((halves,)), dma((1,)), dma((halves,)),
            pltpu.SemaphoreType.REGULAR((max(1, groups.bit_length() - 2),)),
            pltpu.SemaphoreType.REGULAR((2,)),
            dma((1,)), dma((1,)),
        ],
        compiler_params=pltpu.CompilerParams(
            collective_id=0, has_side_effects=True, vmem_limit_bytes=60 * 1024 * 1024
        ),
    )(attention_output, residual, adapter_index.reshape(1, rows), output_weight, down, up)


def solution(mesh):
    return jax.shard_map(
        body,
        mesh=mesh,
        in_specs=(
            P("dp", "tensor"),
            P("dp", "tensor"),
            P("tensor", None),
            P("dp", "tensor", None),
            P("dp", None, "tensor"),
            P("dp"),
        ),
        out_specs=P("dp", "tensor"),
        check_vma=False,
    )
```
